256 devices in a mesh: ctx: 64 (over z, x_hi, y), tp: 4 (over x_lo, core).
Axes of the slice: x: 4 (x_hi: 2, x_lo: 2; x = x_hi * 2 + x_lo), y: 4, z: 8, core: 2. Of those that a mesh axis runs over, the one named last changes fastest.
Arguments:
- queries: bfloat16 [32768, 4096], P('ctx', 'tp'), may hold values from -22 to 22
- keys: bfloat16 [32768, 512], P('ctx', 'tp'), may hold values from -22 to 22
- values: bfloat16 [32768, 512], P('ctx', 'tp'), may hold values from -36 to 36
- positions: int32 [3, 32768], P(None, 'ctx'), may hold values from 0 to 32767
- segment_ids: int32 [32768], replicated, may hold values from 0 to 31, never falling along the last dimension, each value on 1 to 2048 neighbouring positions
- out_weight: bfloat16 [4096, 8192], P('tp', 'ctx'), may hold values from -0.09375 to 0.09375
- residual: bfloat16 [32768, 8192], P(('ctx', 'tp')), may hold values from -3 to 3
Outputs:
- layer_out: bfloat16 [32768, 8192], P(('ctx', 'tp'))
The draws below stay inside these ranges and needn't reach their ends.
Inputs may be any that keep to these rules, and one draw needn't show every extreme that they name: `segment_ids`: ids never fall along the sequence; each document has 1 to 2048 tokens, and one has exactly 2048.
All inputs are finite; a program needn't handle non-finite values.
Results may differ from the reference program's by a relative error of at most 0.013.
Values may be sent and summed in bfloat16 or wider, within the bound.
A program may use at most 128 MiB of HBM per device.

```python
import math
import jax
import jax.numpy as jnp
import numpy as np
from jax import lax

D = 8192
HD = 128
HQ = 32
HK = 4
DOC = 2048
SEQ = 32768
DOCS = 32
N_TP = 4


def drawn_rows(key, row_count, col_count):
    base_key = jax.random.fold_in(key, 0)
    return jnp.clip(jax.random.normal(base_key, (row_count, col_count), jnp.float32), -6.0, 6.0)


def draw_queries(key, part):
    return drawn_rows(jax.random.fold_in(key, 11), SEQ, HQ * HD).astype(jnp.bfloat16)


def draw_keys(key, part):
    return drawn_rows(jax.random.fold_in(key, 23), SEQ, HK * HD).astype(jnp.bfloat16)


def plant(drawn, stream_key, least, largest):
    index_at = [jax.random.randint(jax.random.fold_in(stream_key, axis), (), 0, length) for axis, length in enumerate(drawn.shape)]
    main_axis = drawn.shape.index(max(drawn.shape))
    beside = index_at[:main_axis] + [(index_at[main_axis] + 1) % drawn.shape[main_axis]] + index_at[main_axis + 1:]
    return drawn.at[tuple(index_at)].set(least).at[tuple(beside)].set(largest)


def levels(key, extent, cuts, least, largest):
    gain = 1.0
    for dim, parts in cuts:
        steps = jax.random.uniform(jax.random.fold_in(jax.random.fold_in(key, 6), dim), (parts,), jnp.float32, least / len(cuts), largest / len(cuts))
        gain = gain * jnp.repeat(jnp.exp(steps), extent[dim] // parts).reshape((-1,) + (1,) * (len(extent) - 1 - dim))
    return gain


def length_profile(count, total, reach, lean):
    portions = [(1 << 20) // math.isqrt(grade ** lean) + 1 for grade in range(2, count + 1)]
    surplus, counts = total - reach - (count - 1), [1] * (count - 1)
    while surplus > 0:
        movable = [i for i in range(count - 1) if counts[i] < reach]
        mass, remaining = sum([portions[i] for i in movable]), surplus
        for i in movable:
            extra = min(reach - counts[i], max(1, remaining * portions[i] // mass), surplus)
            counts[i] = counts[i] + extra
            surplus = surplus - extra
    return np.array([reach] + counts)


def uneven(stream_key, number_of, total, bound, skew):
    if number_of == 2:
        one = jax.random.randint(stream_key, (), max(1, total - bound), min(bound, total - 1) + 1)
        return jnp.stack([one, total - one])
    sizes = jnp.asarray(length_profile(number_of, total, bound, skew), jnp.int32)
    couples = (number_of - 1) // 2
    source_of, receiver = sizes[1:1 + 2 * couples:2], sizes[2:2 + 2 * couples:2]
    margin = jnp.minimum(source_of - 1, bound - receiver)
    moved = jax.random.randint(jax.random.fold_in(stream_key, 1), (couples,), 0, 1 << 20) % (margin + 1)
    sizes = sizes.at[1:1 + 2 * couples:2].set(source_of - moved).at[2:2 + 2 * couples:2].set(receiver + moved)
    return sizes[jax.random.permutation(jax.random.fold_in(stream_key, 2), number_of)]


def noise(stream_key, shape, scale, limit, shards=(), kind=jnp.bfloat16):
    array = jax.random.normal(stream_key, shape, jnp.float32) * scale
    if len(shards) > 0:
        array = levels(stream_key, shape, shards, -0.22, 0.18) * array
    return jnp.clip(array, min=-limit, max=limit).astype(kind)


def setup_inputs(seed: int = 0) -> dict:
    seeds = jax.random.split(jax.random.key(seed), 8)
    return {
        "queries": draw_queries(jax.random.fold_in(seeds[7], 71), 0),
        "keys": draw_keys(jax.random.fold_in(seeds[7], 71), 0),
        "values": noise(seeds[2], (SEQ, HK * HD), 6.0, 36.0, ((0, 64), (1, 4))),
        "positions": plant(jax.random.randint(seeds[3], (3, SEQ), 0, SEQ), jax.random.fold_in(seeds[3], 1), 0, SEQ - 1).astype(jnp.int32),
        "segment_ids": jnp.searchsorted(jnp.cumsum(uneven(seeds[4], DOCS, SEQ, DOC, 1)), jnp.arange(SEQ), side="right").astype(jnp.int32),
        "out_weight": noise(seeds[5], (HQ * HD, D), (HQ * HD) ** -0.5, 0.09375, ((0, 4), (1, 64))),
        "residual": noise(seeds[6], (SEQ, D), 0.5, 3.0, ((0, 256),)),
    }


theta_base = 1000000.0

def rotary_tables(positions):
    half_dim = HD // 2
    freq_index = jnp.arange(half_dim)
    inv_freq = theta_base ** (-2.0 * freq_index.astype(jnp.float32) / HD)
    first_end = HD // 8
    second_end = first_end + 3 * HD // 16
    place = positions.astype(jnp.float32)
    chosen = jnp.where(freq_index[None, :] < first_end, place[0][:, None], jnp.where(freq_index[None, :] < second_end, place[1][:, None], place[2][:, None]))
    angle = chosen * inv_freq[None, :]
    return (jnp.cos(angle), jnp.sin(angle))

def rotate(vectors, cosine_table, sine_table):
    half_dim = HD // 2
    lower_half = vectors[..., :half_dim]
    upper_half = vectors[..., half_dim:]
    cos_b = cosine_table[:, None, :]
    sin_b = sine_table[:, None, :]
    return jnp.concatenate([lower_half * cos_b - upper_half * sin_b, upper_half * cos_b + lower_half * sin_b], axis=-1)

def reference(queries, keys, values, positions, segment_ids, out_weight, residual):
    seq_len = queries.shape[0]
    group_size = HQ // HK
    cosine_table, sine_table = rotary_tables(positions)
    rot_q = rotate(queries.reshape(seq_len, HQ, HD).astype(jnp.float32), cosine_table, sine_table).astype(jnp.bfloat16)
    rot_k = rotate(keys.reshape(seq_len, HK, HD).astype(jnp.float32), cosine_table, sine_table).astype(jnp.bfloat16)
    key_heads = rot_k.transpose(1, 0, 2)
    value_heads = values.reshape(seq_len, HK, HD).transpose(1, 0, 2)
    query_rows = math.gcd(seq_len, 512)
    key_span = min(seq_len, DOC + query_rows)
    score_scale = 1.0 / math.sqrt(HD)

    def one_block(block_index):
        begin = (block_index * query_rows).astype(jnp.int32)
        key_start = jnp.clip(begin + query_rows - key_span, 0, seq_len - key_span).astype(jnp.int32)
        query_block = lax.dynamic_slice_in_dim(rot_q, begin, query_rows, 0)
        query_index = begin + jnp.arange(query_rows, dtype=jnp.int32)
        key_index = key_start + jnp.arange(key_span, dtype=jnp.int32)
        query_seg = lax.dynamic_slice_in_dim(segment_ids, begin, query_rows, 0)
        key_seg = lax.dynamic_slice_in_dim(segment_ids, key_start, key_span, 0)
        allowed = (key_index[None, :] <= query_index[:, None]) & (key_seg[None, :] == query_seg[:, None])
        grouped = query_block.reshape(query_rows, HK, group_size, HD).transpose(1, 0, 2, 3)
        key_part = lax.dynamic_slice_in_dim(key_heads, key_start, key_span, 1)
        value_part = lax.dynamic_slice_in_dim(value_heads, key_start, key_span, 1)

        def one_head(operands):
            query_head, key_head, value_head = operands
            score = jnp.einsum('qgd,nd->gqn', query_head.astype(jnp.float32), key_head.astype(jnp.float32)) * score_scale
            score = jnp.where(allowed[None], score, -1e+30)
            row_peak = lax.optimization_barrier(jnp.max(score, axis=-1, keepdims=True))
            prob = jnp.where(allowed[None], jnp.exp(score - row_peak), 0.0)
            row_sum = lax.optimization_barrier(jnp.sum(prob, axis=-1))
            mixed = jnp.einsum('gqn,nd->gqd', prob.astype(jnp.bfloat16).astype(jnp.float32), value_head.astype(jnp.float32))
            return (mixed / row_sum[..., None]).transpose(1, 0, 2)
        heads_out = lax.map(one_head, (grouped, key_part, value_part))
        return heads_out.transpose(1, 0, 2, 3).reshape(query_rows, HQ * HD)
    blocks = lax.map(one_block, jnp.arange(seq_len // query_rows, dtype=jnp.int32))
    attended = blocks.reshape(seq_len, HQ * HD).astype(jnp.bfloat16)
    part_cols = HQ * HD // N_TP
    summed = residual.astype(jnp.float32)
    for part_index in range(N_TP):
        cols = attended[:, part_index * part_cols:(part_index + 1) * part_cols]
        rows_w = out_weight[part_index * part_cols:(part_index + 1) * part_cols]
        partial_sum = jnp.dot(cols, rows_w, preferred_element_type=jnp.float32).astype(jnp.bfloat16)
        summed = summed + partial_sum.astype(jnp.float32)
    return summed.astype(jnp.bfloat16)
```

```python
import functools
import heapq
import math

import jax
import jax.numpy as jnp
from jax import lax
from jax.experimental import pallas as pl
from jax.experimental.pallas import tpu as pltpu
from jax.sharding import PartitionSpec as P

HD = 128
DOC = 2048
HEADS = 8
TOK = 512
ROWS_A = 480
ROWS_B = 1024 - ROWS_A
NC = 64
BACK = 4
KIB = 1024.0
RATE = 46.6e3 / KIB
HOP = 1.7
PIECE = 0.55
theta_base = 1000000.0
MESH = pl.DeviceIdType.MESH
DZS = (0, 1, -1, 2, -2, 3, -3, 4)


def build_tasks():
    t = {}
    rb, ra = ROWS_B / 4, ROWS_A / 4
    for j in range(1, BACK + 1):
        t[("kv", j)] = ("y+" if j < 3 else "x", 256.0, ())
    t[("h", "b")] = ("x", rb * 2, ())
    t[("h", "a")] = ("x", ra * 2, ())

    def b_has(dz, dh):
        if dz == 0:
            return () if dh == 0 else (("h", "b"),)
        if abs(dz) == 4:
            return (("bz+", 3, dh), ("bz-", 3, dh))
        return (("bz+", dz * -1 - 1, dh),) if dz < 0 else (("bz-", dz - 1, dh),)

    for s in range(4):
        for dh in (0, 1):
            size = rb if s < 3 else rb / 2
            t[("bz+", s, dh)] = ("z+", size, b_has(-s, dh))
            t[("bz-", s, dh)] = ("z-", size, b_has(s, dh))
    for dh in (0, 1):
        t[("ay+", dh)] = ("y+", ra, () if dh == 0 else (("h", "a"),))
        t[("ay-", dh)] = ("y-", ra, () if dh == 0 else (("h", "a"),))
        t[("ar+", dh)] = ("y+", ra / 2, (("ay+", dh),))
        t[("ar-", dh)] = ("y-", ra / 2, (("ay-", dh),))
    column = (("h", "a"),) + tuple((k, dh) for dh in (0, 1) for k in ("ay+", "ay-", "ar+", "ar-"))
    for s in range(4):
        size = ra * 8 if s < 3 else ra * 4
        t[("az+", s)] = ("z+", size, column if s == 0 else (("az+", s - 1),))
        t[("az-", s)] = ("z-", size, column if s == 0 else (("az-", s - 1),))
    for dz in DZS:
        for dh in (0, 1):
            need = b_has(dz, dh)
            t[("by+", dz, dh)] = ("y+", rb, need)
            t[("by-", dz, dh)] = ("y-", rb, need)
            t[("br+", dz, dh)] = ("y+", rb / 2, (("by+", dz, dh),))
            t[("br-", dz, dh)] = ("y-", rb / 2, (("by-", dz, dh),))
    return t


def group_needs(t, dz):
    need = set()
    for dh in (0, 1):
        need |= set(t[("by+", dz, dh)][2])
        need |= {(k, dz, dh) for k in ("by+", "by-", "br+", "br-")}
    if dz == 0:
        need |= set(t[("az+", 0)][2])
    elif dz == 4:
        need |= {("az+", 3), ("az-", 3)}
    else:
        need.add(("az+", -dz - 1) if dz < 0 else ("az-", dz - 1))
    return tuple(sorted(need, key=str))


def plan(t):
    rank = {}
    for n, name in enumerate(t):
        kind = name[0]
        if kind == "kv":
            r = 0
        elif kind == "h":
            r = 1
        elif kind in ("bz+", "bz-"):
            r = 3 + name[1]
        elif kind[0] == "a" and kind[1] in "yr":
            r = 2
        elif kind[:2] == "az":
            r = 10
        else:
            r = 4 + 4 * abs(name[1])
        rank[name] = (r, n)
    link_free = {}
    arrive = {}
    pending = sorted(t, key=lambda k: rank[k])
    order, now = [], 0.0
    computes = [("attn", s, h) for s in range(BACK + 1) for h in range(HEADS)]
    mats = [("M", dz) for dz in DZS]
    sums, finals = [], []
    done = {}
    cost = {"M": 2.0, "S": 0.6, "F": 0.3}

    def needs_of(c):
        if c[0] == "attn":
            return (("kv", c[1]),) if c[1] else ()
        if c[0] == "M":
            return group_needs(t, c[1])
        return ()

    def ready(names):
        return all(arrive.get(n, 1e9) <= now for n in names)

    def send(name, link, size):
        start = max(now, link_free.get(link, 0.0))
        link_free[link] = start + size / RATE
        arrive[name] = link_free[link] + HOP

    while pending or computes or mats or sums or finals:
        moved = [n for n in pending if ready(t[n][2])]
        for n in moved:
            order.append(("send", n))
            send(n, t[n][0], t[n][1])
            pending.remove(n)
        pick = None
        if finals and arrive[("c", finals[0])] <= now and not computes:
            pick = ("F", finals.pop(0))
        elif sums and arrive[("d", sums[0])] <= now:
            pick = ("S", sums.pop(0))
        elif computes and ready(needs_of(computes[0])):
            pick = computes.pop(0)
        elif not computes and mats:
            ok = [c for c in mats if ready(needs_of(c))]
            if ok:
                pick = ok[0]
                mats.remove(pick)
        if pick:
            order.append(pick)
            now += PIECE if pick[0] == "attn" else cost[pick[0]]
            done[pick] = now
            if pick[0] == "M":
                send(("d", pick[1]), "d", 512.0 / 12)
                sums.append(pick[1])
            if pick[0] == "S":
                send(("c", pick[1]), "c", 256.0)
                finals.append(pick[1])
            continue
        later = [a for a in arrive.values() if a > now]
        assert later, "stuck"
        now = min(later) + 1e-6
    return order, now


TASKS = build_tasks()
ORDER, MODEL_US = plan(TASKS)
NAMES = list(TASKS)
NUMBER = {n: i for i, n in enumerate(NAMES)}


def kernel(
    q_hbm, k_hbm, v_hbm, cos_hbm, sin_hbm, segq_ref, segk_ref, w_hbm, res_hbm, out_ref,
    wa, wb, q, cos, sin, kbuf, vbuf, bias, vone, top, acc, att,
    dsend, drecv, keep, other, csend, crecv, res,
    send_sem, recv_sem, dsem, drsem, csem, crsem, kvs2, kvr2, hs2, hr2, local,
):
    c = lax.axis_index("ctx")
    t = lax.axis_index("tp")
    z, h, y = c // 8, (c // 4) % 2, c % 4
    core = t % 2
    chip = t // 2
    mate = chip * 2 + (1 - core)
    across = (1 - chip) * 2 + core

    def at(dz, dh, dy):
        return ((z + dz + 8) % 8) * 8 + ((h + dh) % 2) * 4 + (y + dy + 4) % 4

    def ctx_of(dz, dh, dy):
        return (at(dz, dh, dy), t)

    barrier = pltpu.get_barrier_semaphore()
    partners = [ctx_of(1, 0, 0), ctx_of(-1, 0, 0), ctx_of(0, 0, 1), ctx_of(0, 0, -1),
                ctx_of(0, 1, 0), (c, mate), (c, across)]
    for j in range(1, BACK + 1):
        partners.append(((c + j) % NC, t))
        partners.append(((c - j + NC) % NC, t))
    for d in partners:
        pl.semaphore_signal(barrier, inc=1, device_id=d, device_id_type=MESH)

    loads = {
        "wa": pltpu.make_async_copy(w_hbm.at[pl.ds(0, ROWS_A)], wa.at[c], local.at[0]),
        "wb": pltpu.make_async_copy(w_hbm.at[pl.ds(ROWS_A, ROWS_B)], wb.at[c], local.at[1]),
        "k": pltpu.make_async_copy(k_hbm, kbuf.at[0], local.at[2]),
        "v": pltpu.make_async_copy(v_hbm, vbuf.at[0], local.at[3]),
        "q": pltpu.make_async_copy(q_hbm, q, local.at[4]),
        "cos": pltpu.make_async_copy(cos_hbm, cos, local.at[5]),
        "sin": pltpu.make_async_copy(sin_hbm, sin, local.at[6]),
        "res": pltpu.make_async_copy(res_hbm, res, local.at[7]),
    }
    for k in ("k", "v", "wb", "wa", "q", "cos", "sin", "res"):
        loads[k].start()
    pl.semaphore_wait(barrier, len(partners))
    for k in ("k", "v", "wb", "wa"):
        loads[k].wait()

    half_b = ROWS_B // 2
    half_a = ROWS_A // 2

    def copies(name, incoming):
        kind = name[0]
        n = NUMBER[name]
        sems = (send_sem.at[n], recv_sem.at[n])

        def one(src, dst, dev, pair=sems):
            return pltpu.make_async_remote_copy(
                src_ref=src, dst_ref=dst, send_sem=pair[0], recv_sem=pair[1],
                device_id=dev, device_id_type=MESH)

        def same(ref, dev, pair=sems):
            return one(ref, ref, dev, pair)

        if kind == "kv":
            j = name[1]
            dev = ((c + j) % NC, t)
            return [one(kbuf.at[0], kbuf.at[j], dev),
                    one(vbuf.at[0], vbuf.at[j], dev, (kvs2.at[j - 1], kvr2.at[j - 1]))]
        if kind == "h":
            i = at(0, 1, 0) if incoming else c
            dev = ctx_of(0, 1, 0)
            return [same((wb if name[1] == "b" else wa).at[i], dev)]
        sign = 1 if kind[2] == "+" else -1
        if kind[:2] == "bz":
            s, dh = name[1], name[2]
            i = at(-sign * (s + (1 if incoming else 0)), dh, 0)
            ref = wb.at[i]
            if s == 3:
                ref = wb.at[i, pl.ds(0 if sign > 0 else half_b, half_b)]
            return [same(ref, ctx_of(sign, 0, 0))]
        if kind[:2] == "az":
            s = name[1]
            zz = ((z - sign * (s + (1 if incoming else 0)) + 8) % 8) * 8
            if s < 3:
                ref = wa.at[pl.ds(zz, 8)]
            else:
                ref = wa.at[pl.ds(zz + (0 if sign > 0 else 4), 4)]
            return [same(ref, ctx_of(sign, 0, 0))]
        if kind[0] == "a":
            dz, dh, buf, half = 0, name[1], wa, half_a
        else:
            dz, dh, buf, half = name[1], name[2], wb, half_b
        relay = kind[1] == "r"
        step = (1 if relay else 0) + (1 if incoming else 0)
        i = at(dz, dh, -sign * step)
        ref = buf.at[i]
        if relay:
            ref = buf.at[i, pl.ds(0 if sign > 0 else half, half)]
        return [same(ref, ctx_of(0, 0, sign))]

    got = set()

    def need(names):
        for name in names:
            if name not in got:
                got.add(name)
                for cp in copies(name, True):
                    cp.wait_recv()

    def send(name):
        need(TASKS[name][2])
        for cp in copies(name, False):
            cp.start()

    ready = {"attn": False}
    qk = (((1,), (1,)), ((), ()))
    scale2 = (1.0 / math.sqrt(HD)) * math.log2(math.e)

    def attn_setup(s):
        if s == 0:
            for k in ("q", "cos", "sin"):
                loads[k].wait()
            vone[:, HD:] = jnp.ones((TOK, HD), jnp.bfloat16)
        need((("kv", s),) if s else ())
        segk = segk_ref[pl.ds(BACK - s, 1), :]
        same = segq_ref[...] == segk
        if s == 0:
            row = lax.broadcasted_iota(jnp.int32, (TOK, TOK), 0)
            col = lax.broadcasted_iota(jnp.int32, (TOK, TOK), 1)
            same = same & (col <= row)
        bias[...] = jnp.where(same, 0.0, -1e30).astype(jnp.float32)
        vone[:, :HD] = vbuf[s]

    def attn_piece(s, hd):
        cols = pl.ds(pl.multiple_of(hd * HD, HD), HD)
        if s == 0:
            x = q[:, cols].astype(jnp.float32)
            x = x * cos[...] + pltpu.roll(x, HD // 2, 1) * sin[...]
            qh = x.astype(jnp.bfloat16)
            q[:, cols] = qh
        else:
            qh = q[:, cols]
        score = lax.dot_general(qh, kbuf[s], qk, preferred_element_type=jnp.float32) + bias[...]
        peak = jnp.max(score, axis=1, keepdims=True)
        if s > 0:
            old = top[hd]
            peak = jnp.maximum(peak, old)
        prob = jnp.exp2((score - peak) * scale2).astype(jnp.bfloat16)
        mixed = jnp.dot(prob, vone[...], preferred_element_type=jnp.float32)
        if s > 0:
            mixed = mixed + acc[hd] * jnp.exp2((old - peak) * scale2)
        if s < BACK:
            top[hd] = peak
            acc[hd] = mixed
        else:
            att[:, cols] = (mixed[:, :HD] / mixed[:, HD:]).astype(jnp.bfloat16)

    def group(dz):
        return (z + dz + 8) % 8

    def d_copy(n):
        return pltpu.make_async_remote_copy(
            src_ref=dsend.at[n], dst_ref=drecv.at[n], send_sem=dsem.at[n], recv_sem=drsem.at[n],
            device_id=(c, mate), device_id_type=MESH)

    def c_copy(n):
        return pltpu.make_async_remote_copy(
            src_ref=csend.at[n], dst_ref=crecv.at[n], send_sem=csem.at[n], recv_sem=crsem.at[n],
            device_id=(c, across), device_id_type=MESH)

    def rows_of(tp):
        return pl.ds(pl.multiple_of(tp * 128, 128), 128)

    across_mate = (1 - chip) * 2 + (1 - core)

    def matmul(dz):
        n = DZS.index(dz)
        need(group_needs(TASKS, dz))
        base = group(dz) * 8

        def body(j, carry):
            i = base + 2 * j
            rhs = jnp.concatenate(
                [jnp.concatenate([wa[i], wb[i]], axis=0),
                 jnp.concatenate([wa[i + 1], wb[i + 1]], axis=0)], axis=1)
            cols = pl.ds(pl.multiple_of(j * 256, 256), 256)

            def part(tp):
                return jnp.dot(att[rows_of(tp), :], rhs, preferred_element_type=jnp.float32)

            dsend[n, 0, :, cols] = part(mate).astype(jnp.bfloat16)
            dsend[n, 1, :, cols] = part(across_mate).astype(jnp.bfloat16)
            keep[n, :, cols] = part(t)
            other[n, :, cols] = part(across)
            return carry

        lax.fori_loop(0, 4, body, 0)
        d_copy(n).start()

    def summed(dz):
        n = DZS.index(dz)
        d_copy(n).wait_recv()

        def body(j, carry):
            cols = pl.ds(pl.multiple_of(j * 256, 256), 256)
            csend[n, :, cols] = (
                other[n, :, cols] + drecv[n, 1, :, cols].astype(jnp.float32)).astype(jnp.bfloat16)
            return carry

        lax.fori_loop(0, 4, body, 0)
        c_copy(n).start()

    def final(dz):
        n = DZS.index(dz)
        if n == 0:
            loads["res"].wait()
        c_copy(n).wait_recv()
        first = group(dz) * 1024

        def body(j, carry):
            cols = pl.ds(pl.multiple_of(j * 256, 256), 256)
            wide = pl.ds(pl.multiple_of(first + j * 256, 256), 256)
            total = keep[n, :, cols] + drecv[n, 0, :, cols].astype(jnp.float32)
            total = total + crecv[n, :, cols].astype(jnp.float32)
            out_ref[:, wide] = (total + res[:, wide].astype(jnp.float32)).astype(jnp.bfloat16)
            return carry

        lax.fori_loop(0, 4, body, 0)

    i = 0
    items = ORDER
    while i < len(items):
        item = items[i]
        if item[0] == "attn":
            seg = item[1]
            slots = {}
            hd = -1
            while i < len(items) and (items[i][0] == "send" or items[i][:2] == ("attn", seg)):
                if items[i][0] == "attn":
                    hd = items[i][2]
                else:
                    slots.setdefault(hd, []).append(items[i][1])
                i += 1
            attn_setup(seg)

            def body(hd, carry, seg=seg, slots=slots):
                attn_piece(seg, hd)
                for k, names in slots.items():
                    def issue(names=names):
                        for name in names:
                            send(name)
                    pl.when(hd == k)(issue)
                return carry

            lax.fori_loop(0, HEADS, body, 0)
            continue
        if item[0] == "send":
            send(item[1])
        elif item[0] == "M":
            matmul(item[1])
        elif item[0] == "S":
            summed(item[1])
        else:
            final(item[1])
        i += 1
    for name in NAMES:
        assert name in got, name
        for cp in copies(name, False):
            cp.wait_send()
    for n in range(8):
        d_copy(n).wait_send()
        c_copy(n).wait_send()


def rotary_tables(positions):
    half_dim = HD // 2
    freq_index = jnp.arange(half_dim)
    inv_freq = theta_base ** (-2.0 * freq_index.astype(jnp.float32) / HD)
    first_end = HD // 8
    second_end = first_end + 3 * HD // 16
    place = positions.astype(jnp.float32)
    chosen = jnp.where(
        freq_index[None, :] < first_end,
        place[0][:, None],
        jnp.where(freq_index[None, :] < second_end, place[1][:, None], place[2][:, None]),
    )
    angle = chosen * inv_freq[None, :]
    return (jnp.cos(angle), jnp.sin(angle))


def on_device(queries, keys, values, positions, segment_ids, out_weight, residual):
    cosine, sine = rotary_tables(positions)
    cos2 = jnp.concatenate([cosine, cosine], axis=1)
    sin2 = jnp.concatenate([-sine, sine], axis=1)
    kf = keys.astype(jnp.float32)
    swapped = jnp.concatenate([kf[:, HD // 2:], kf[:, :HD // 2]], axis=1)
    rot_k = (kf * cos2 + swapped * sin2).astype(jnp.bfloat16)
    my = lax.axis_index("ctx")
    wrapped = jnp.concatenate([segment_ids[-BACK * TOK:], segment_ids])
    window = lax.dynamic_slice_in_dim(wrapped, my * TOK, (BACK + 1) * TOK, 0)
    segk = jnp.concatenate(
        [window.reshape(BACK + 1, TOK), jnp.zeros((7 - BACK, TOK), jnp.int32)], axis=0)
    segq = window[BACK * TOK:].reshape(TOK, 1)
    anyspec = pl.BlockSpec(memory_space=pl.ANY)
    vmem = pl.BlockSpec(memory_space=pltpu.VMEM)
    nt = len(NAMES)
    bf, f32 = jnp.bfloat16, jnp.float32
    return pl.pallas_call(
        kernel,
        out_shape=jax.ShapeDtypeStruct((128, 8192), bf),
        in_specs=[anyspec] * 5 + [vmem] * 2 + [anyspec] * 2,
        out_specs=vmem,
        scratch_shapes=[
            pltpu.VMEM((NC, ROWS_A, 128), bf),
            pltpu.VMEM((NC, ROWS_B, 128), bf),
            pltpu.VMEM((TOK, 1024), bf),
            pltpu.VMEM((TOK, HD), f32),
            pltpu.VMEM((TOK, HD), f32),
            pltpu.VMEM((BACK + 1, TOK, HD), bf),
            pltpu.VMEM((BACK + 1, TOK, HD), bf),
            pltpu.VMEM((TOK, TOK), f32),
            pltpu.VMEM((TOK, 2 * HD), bf),
            pltpu.VMEM((HEADS, TOK, 1), f32),
            pltpu.VMEM((HEADS, TOK, 2 * HD), f32),
            pltpu.VMEM((TOK, 1024), bf),
            pltpu.VMEM((8, 2, 128, 1024), bf),
            pltpu.VMEM((8, 2, 128, 1024), bf),
            pltpu.VMEM((8, 128, 1024), f32),
            pltpu.VMEM((8, 128, 1024), f32),
            pltpu.VMEM((8, 128, 1024), bf),
            pltpu.VMEM((8, 128, 1024), bf),
            pltpu.VMEM((128, 8192), bf),
            pltpu.SemaphoreType.DMA((nt,)),
            pltpu.SemaphoreType.DMA((nt,)),
            pltpu.SemaphoreType.DMA((8,)),
            pltpu.SemaphoreType.DMA((8,)),
            pltpu.SemaphoreType.DMA((8,)),
            pltpu.SemaphoreType.DMA((8,)),
            pltpu.SemaphoreType.DMA((BACK,)),
            pltpu.SemaphoreType.DMA((BACK,)),
            pltpu.SemaphoreType.DMA((1,)),
            pltpu.SemaphoreType.DMA((1,)),
            pltpu.SemaphoreType.DMA((8,)),
        ],
        compiler_params=pltpu.CompilerParams(
            collective_id=0, has_side_effects=True, vmem_limit_bytes=62 * 1024 * 1024),
    )(queries, rot_k, values, cos2, sin2, segq, segk, out_weight, residual)


def solution(mesh):
    return jax.shard_map(
        on_device,
        mesh=mesh,
        in_specs=(
            P("ctx", "tp"),
            P("ctx", "tp"),
            P("ctx", "tp"),
            P(None, "ctx"),
            P(),
            P("tp", "ctx"),
            P(("ctx", "tp"), None),
        ),
        out_specs=P(("ctx", "tp"), None),
        check_vma=False,
    )
```

```python
import functools
import heapq
import math

import jax
import jax.numpy as jnp
from jax import lax
from jax.experimental import pallas as pl
from jax.experimental.pallas import tpu as pltpu
from jax.sharding import PartitionSpec as P

HD = 128
DOC = 2048
HEADS = 8
TOK = 512
ROWS_A = 480
ROWS_B = 1024 - ROWS_A
NC = 64
BACK = 4
KIB = 1024.0
RATE = 46.6e3 / KIB
HOP = 1.7
PIECE = 0.55
AHEAD = 4.0
theta_base = 1000000.0
MESH = pl.DeviceIdType.MESH
DZS = (0, 1, -1, 2, -2, 3, -3, 4)


def build_tasks():
    t = {}
    rb, ra = ROWS_B / 4, ROWS_A / 4
    for j in range(1, BACK + 1):
        t[("kv", j)] = ("y+" if j < 3 else "x", 256.0, ())
    t[("h", "b")] = ("x", rb * 2, ())
    t[("h", "a")] = ("x", ra * 2, ())

    def b_has(dz, dh):
        if dz == 0:
            return () if dh == 0 else (("h", "b"),)
        if abs(dz) == 4:
            return (("bz+", 3, dh), ("bz-", 3, dh))
        return (("bz+", dz * -1 - 1, dh),) if dz < 0 else (("bz-", dz - 1, dh),)

    for s in range(4):
        for dh in (0, 1):
            size = rb if s < 3 else rb / 2
            t[("bz+", s, dh)] = ("z+", size, b_has(-s, dh))
            t[("bz-", s, dh)] = ("z-", size, b_has(s, dh))
    for dh in (0, 1):
        t[("ay+", dh)] = ("y+", ra, () if dh == 0 else (("h", "a"),))
        t[("ay-", dh)] = ("y-", ra, () if dh == 0 else (("h", "a"),))
        t[("ar+", dh)] = ("y+", ra / 2, (("ay+", dh),))
        t[("ar-", dh)] = ("y-", ra / 2, (("ay-", dh),))
    column = (("h", "a"),) + tuple((k, dh) for dh in (0, 1) for k in ("ay+", "ay-", "ar+", "ar-"))
    for s in range(4):
        size = ra * 8 if s < 3 else ra * 4
        t[("az+", s)] = ("z+", size, column if s == 0 else (("az+", s - 1),))
        t[("az-", s)] = ("z-", size, column if s == 0 else (("az-", s - 1),))
    for dz in DZS:
        for dh in (0, 1):
            need = b_has(dz, dh)
            t[("by+", dz, dh)] = ("y+", rb, need)
            t[("by-", dz, dh)] = ("y-", rb, need)
            t[("br+", dz, dh)] = ("y+", rb / 2, (("by+", dz, dh),))
            t[("br-", dz, dh)] = ("y-", rb / 2, (("by-", dz, dh),))
    return t


def group_needs(t, dz):
    need = set()
    for dh in (0, 1):
        need |= set(t[("by+", dz, dh)][2])
        need |= {(k, dz, dh) for k in ("by+", "by-", "br+", "br-")}
    if dz == 0:
        need |= set(t[("az+", 0)][2])
    elif dz == 4:
        need |= {("az+", 3), ("az-", 3)}
    else:
        need.add(("az+", -dz - 1) if dz < 0 else ("az-", dz - 1))
    return tuple(sorted(need, key=str))


def plan(t):
    rank = {}
    for n, name in enumerate(t):
        kind = name[0]
        if kind == "h":
            r = 0 if name[1] == "a" else 2
        elif kind[0] == "a" and kind[1] in "yr":
            r = 1
        elif kind == "kv":
            r = 2
        elif kind in ("bz+", "bz-"):
            r = 3 + name[1]
        elif kind[:2] == "az":
            r = 10
        else:
            r = 4 + 4 * abs(name[1])
        rank[name] = (r, n)
    link_free = {}
    arrive = {}
    pending = sorted(t, key=lambda k: rank[k])
    order, now = [], 0.0
    computes = [("attn", s, h) for s in range(BACK + 1) for h in range(HEADS)]
    mats = [("M", dz) for dz in DZS]
    sums, finals = [], []
    done = {}
    cost = {"M": 2.0, "S": 0.6, "F": 0.3}

    def needs_of(c):
        if c[0] == "attn":
            return (("kv", c[1]),) if c[1] else ()
        if c[0] == "M":
            return group_needs(t, c[1])
        return ()

    def ready(names):
        return all(arrive.get(n, 1e9) <= now for n in names)

    def send(name, link, size):
        start = max(now, link_free.get(link, 0.0))
        link_free[link] = start + size / RATE
        arrive[name] = link_free[link] + HOP

    while pending or computes or mats or sums or finals:
        for n in list(pending):
            if ready(t[n][2]) and link_free.get(t[n][0], 0.0) - now < AHEAD:
                order.append(("send", n))
                send(n, t[n][0], t[n][1])
                pending.remove(n)
        pick = None
        if finals and arrive[("c", finals[0])] <= now and not computes:
            pick = ("F", finals.pop(0))
        elif sums and arrive[("d", sums[0])] <= now:
            pick = ("S", sums.pop(0))
        elif computes and ready(needs_of(computes[0])):
            pick = computes.pop(0)
        elif not computes and mats:
            ok = [c for c in mats if ready(needs_of(c))]
            if ok:
                pick = ok[0]
                mats.remove(pick)
        if pick:
            order.append(pick)
            now += PIECE if pick[0] == "attn" else cost[pick[0]]
            done[pick] = now
            if pick[0] == "M":
                send(("d", pick[1]), "d", 512.0 / 12)
                sums.append(pick[1])
            if pick[0] == "S":
                send(("c", pick[1]), "c", 256.0)
                finals.append(pick[1])
            continue
        later = [a for a in arrive.values() if a > now]
        later += [f - AHEAD for f in link_free.values() if f - AHEAD > now]
        assert later, "stuck"
        now = min(later) + 1e-6
    return order, now


TASKS = build_tasks()
ORDER, MODEL_US = plan(TASKS)
NAMES = list(TASKS)
NUMBER = {n: i for i, n in enumerate(NAMES)}


def kernel(
    q_hbm, k_hbm, v_hbm, cos_hbm, sin_hbm, segq_ref, segk_ref, w_hbm, res_hbm, out_ref,
    wa, wb, q, cos, sin, kbuf, vbuf, bias, vone, top, acc, att,
    dsend, drecv, keep, other, csend, crecv, res,
    send_sem, recv_sem, dsem, drsem, csem, crsem, kvs2, kvr2, hs2, hr2, local,
):
    c = lax.axis_index("ctx")
    t = lax.axis_index("tp")
    z, h, y = c // 8, (c // 4) % 2, c % 4
    core = t % 2
    chip = t // 2
    mate = chip * 2 + (1 - core)
    across = (1 - chip) * 2 + core

    def at(dz, dh, dy):
        return ((z + dz + 8) % 8) * 8 + ((h + dh) % 2) * 4 + (y + dy + 4) % 4

    def ctx_of(dz, dh, dy):
        return (at(dz, dh, dy), t)

    barrier = pltpu.get_barrier_semaphore()
    partners = [ctx_of(1, 0, 0), ctx_of(-1, 0, 0), ctx_of(0, 0, 1), ctx_of(0, 0, -1),
                ctx_of(0, 1, 0), (c, mate), (c, across)]
    for j in range(1, BACK + 1):
        partners.append(((c + j) % NC, t))
        partners.append(((c - j + NC) % NC, t))
    for d in partners:
        pl.semaphore_signal(barrier, inc=1, device_id=d, device_id_type=MESH)

    loads = {
        "wa": pltpu.make_async_copy(w_hbm.at[pl.ds(0, ROWS_A)], wa.at[c], local.at[0]),
        "wb": pltpu.make_async_copy(w_hbm.at[pl.ds(ROWS_A, ROWS_B)], wb.at[c], local.at[1]),
        "k": pltpu.make_async_copy(k_hbm, kbuf.at[0], local.at[2]),
        "v": pltpu.make_async_copy(v_hbm, vbuf.at[0], local.at[3]),
        "q": pltpu.make_async_copy(q_hbm, q, local.at[4]),
        "cos": pltpu.make_async_copy(cos_hbm, cos, local.at[5]),
        "sin": pltpu.make_async_copy(sin_hbm, sin, local.at[6]),
        "res": pltpu.make_async_copy(res_hbm, res, local.at[7]),
    }
    for k in ("k", "v", "wb", "wa", "q", "cos", "sin", "res"):
        loads[k].start()
    pl.semaphore_wait(barrier, len(partners))
    for k in ("k", "v", "wb", "wa"):
        loads[k].wait()

    half_b = ROWS_B // 2
    half_a = ROWS_A // 2

    def copies(name, incoming):
        kind = name[0]
        n = NUMBER[name]
        sems = (send_sem.at[n], recv_sem.at[n])

        def one(src, dst, dev, pair=sems):
            return pltpu.make_async_remote_copy(
                src_ref=src, dst_ref=dst, send_sem=pair[0], recv_sem=pair[1],
                device_id=dev, device_id_type=MESH)

        def same(ref, dev, pair=sems):
            return one(ref, ref, dev, pair)

        if kind == "kv":
            j = name[1]
            dev = ((c + j) % NC, t)
            return [one(kbuf.at[0], kbuf.at[j], dev),
                    one(vbuf.at[0], vbuf.at[j], dev, (kvs2.at[j - 1], kvr2.at[j - 1]))]
        if kind == "h":
            i = at(0, 1, 0) if incoming else c
            dev = ctx_of(0, 1, 0)
            return [same((wb if name[1] == "b" else wa).at[i], dev)]
        sign = 1 if kind[2] == "+" else -1
        if kind[:2] == "bz":
            s, dh = name[1], name[2]
            i = at(-sign * (s + (1 if incoming else 0)), dh, 0)
            ref = wb.at[i]
            if s == 3:
                ref = wb.at[i, pl.ds(0 if sign > 0 else half_b, half_b)]
            return [same(ref, ctx_of(sign, 0, 0))]
        if kind[:2] == "az":
            s = name[1]
            zz = ((z - sign * (s + (1 if incoming else 0)) + 8) % 8) * 8
            if s < 3:
                ref = wa.at[pl.ds(zz, 8)]
            else:
                ref = wa.at[pl.ds(zz + (0 if sign > 0 else 4), 4)]
            return [same(ref, ctx_of(sign, 0, 0))]
        if kind[0] == "a":
            dz, dh, buf, half = 0, name[1], wa, half_a
        else:
            dz, dh, buf, half = name[1], name[2], wb, half_b
        relay = kind[1] == "r"
        step = (1 if relay else 0) + (1 if incoming else 0)
        i = at(dz, dh, -sign * step)
        ref = buf.at[i]
        if relay:
            ref = buf.at[i, pl.ds(0 if sign > 0 else half, half)]
        return [same(ref, ctx_of(0, 0, sign))]

    got = set()

    def need(names):
        for name in names:
            if name not in got:
                got.add(name)
                for cp in copies(name, True):
                    cp.wait_recv()

    def send(name):
        need(TASKS[name][2])
        for cp in copies(name, False):
            cp.start()

    ready = {"attn": False}
    qk = (((1,), (1,)), ((), ()))
    scale2 = (1.0 / math.sqrt(HD)) * math.log2(math.e)

    def attn_setup(s):
        if s == 0:
            for k in ("q", "cos", "sin"):
                loads[k].wait()
            vone[:, HD:] = jnp.ones((TOK, HD), jnp.bfloat16)
        need((("kv", s),) if s else ())
        segk = segk_ref[pl.ds(BACK - s, 1), :]
        same = segq_ref[...] == segk
        if s == 0:
            row = lax.broadcasted_iota(jnp.int32, (TOK, TOK), 0)
            col = lax.broadcasted_iota(jnp.int32, (TOK, TOK), 1)
            same = same & (col <= row)
        bias[...] = jnp.where(same, 0.0, -1e30).astype(jnp.float32)
        vone[:, :HD] = vbuf[s]

    def attn_piece(s, hd):
        cols = pl.ds(pl.multiple_of(hd * HD, HD), HD)
        if s == 0:
            x = q[:, cols].astype(jnp.float32)
            x = x * cos[...] + pltpu.roll(x, HD // 2, 1) * sin[...]
            qh = x.astype(jnp.bfloat16)
            q[:, cols] = qh
        else:
            qh = q[:, cols]
        score = lax.dot_general(qh, kbuf[s], qk, preferred_element_type=jnp.float32) + bias[...]
        peak = jnp.max(score, axis=1, keepdims=True)
        if s > 0:
            old = top[hd]
            peak = jnp.maximum(peak, old)
        prob = jnp.exp2((score - peak) * scale2).astype(jnp.bfloat16)
        mixed = jnp.dot(prob, vone[...], preferred_element_type=jnp.float32)
        if s > 0:
            mixed = mixed + acc[hd] * jnp.exp2((old - peak) * scale2)
        if s < BACK:
            top[hd] = peak
            acc[hd] = mixed
        else:
            att[:, cols] = (mixed[:, :HD] / mixed[:, HD:]).astype(jnp.bfloat16)

    def group(dz):
        return (z + dz + 8) % 8

    def d_copy(n):
        return pltpu.make_async_remote_copy(
            src_ref=dsend.at[n], dst_ref=drecv.at[n], send_sem=dsem.at[n], recv_sem=drsem.at[n],
            device_id=(c, mate), device_id_type=MESH)

    def c_copy(n):
        return pltpu.make_async_remote_copy(
            src_ref=csend.at[n], dst_ref=crecv.at[n], send_sem=csem.at[n], recv_sem=crsem.at[n],
            device_id=(c, across), device_id_type=MESH)

    def rows_of(tp):
        return pl.ds(pl.multiple_of(tp * 128, 128), 128)

    across_mate = (1 - chip) * 2 + (1 - core)

    def matmul(dz):
        n = DZS.index(dz)
        need(group_needs(TASKS, dz))
        base = group(dz) * 8

        def body(j, carry):
            i = base + 2 * j
            rhs = jnp.concatenate(
                [jnp.concatenate([wa[i], wb[i]], axis=0),
                 jnp.concatenate([wa[i + 1], wb[i + 1]], axis=0)], axis=1)
            cols = pl.ds(pl.multiple_of(j * 256, 256), 256)

            def part(tp):
                return jnp.dot(att[rows_of(tp), :], rhs, preferred_element_type=jnp.float32)

            dsend[n, 0, :, cols] = part(mate).astype(jnp.bfloat16)
            dsend[n, 1, :, cols] = part(across_mate).astype(jnp.bfloat16)
            keep[n, :, cols] = part(t)
            other[n, :, cols] = part(across)
            return carry

        lax.fori_loop(0, 4, body, 0)
        d_copy(n).start()

    def summed(dz):
        n = DZS.index(dz)
        d_copy(n).wait_recv()

        def body(j, carry):
            cols = pl.ds(pl.multiple_of(j * 256, 256), 256)
            csend[n, :, cols] = (
                other[n, :, cols] + drecv[n, 1, :, cols].astype(jnp.float32)).astype(jnp.bfloat16)
            return carry

        lax.fori_loop(0, 4, body, 0)
        c_copy(n).start()

    def final(dz):
        n = DZS.index(dz)
        if n == 0:
            loads["res"].wait()
        c_copy(n).wait_recv()
        first = group(dz) * 1024

        def body(j, carry):
            cols = pl.ds(pl.multiple_of(j * 256, 256), 256)
            wide = pl.ds(pl.multiple_of(first + j * 256, 256), 256)
            total = keep[n, :, cols] + drecv[n, 0, :, cols].astype(jnp.float32)
            total = total + crecv[n, :, cols].astype(jnp.float32)
            out_ref[:, wide] = (total + res[:, wide].astype(jnp.float32)).astype(jnp.bfloat16)
            return carry

        lax.fori_loop(0, 4, body, 0)

    i = 0
    items = ORDER
    while i < len(items):
        item = items[i]
        if item[0] == "attn":
            seg = item[1]
            slots = {}
            hd = -1
            while i < len(items) and (items[i][0] == "send" or items[i][:2] == ("attn", seg)):
                if items[i][0] == "attn":
                    hd = items[i][2]
                else:
                    slots.setdefault(hd, []).append(items[i][1])
                i += 1
            attn_setup(seg)

            def body(hd, carry, seg=seg, slots=slots):
                attn_piece(seg, hd)
                for k, names in slots.items():
                    def issue(names=names):
                        for name in names:
                            send(name)
                    pl.when(hd == k)(issue)
                return carry

            lax.fori_loop(0, HEADS, body, 0)
            continue
        if item[0] == "send":
            send(item[1])
        elif item[0] == "M":
            matmul(item[1])
        elif item[0] == "S":
            summed(item[1])
        else:
            final(item[1])
        i += 1
    for name in NAMES:
        assert name in got, name
        for cp in copies(name, False):
            cp.wait_send()
    for n in range(8):
        d_copy(n).wait_send()
        c_copy(n).wait_send()


def rotary_tables(positions):
    half_dim = HD // 2
    freq_index = jnp.arange(half_dim)
    inv_freq = theta_base ** (-2.0 * freq_index.astype(jnp.float32) / HD)
    first_end = HD // 8
    second_end = first_end + 3 * HD // 16
    place = positions.astype(jnp.float32)
    chosen = jnp.where(
        freq_index[None, :] < first_end,
        place[0][:, None],
        jnp.where(freq_index[None, :] < second_end, place[1][:, None], place[2][:, None]),
    )
    angle = chosen * inv_freq[None, :]
    return (jnp.cos(angle), jnp.sin(angle))


def on_device(queries, keys, values, positions, segment_ids, out_weight, residual):
    cosine, sine = rotary_tables(positions)
    cos2 = jnp.concatenate([cosine, cosine], axis=1)
    sin2 = jnp.concatenate([-sine, sine], axis=1)
    kf = keys.astype(jnp.float32)
    swapped = jnp.concatenate([kf[:, HD // 2:], kf[:, :HD // 2]], axis=1)
    rot_k = (kf * cos2 + swapped * sin2).astype(jnp.bfloat16)
    my = lax.axis_index("ctx")
    wrapped = jnp.concatenate([segment_ids[-BACK * TOK:], segment_ids])
    window = lax.dynamic_slice_in_dim(wrapped, my * TOK, (BACK + 1) * TOK, 0)
    segk = jnp.concatenate(
        [window.reshape(BACK + 1, TOK), jnp.zeros((7 - BACK, TOK), jnp.int32)], axis=0)
    segq = window[BACK * TOK:].reshape(TOK, 1)
    anyspec = pl.BlockSpec(memory_space=pl.ANY)
    vmem = pl.BlockSpec(memory_space=pltpu.VMEM)
    nt = len(NAMES)
    bf, f32 = jnp.bfloat16, jnp.float32
    return pl.pallas_call(
        kernel,
        out_shape=jax.ShapeDtypeStruct((128, 8192), bf),
        in_specs=[anyspec] * 5 + [vmem] * 2 + [anyspec] * 2,
        out_specs=vmem,
        scratch_shapes=[
            pltpu.VMEM((NC, ROWS_A, 128), bf),
            pltpu.VMEM((NC, ROWS_B, 128), bf),
            pltpu.VMEM((TOK, 1024), bf),
            pltpu.VMEM((TOK, HD), f32),
            pltpu.VMEM((TOK, HD), f32),
            pltpu.VMEM((BACK + 1, TOK, HD), bf),
            pltpu.VMEM((BACK + 1, TOK, HD), bf),
            pltpu.VMEM((TOK, TOK), f32),
            pltpu.VMEM((TOK, 2 * HD), bf),
            pltpu.VMEM((HEADS, TOK, 1), f32),
            pltpu.VMEM((HEADS, TOK, 2 * HD), f32),
            pltpu.VMEM((TOK, 1024), bf),
            pltpu.VMEM((8, 2, 128, 1024), bf),
            pltpu.VMEM((8, 2, 128, 1024), bf),
            pltpu.VMEM((8, 128, 1024), f32),
            pltpu.VMEM((8, 128, 1024), f32),
            pltpu.VMEM((8, 128, 1024), bf),
            pltpu.VMEM((8, 128, 1024), bf),
            pltpu.VMEM((128, 8192), bf),
            pltpu.SemaphoreType.DMA((nt,)),
            pltpu.SemaphoreType.DMA((nt,)),
            pltpu.SemaphoreType.DMA((8,)),
            pltpu.SemaphoreType.DMA((8,)),
            pltpu.SemaphoreType.DMA((8,)),
            pltpu.SemaphoreType.DMA((8,)),
            pltpu.SemaphoreType.DMA((BACK,)),
            pltpu.SemaphoreType.DMA((BACK,)),
            pltpu.SemaphoreType.DMA((1,)),
            pltpu.SemaphoreType.DMA((1,)),
            pltpu.SemaphoreType.DMA((8,)),
        ],
        compiler_params=pltpu.CompilerParams(
            collective_id=0, has_side_effects=True, vmem_limit_bytes=62 * 1024 * 1024),
    )(queries, rot_k, values, cos2, sin2, segq, segk, out_weight, residual)


def solution(mesh):
    return jax.shard_map(
        on_device,
        mesh=mesh,
        in_specs=(
            P("ctx", "tp"),
            P("ctx", "tp"),
            P("ctx", "tp"),
            P(None, "ctx"),
            P(),
            P("tp", "ctx"),
            P(("ctx", "tp"), None),
        ),
        out_specs=P(("ctx", "tp"), None),
        check_vma=False,
    )
```

```python
import math

import jax
import jax.numpy as jnp
from jax import lax
from jax.experimental import pallas as pl
from jax.experimental.pallas import tpu as pltpu
from jax.sharding import PartitionSpec as P

HD = 128
HEADS = 8
TOK = 512
CHUNK = 128
BACK = 4
SPAN = (BACK + 1) * TOK
WINDOW = BACK * TOK + CHUNK
ROWS_A = 512
ROWS_B = 1024 - ROWS_A
RATE = 45.5
HOP = 1.9
STEP = 3.0
AHEAD = 6.0
BIG = 2.0**100
theta_base = 1000000.0
MESH = pl.DeviceIdType.MESH
PARTS = ((0, 1, -1, 2), (-2, 3, -3, 4))
NEAR = (0, 1, 2, -1)


def build_tasks():
    t = {}
    ra, rb = float(ROWS_A), float(ROWS_B)
    for j in range(1, BACK + 1):
        t[("kv", j)] = ("y+" if j < 3 else "x+", 256.0, (), 2.0)
    for k, rows in (("a", ra), ("b", rb)):
        t[("tg", k)] = ("x-", rows / 4, (), 1.0)
    for half in (0, 1):
        t[("ay+", half)] = ("y+", ra / 4, (("tg", "a"),), 0.0)
        t[("ay-", half)] = ("y-", ra / 4, (("tg", "a"),), 0.0)
    t[("ar+", 0)] = ("y+", ra / 4, (("ay+", 0),), 0.0)
    t[("ar-", 1)] = ("y-", ra / 4, (("ay-", 1),), 0.0)
    for p in range(4):
        for s, order in (("+", p), ("-", 3 - p)):
            t[("bs" + s, order)] = ("z" + s, rb / 4, (("tg", "b"),), 0.0)
            t[("br" + s, order)] = ("z" + s, 1.0, (("bs" + s, order),), 2 * HOP)
    column = (("tg", "a"), ("ay+", 0), ("ay+", 1), ("ay-", 0), ("ay-", 1), ("ar+", 0), ("ar-", 1))
    for s in range(4):
        size = ra if s < 3 else ra / 2
        t[("az+", s)] = ("z+", size, column if s == 0 else (("az+", s - 1),), 0.0)
        t[("az-", s)] = ("z-", size, column if s == 0 else (("az-", s - 1),), 0.0)
    for slot in "NF":
        for half in (0, 1):
            pieces = (2 * half, 2 * half + 1)
            kind = "bs" if slot == "N" else "br"
            need = (("tg", "b"),) + tuple((kind + s, p) for s in "+-" for p in pieces)
            t[("by+", slot, half)] = ("y+", rb / 2, need, 0.0)
            t[("by-", slot, half)] = ("y-", rb / 2, need, 0.0)
        t[("bq+", slot, 0)] = ("y+", rb / 2, (("by+", slot, 0),), 0.0)
        t[("bq-", slot, 1)] = ("y-", rb / 2, (("by-", slot, 1),), 0.0)
    for m in range(4):
        for s in "+-":
            t[("at" + s, m)] = ("x" + s, 256.0, (("att", m),), 0.0)
            t[("ar2" + s, m)] = ("x" + s, 128.0, (("at" + s, m),), 0.0)
        t[("am", m, "own")] = ("d", 256.0 / 12, (("att", m),), 0.0)
        for s in "+-":
            t[("am", m, s)] = ("d", 256.0 / 12, (("at" + s, m),), 0.0)
            t[("am", m, s + "2")] = ("d", 128.0 / 12, (("ar2" + s, m),), 0.0)
    return t


def b_names(slots):
    out = []
    for slot in slots:
        for half in (0, 1):
            out += [("by+", slot, half), ("by-", slot, half)]
        out += [("bq+", slot, 0), ("bq-", slot, 1)]
    return out


def mat_needs(m, part):
    need = [("am", m, k) for k in ("own", "+", "-", "+2", "-2")]
    need += [("at+", m), ("at-", m), ("ar2+", m), ("ar2-", m)]
    need += b_names("N" if part == 0 else "NF")
    deep = 2 if part == 0 else 4
    for s in range(deep):
        need += [("az+", s), ("az-", s)]
    return tuple(need)


def plan(t):
    rank = {}
    for n, name in enumerate(t):
        k = name[0]
        if k == "kv":
            r = 1
        elif k == "tg":
            r = 0
        elif k in ("ay+", "ay-", "ar+", "ar-"):
            r = 2
        elif k in ("bs+", "bs-", "br+", "br-"):
            r = 3
        elif k in ("az+", "az-"):
            r = 6
        elif k in ("at+", "at-"):
            r = 4
        elif k in ("ar2+", "ar2-"):
            r = 3
        elif k == "am":
            r = 4
        else:
            r = 5 if name[1] == "N" else 7
        rank[name] = (r, n)
    link_free, arrive = {}, {}
    pending = sorted(t, key=lambda k: rank[k])
    order, now = [], 0.0
    steps = [(m, g) for m in range(4) for g in range(2)]
    mats = [(m, part) for part in range(2) for m in range(4)]
    finals = []
    sent = {0: [], 1: []}

    def ready(names):
        return all(arrive.get(n, 1e9) <= now for n in names)

    def send(name, link, size, extra):
        start = max(now, link_free.get(link, 0.0))
        link_free[link] = start + size / RATE
        arrive[name] = link_free[link] + HOP + extra

    while pending or steps or mats or finals:
        for n in list(pending):
            if ready(t[n][2]) and link_free.get(t[n][0], 0.0) - now < AHEAD:
                order.append(("send", n))
                send(n, *[t[n][i] for i in (0, 1, 3)])
                pending.remove(n)
        if steps:
            if ready([("kv", j) for j in range(1, BACK + 1)]):
                m, g = steps.pop(0)
                order.append(("step", m, g))
                now += STEP
                if g == 1:
                    arrive[("att", m)] = now
                continue
        elif mats:
            ok = [c for c in mats if ready(mat_needs(*c))]
            if ok:
                m, part = ok[0]
                mats.remove(ok[0])
                order.append(("M", m, part))
                now += 1.5
                send(("c", m, part), "x+", 140.0, 1.0)
                sent[part].append(("c", m, part))
                if len(sent[part]) == 4:
                    finals.append(part)
                continue
        if finals and not steps and ready(sent[finals[0]]):
            order.append(("F", finals.pop(0)))
            now += 1.0
            continue
        later = [a for a in arrive.values() if a > now]
        later += [f - AHEAD for f in link_free.values() if f - AHEAD > now]
        assert later, "stuck"
        now = min(later) + 1e-6
    return order, now, arrive


TASKS = build_tasks()
ORDER, MODEL_US, ARRIVE = plan(TASKS)
NAMES = list(TASKS)
NUMBER = {n: i for i, n in enumerate(NAMES)}


def kernel(
    q_hbm, k_hbm, v_hbm, cos_hbm, sin_hbm, hot_hbm, w_hbm, res_hbm, out_ref,
    wa, wb, q, cos, sin, kbuf, vbuf, hot, att, csend, crecv, res,
    send_sem, recv_sem, kv_send, kv_recv, tg_recv, c_send, c_recv, local,
):
    c = lax.axis_index("ctx")
    t = lax.axis_index("tp")
    z, h, y = c // 8, (c // 4) % 2, c % 4
    core = t % 2
    chip = t // 2
    x = h * 2 + chip
    owner = (z + y) % 4
    r = (t - z - y + 16) % 4
    me = h * 4 + t

    def ctx_of(dz, dh, dy):
        return (((z + dz + 8) % 8) * 8 + ((h + dh) % 2) * 4 + (y + dy + 4) % 4, t)

    def ring(d):
        other = (x + d + 4) % 4
        return (z * 8 + (other // 2) * 4 + y, (other % 2) * 2 + core)

    mate = (c, chip * 2 + (1 - core))
    barrier = pltpu.get_barrier_semaphore()
    partners = [ctx_of(1, 0, 0), ctx_of(-1, 0, 0), ctx_of(0, 0, 1), ctx_of(0, 0, -1)]
    for d in range(4):
        for k in range(2):
            other = (x + d) % 4
            who = (z * 8 + (other // 2) * 4 + y, (other % 2) * 2 + (core + k) % 2)
            if d or k:
                partners.append(who)
    for j in range(1, BACK + 1):
        partners.append(((c + j) % 64, t))
        partners.append(((c - j + 64) % 64, t))
    for d in partners:
        pl.semaphore_signal(barrier, inc=1, device_id=d, device_id_type=MESH)

    own = pl.ds(BACK * TOK, TOK)
    loads = {
        "k": pltpu.make_async_copy(k_hbm, kbuf.at[own], local.at[0]),
        "v": pltpu.make_async_copy(v_hbm, vbuf.at[own], local.at[1]),
        "q": pltpu.make_async_copy(q_hbm, q, local.at[2]),
        "cos": pltpu.make_async_copy(cos_hbm, cos, local.at[3]),
        "sin": pltpu.make_async_copy(sin_hbm, sin, local.at[4]),
        "hot": pltpu.make_async_copy(hot_hbm, hot, local.at[5]),
        "res": pltpu.make_async_copy(res_hbm, res, local.at[6]),
    }
    for cp in loads.values():
        cp.start()
    w_rows = {"a": pl.ds(0, ROWS_A), "b": pl.ds(ROWS_A, ROWS_B)}
    w_buf = {"a": wa, "b": wb}
    w_local = {
        k: pltpu.make_async_copy(w_hbm.at[w_rows[k]], w_buf[k].at[z, t], local.at[7 + i])
        for i, k in enumerate("ab")
    }

    @pl.when(owner == t)
    def _():
        for k in "ab":
            w_local[k].start()

    with jax.named_scope("barrier"):
        pl.semaphore_wait(barrier, len(partners))
    with jax.named_scope("kvload"):
        loads["k"].wait()
        loads["v"].wait()

    def slot(which, dy):
        rr = (r - dy + 8) % 4
        near = jnp.where(rr == 3, -1, rr)
        return (z + near + (8 if which == "N" else 12)) % 8

    def halves(half):
        return pl.ds(2 * half, 2)

    def copies(name, incoming):
        kind = name[0]
        n = NUMBER.get(name)

        def one(src, dst, dev, ss=None, rs=None):
            return pltpu.make_async_remote_copy(
                src_ref=src, dst_ref=dst,
                send_sem=send_sem.at[n] if ss is None else ss,
                recv_sem=recv_sem.at[n] if rs is None else rs,
                device_id=dev, device_id_type=MESH)

        def same(ref, dev, **k):
            return one(ref, ref, dev, **k)

        if kind == "kv":
            j = name[1]
            dev = ((c + j) % 64, t)
            to = pl.ds((BACK - j) * TOK, TOK)
            return [(None, one(kbuf.at[own], kbuf.at[to], dev)),
                    (None, one(vbuf.at[own], vbuf.at[to], dev, kv_send.at[j - 1], kv_recv.at[j - 1]))]
        if kind == "tg":
            k = name[1]
            i = "ab".index(k)
            if not incoming:
                return [(owner != t, one(w_hbm.at[w_rows[k]], w_buf[k].at[z, t], (c, owner),
                                         rs=tg_recv.at[i, t]))]
            return [((r == 0) & (t != u),
                     same(w_buf[k].at[z, u], (c, owner), rs=tg_recv.at[i, u])) for u in range(4)]
        if kind in ("at+", "at-", "ar2+", "ar2-", "am"):
            m = name[1]
            rows = pl.ds(m * CHUNK, CHUNK)
            if kind == "am":
                k = name[2]
                d = {"own": 0, "+": -1, "-": 1, "+2": 2, "-2": 2}[k]
                from_core = (1 - core) if incoming else core
                if k == "+2":
                    rows = pl.ds(m * CHUNK, CHUNK // 2)
                if k == "-2":
                    rows = pl.ds(m * CHUNK + CHUNK // 2, CHUNK // 2)
                i = ((x + d + 4) % 4) * 2 + from_core
                return [(None, same(att.at[i, rows], mate))]
            sign = 1 if kind[-1] == "+" else -1
            d = -sign * ((1 if kind[:3] == "ar2" else 0) + (1 if incoming else 0))
            if kind[:3] == "ar2":
                rows = pl.ds(m * CHUNK + (0 if sign > 0 else CHUNK // 2), CHUNK // 2)
            i = ((x + d + 4) % 4) * 2 + core
            return [(None, same(att.at[i, rows], ring(sign)))]
        sign = 1 if kind[2] == "+" else -1
        if kind[:2] in ("ay", "ar"):
            half = name[1]
            ref = wa.at[z, halves(half)]
            if kind[:2] == "ay":
                cond = (r == (3 if sign > 0 else 1)) if incoming else (r == 0)
            else:
                cond = (r == 2) if incoming else (r == (3 if sign > 0 else 1))
            return [(cond, same(ref, ctx_of(0, 0, sign)))]
        if kind[:2] == "az":
            s = name[1]
            zz = (z - sign * (s + (1 if incoming else 0)) + 8) % 8
            ref = wa.at[zz] if s < 3 else wa.at[zz, halves(0 if sign > 0 else 1)]
            return [(None, same(ref, ctx_of(sign, 0, 0)))]
        if kind[:2] in ("bs", "br", "bz"):
            p = name[1]
            far = (4 - r) % 4 if sign > 0 else r
            n = NUMBER[("bs" + kind[2], p)]
            carried = p < 2 if sign > 0 else p >= 2
            last = 1 if sign > 0 else 3
            if not incoming:
                zs = (z - sign * far + 8) % 8
                if kind[:2] == "bs":
                    cond = r == 0
                else:
                    cond = (r != 0) if carried else ((r != 0) & (r != last))
                return [(cond, same(wb.at[zs, p], ctx_of(sign, 0, 0)))]
            zs = (z - sign * ((far + 3) % 4 + 1) + 16) % 8
            cp = same(wb.at[zs, p], ctx_of(sign, 0, 0))
            near = (r == 3) if sign > 0 else ((r == 1) | (r == 2))
            if kind[:2] == "bs":
                return [(near, cp)]
            far_end = (r != 0) & jnp.logical_not(near)
            return [(far_end if kind[:2] == "br" else r == 0, cp)]
        which, half = name[1], name[2]
        step = (1 if kind[:2] == "bq" else 0) + (1 if incoming else 0)
        zs = slot(which, -sign * step)
        return [(None, same(wb.at[zs, halves(half)], ctx_of(0, 0, sign)))]

    def under(cond, act):
        if cond is None:
            act()
        else:
            pl.when(cond)(act)

    got = set()

    def need(names):
        for name in names:
            if name not in got and name[0] != "att":
                got.add(name)
                if name[0] == "tg":
                    @pl.when(owner == t)
                    def _(name=name):
                        w_local[name[1]].wait()
                for cond, cp in copies(name, True):
                    under(cond, cp.wait_recv)

    def send(name):
        need(TASKS[name][2])
        if name[0] in ("br+", "br-"):
            need([name])
        if name[0] in ("by+", "by-") and name[1] == "F":
            need([("bz+", p) for p in (0, 1)] if name[2] == 0 else [("bz-", p) for p in (2, 3)])
        for cond, cp in copies(name, False):
            under(cond, cp.start)

    scale2 = (1.0 / math.sqrt(HD)) * math.log2(math.e)

    def rotate_queries():
        for k in ("q", "cos", "sin", "hot"):
            loads[k].wait()

        def body(hd, carry):
            cols = pl.ds(pl.multiple_of(hd * HD, HD), HD)
            v = q[:, cols].astype(jnp.float32)
            v = v * cos[...] + pltpu.roll(v, HD // 2, 1) * sin[...]
            q[:, cols] = v.astype(jnp.bfloat16)
            return carry

        lax.fori_loop(0, HEADS, body, 0)

    def attend(m, g):
        rows = pl.ds(pl.multiple_of(m * CHUNK, CHUNK), CHUNK)
        keys = pl.ds(pl.multiple_of(m * CHUNK, CHUNK), WINDOW)
        mine = hot[pl.ds(pl.multiple_of(BACK * TOK + m * CHUNK, CHUNK), CHUNK), :]
        heads = []
        for i in range(4):
            qh = q[rows, pl.ds(pl.multiple_of((g * 4 + i) * HD, HD), HD)]
            heads.append(jnp.concatenate([qh, mine], axis=1))
        qs = jnp.concatenate(heads, axis=0)
        other = ((hot[keys, :].astype(jnp.float32) - 1.0) * BIG).astype(jnp.bfloat16)
        ks = jnp.concatenate([kbuf[keys, :], other], axis=1)
        score = lax.dot_general(
            qs, ks, (((1,), (1,)), ((), ())), preferred_element_type=jnp.float32)
        row = lax.broadcasted_iota(jnp.int32, (4 * CHUNK, CHUNK), 0) % CHUNK
        col = lax.broadcasted_iota(jnp.int32, (4 * CHUNK, CHUNK), 1)
        edge = jnp.where(col <= row, score[:, WINDOW - CHUNK:], -BIG)
        score = jnp.concatenate([score[:, :WINDOW - CHUNK], edge], axis=1)
        peak = jnp.max(score, axis=1, keepdims=True)
        prob = jnp.exp2((score - peak) * scale2).astype(jnp.bfloat16)
        vs = jnp.concatenate([vbuf[keys, :], jnp.ones((WINDOW, HD), jnp.bfloat16)], axis=1)
        mixed = jnp.dot(prob, vs, preferred_element_type=jnp.float32)
        result = (mixed[:, :HD] / mixed[:, HD:]).astype(jnp.bfloat16)
        for i in range(4):
            att[me, rows, pl.ds(pl.multiple_of((g * 4 + i) * HD, HD), HD)] = (
                result[i * CHUNK:(i + 1) * CHUNK])

    def c_copy(m, hh, part):
        return pltpu.make_async_remote_copy(
            src_ref=csend.at[m, hh, part], dst_ref=crecv.at[me, part],
            send_sem=c_send.at[m, hh, part], recv_sem=c_recv.at[me, part],
            device_id=(z * 8 + hh * 4 + y, m), device_id_type=MESH)

    def matmul(m, part):
        need(mat_needs(m, part))
        rows = pl.ds(m * CHUNK, CHUNK)
        for pair in range(2):
            total = None
            z0, z1 = [(z + PARTS[part][2 * pair + i] + 8) % 8 for i in range(2)]
            for u in range(4):
                lhs = jnp.concatenate([att[u, rows, :], att[4 + u, rows, :]], axis=0)
                rhs = jnp.concatenate(
                    [jnp.concatenate([wa[z0, u], wb[z0, u]], axis=0),
                     jnp.concatenate([wa[z1, u], wb[z1, u]], axis=0)], axis=1)
                one = jnp.dot(lhs, rhs, preferred_element_type=jnp.float32)
                total = one if total is None else total + one
            total = total.astype(jnp.bfloat16)
            cols = pl.ds(pair * 256, 256)
            for hh in range(2):
                csend[m, hh, part, :, cols] = total[hh * CHUNK:(hh + 1) * CHUNK]
        for hh in range(2):
            mine = (h == hh) & (t == m)

            @pl.when(mine)
            def _(hh=hh):
                crecv[me, part] = csend[m, hh, part]

            pl.when(jnp.logical_not(mine))(c_copy(m, hh, part).start)

    def final(part):
        if part == 0:
            loads["res"].wait()

        def body(s, carry):
            hs, ts = s // 4, s % 4
            cp = pltpu.make_async_remote_copy(
                src_ref=csend.at[0, 0, part], dst_ref=crecv.at[s, part],
                send_sem=c_send.at[0, 0, part], recv_sem=c_recv.at[s, part],
                device_id=mate, device_id_type=MESH)
            pl.when(s != me)(cp.wait_recv)
            for i, dz in enumerate(PARTS[part]):
                zs = (z + dz + 8) % 8
                col = (zs * 8 + hs * 4 + (ts - zs + 8) % 4) * HD
                wide = pl.ds(pl.multiple_of(col, HD), HD)
                got_c = crecv[s, part, :, i * HD:(i + 1) * HD].astype(jnp.float32)
                out_ref[:, wide] = (got_c + res[:, wide].astype(jnp.float32)).astype(jnp.bfloat16)
            return carry

        lax.fori_loop(0, 8, body, 0)

    items = list(ORDER)
    first = next(i for i, it in enumerate(items) if it[0] == "step")
    last = max(i for i, it in enumerate(items) if it[0] == "step")
    rotated = False
    for it in items[:first]:
        if not rotated and it[1][0] not in ("tg", "kv"):
            rotated = True
            with jax.named_scope("rotq"):
                rotate_queries()
        with jax.named_scope("s_" + "_".join(map(str, it[1])).replace("+", "p").replace("-", "m")):
            send(it[1])
    need([("kv", j) for j in range(1, BACK + 1)])
    slots, at_step = {}, -1
    for it in items[first:last + 1]:
        if it[0] == "step":
            at_step += 1
        else:
            slots.setdefault(at_step, []).append(it[1])

    def step(i, carry):
        with jax.named_scope("attend"):
            attend(i // 2, i % 2)
        for k, names in slots.items():
            def issue(names=names):
                for name in names:
                    send(name)
            pl.when(i == k)(issue)
        return carry

    lax.fori_loop(0, 8, step, 0)
    for it in items[last + 1:]:
        if it[0] == "send":
            with jax.named_scope("s_" + "_".join(map(str, it[1])).replace("+", "p").replace("-", "m")):
                send(it[1])
        elif it[0] == "M":
            with jax.named_scope("M%d%d" % it[1:]):
                matmul(*it[1:])
        else:
            with jax.named_scope("F%d" % it[1]):
                final(it[1])
    for name in NAMES:
        need([name])
        for cond, cp in copies(name, False):
            under(cond, cp.wait_send)
    for m in range(4):
        for hh in range(2):
            for part in range(2):
                pl.when(jnp.logical_not((h == hh) & (t == m)))(c_copy(m, hh, part).wait_send)


def rotary_tables(positions):
    half_dim = HD // 2
    freq_index = jnp.arange(half_dim)
    inv_freq = theta_base ** (-2.0 * freq_index.astype(jnp.float32) / HD)
    first_end = HD // 8
    second_end = first_end + 3 * HD // 16
    place = positions.astype(jnp.float32)
    chosen = jnp.where(
        freq_index[None, :] < first_end,
        place[0][:, None],
        jnp.where(freq_index[None, :] < second_end, place[1][:, None], place[2][:, None]),
    )
    angle = chosen * inv_freq[None, :]
    return (jnp.cos(angle), jnp.sin(angle))


def on_device(queries, keys, values, positions, segment_ids, out_weight, residual):
    cosine, sine = rotary_tables(positions)
    cos2 = jnp.concatenate([cosine, cosine], axis=1)
    sin2 = jnp.concatenate([-sine, sine], axis=1)
    kf = keys.astype(jnp.float32)
    swapped = jnp.concatenate([kf[:, HD // 2:], kf[:, :HD // 2]], axis=1)
    rot_k = (kf * cos2 + swapped * sin2).astype(jnp.bfloat16)
    my = lax.axis_index("ctx")
    wrapped = jnp.concatenate([segment_ids[-BACK * TOK:], segment_ids])
    window = lax.dynamic_slice_in_dim(wrapped, my * TOK, SPAN, 0)
    hot = (window[:, None] == jnp.arange(HD, dtype=jnp.int32)[None, :]).astype(jnp.bfloat16)
    anyspec = pl.BlockSpec(memory_space=pl.ANY)
    nt = len(NAMES)
    bf, f32 = jnp.bfloat16, jnp.float32
    dma = pltpu.SemaphoreType.DMA
    return pl.pallas_call(
        kernel,
        out_shape=jax.ShapeDtypeStruct((CHUNK, 8192), bf),
        in_specs=[anyspec] * 8,
        out_specs=pl.BlockSpec(memory_space=pltpu.VMEM),
        scratch_shapes=[
            pltpu.VMEM((8, 4, ROWS_A, HD), bf),
            pltpu.VMEM((8, 4, ROWS_B, HD), bf),
            pltpu.VMEM((TOK, 1024), bf),
            pltpu.VMEM((TOK, HD), f32),
            pltpu.VMEM((TOK, HD), f32),
            pltpu.VMEM((SPAN, HD), bf),
            pltpu.VMEM((SPAN, HD), bf),
            pltpu.VMEM((SPAN, HD), bf),
            pltpu.VMEM((8, TOK, 1024), bf),
            pltpu.VMEM((4, 2, 2, CHUNK, 512), bf),
            pltpu.VMEM((8, 2, CHUNK, 512), bf),
            pltpu.VMEM((CHUNK, 8192), bf),
            dma((nt,)),
            dma((nt,)),
            dma((BACK,)),
            dma((BACK,)),
            dma((2, 4)),
            dma((4, 2, 2)),
            dma((8, 2)),
            dma((9,)),
        ],
        compiler_params=pltpu.CompilerParams(
            collective_id=0, has_side_effects=True, vmem_limit_bytes=62 * 1024 * 1024),
    )(queries, rot_k, values, cos2, sin2, hot, out_weight, residual)


def solution(mesh):
    return jax.shard_map(
        on_device,
        mesh=mesh,
        in_specs=(
            P("ctx", "tp"),
            P("ctx", "tp"),
            P("ctx", "tp"),
            P(None, "ctx"),
            P(),
            P("tp", "ctx"),
            P(("ctx", "tp"), None),
        ),
        out_specs=P(("ctx", "tp"), None),
        check_vma=False,
    )
```

```python
import math

import jax
import jax.numpy as jnp
from jax import lax
from jax.experimental import pallas as pl
from jax.experimental.pallas import tpu as pltpu
from jax.sharding import PartitionSpec as P

HD = 128
HEADS = 8
TOK = 512
CHUNK = 128
BACK = 4
SPAN = (BACK + 1) * TOK
WINDOW = BACK * TOK + CHUNK
ROWS_A = 512
ROWS_B = 1024 - ROWS_A
RATE = 45.5
HOP = 1.9
STEP = 3.0
AHEAD = 6.0
BIG = 2.0**100
theta_base = 1000000.0
MESH = pl.DeviceIdType.MESH
PARTS = ((0, 1, -1, 2), (-2, 3, -3, 4))
NEAR = (0, 1, 2, -1)


def build_tasks():
    t = {}
    ra, rb = float(ROWS_A), float(ROWS_B)
    for j in range(1, BACK + 1):
        t[("kv", j)] = ("y+" if j < 3 else "x+", 256.0, (), 2.0)
    for k, rows in (("a", ra), ("b", rb)):
        t[("tg", k)] = ("x-", rows / 4, (), 1.0)
    for half in (0, 1):
        t[("ay+", half)] = ("y+", ra / 4, (("tg", "a"),), 0.0)
        t[("ay-", half)] = ("y-", ra / 4, (("tg", "a"),), 0.0)
    t[("ar+", 0)] = ("y+", ra / 4, (("ay+", 0),), 0.0)
    t[("ar-", 1)] = ("y-", ra / 4, (("ay-", 1),), 0.0)
    for p in range(4):
        for s, order in (("+", p), ("-", 3 - p)):
            t[("bs" + s, order)] = ("z" + s, rb / 4, (("tg", "b"),), 0.0)
    for hop in (1, 2, 3):
        for k in range(4 if hop < 3 else 2):
            before = (("bs+", k), ("bs-", 3 - k)) if hop == 1 else (("b", hop - 1, k),)
            t[("b", hop, k)] = ("z+", 1.0, before, rb / 4 / RATE)
    column = (("tg", "a"), ("ay+", 0), ("ay+", 1), ("ay-", 0), ("ay-", 1), ("ar+", 0), ("ar-", 1))
    for s in range(4):
        size = ra if s < 3 else ra / 2
        t[("az+", s)] = ("z+", size, column if s == 0 else (("az+", s - 1),), 0.0)
        t[("az-", s)] = ("z-", size, column if s == 0 else (("az-", s - 1),), 0.0)
    for slot in "NF":
        for half in (0, 1):
            need = (("tg", "b"),) + tuple(("b", 1 if slot == "N" else 2, k) for k in range(4))
            if slot == "F":
                need = need + (("b", 3, 0), ("b", 3, 1))
            t[("by+", slot, half)] = ("y+", rb / 2, need, 0.0)
            t[("by-", slot, half)] = ("y-", rb / 2, need, 0.0)
        t[("bq+", slot, 0)] = ("y+", rb / 2, (("by+", slot, 0),), 0.0)
        t[("bq-", slot, 1)] = ("y-", rb / 2, (("by-", slot, 1),), 0.0)
    for m in range(4):
        for s in "+-":
            t[("at" + s, m)] = ("x" + s, 256.0, (("att", m),), 0.0)
            t[("ar2" + s, m)] = ("x" + s, 128.0, (("at" + s, m),), 0.0)
        t[("am", m, "own")] = ("d", 256.0 / 12, (("att", m),), 0.0)
        for s in "+-":
            t[("am", m, s)] = ("d", 256.0 / 12, (("at" + s, m),), 0.0)
            t[("am", m, s + "2")] = ("d", 128.0 / 12, (("ar2" + s, m),), 0.0)
    return t


def b_names(slots):
    out = []
    for slot in slots:
        for half in (0, 1):
            out += [("by+", slot, half), ("by-", slot, half)]
        out += [("bq+", slot, 0), ("bq-", slot, 1)]
    return out


def mat_needs(m, part):
    need = [("am", m, k) for k in ("own", "+", "-", "+2", "-2")]
    need += [("at+", m), ("at-", m), ("ar2+", m), ("ar2-", m)]
    need += b_names("N" if part == 0 else "NF")
    deep = 2 if part == 0 else 4
    for s in range(deep):
        need += [("az+", s), ("az-", s)]
    return tuple(need)


def plan(t):
    rank = {}
    for n, name in enumerate(t):
        k = name[0]
        if k == "kv":
            r = 1
        elif k == "tg":
            r = 0
        elif k in ("ay+", "ay-", "ar+", "ar-"):
            r = 2
        elif k in ("bs+", "bs-", "b"):
            r = 3
        elif k in ("az+", "az-"):
            r = 6
        elif k in ("at+", "at-"):
            r = 4
        elif k in ("ar2+", "ar2-"):
            r = 3
        elif k == "am":
            r = 4
        else:
            r = 5 if name[1] == "N" else 7
        rank[name] = (r, n)
    link_free, arrive = {}, {}
    pending = sorted(t, key=lambda k: rank[k])
    order, now = [], 0.0
    steps = [(m, g) for m in range(4) for g in range(2)]
    mats = [(m, part) for part in range(2) for m in range(4)]
    finals = []
    sent = {0: [], 1: []}

    def ready(names):
        return all(arrive.get(n, 1e9) <= now for n in names)

    def send(name, link, size, extra):
        start = max(now, link_free.get(link, 0.0))
        link_free[link] = start + size / RATE
        arrive[name] = link_free[link] + HOP + extra

    while pending or steps or mats or finals:
        for n in list(pending):
            if ready(t[n][2]) and link_free.get(t[n][0], 0.0) - now < AHEAD:
                order.append(("send", n))
                send(n, *[t[n][i] for i in (0, 1, 3)])
                pending.remove(n)
        if steps:
            if ready([("kv", j) for j in range(1, BACK + 1)]):
                m, g = steps.pop(0)
                order.append(("step", m, g))
                now += STEP
                if g == 1:
                    arrive[("att", m)] = now
                continue
        elif mats:
            ok = [c for c in mats if ready(mat_needs(*c))]
            if ok:
                m, part = ok[0]
                mats.remove(ok[0])
                order.append(("M", m, part))
                now += 1.5
                send(("c", m, part), "x+", 140.0, 1.0)
                sent[part].append(("c", m, part))
                if len(sent[part]) == 4:
                    finals.append(part)
                continue
        if finals and not steps and ready(sent[finals[0]]):
            order.append(("F", finals.pop(0)))
            now += 1.0
            continue
        later = [a for a in arrive.values() if a > now]
        later += [f - AHEAD for f in link_free.values() if f - AHEAD > now]
        assert later, "stuck"
        now = min(later) + 1e-6
    return order, now, arrive


TASKS = build_tasks()
ORDER, MODEL_US, ARRIVE = plan(TASKS)
NAMES = list(TASKS)
NUMBER = {n: i for i, n in enumerate(NAMES)}


def kernel(
    q_hbm, k_hbm, v_hbm, cos_hbm, sin_hbm, hot_hbm, w_hbm, res_hbm, out_ref,
    wa, wb, q, cos, sin, kbuf, vbuf, hot, att, csend, crecv, res,
    send_sem, recv_sem, kv_send, kv_recv, tg_recv, c_send, c_recv, local,
):
    c = lax.axis_index("ctx")
    t = lax.axis_index("tp")
    z, h, y = c // 8, (c // 4) % 2, c % 4
    core = t % 2
    chip = t // 2
    x = h * 2 + chip
    owner = (z + y) % 4
    r = (t - z - y + 16) % 4
    me = h * 4 + t

    def ctx_of(dz, dh, dy):
        return (((z + dz + 8) % 8) * 8 + ((h + dh) % 2) * 4 + (y + dy + 4) % 4, t)

    def ring(d):
        other = (x + d + 4) % 4
        return (z * 8 + (other // 2) * 4 + y, (other % 2) * 2 + core)

    mate = (c, chip * 2 + (1 - core))
    barrier = pltpu.get_barrier_semaphore()
    partners = [ctx_of(1, 0, 0), ctx_of(-1, 0, 0), ctx_of(0, 0, 1), ctx_of(0, 0, -1)]
    for d in range(4):
        for k in range(2):
            other = (x + d) % 4
            who = (z * 8 + (other // 2) * 4 + y, (other % 2) * 2 + (core + k) % 2)
            if d or k:
                partners.append(who)
    for j in range(1, BACK + 1):
        partners.append(((c + j) % 64, t))
        partners.append(((c - j + 64) % 64, t))
    for d in partners:
        pl.semaphore_signal(barrier, inc=1, device_id=d, device_id_type=MESH)

    own = pl.ds(BACK * TOK, TOK)
    loads = {
        "k": pltpu.make_async_copy(k_hbm, kbuf.at[own], local.at[0]),
        "v": pltpu.make_async_copy(v_hbm, vbuf.at[own], local.at[1]),
        "q": pltpu.make_async_copy(q_hbm, q, local.at[2]),
        "cos": pltpu.make_async_copy(cos_hbm, cos, local.at[3]),
        "sin": pltpu.make_async_copy(sin_hbm, sin, local.at[4]),
        "hot": pltpu.make_async_copy(hot_hbm, hot, local.at[5]),
        "res": pltpu.make_async_copy(res_hbm, res, local.at[6]),
    }
    for cp in loads.values():
        cp.start()
    w_rows = {"a": pl.ds(0, ROWS_A), "b": pl.ds(ROWS_A, ROWS_B)}
    w_buf = {"a": wa, "b": wb}
    w_local = {
        k: pltpu.make_async_copy(w_hbm.at[w_rows[k]], w_buf[k].at[z, t], local.at[7 + i])
        for i, k in enumerate("ab")
    }

    @pl.when(owner == t)
    def _():
        for k in "ab":
            w_local[k].start()

    with jax.named_scope("barrier"):
        pl.semaphore_wait(barrier, len(partners))
    with jax.named_scope("kvload"):
        loads["k"].wait()
        loads["v"].wait()

    def slot(which, dy):
        rr = (r - dy + 8) % 4
        near = jnp.where(rr == 3, -1, rr)
        return (z + near + (8 if which == "N" else 12)) % 8

    def halves(half):
        return pl.ds(2 * half, 2)

    def copies(name, incoming):
        kind = name[0]
        n = NUMBER.get(name)

        def one(src, dst, dev, ss=None, rs=None):
            return pltpu.make_async_remote_copy(
                src_ref=src, dst_ref=dst,
                send_sem=send_sem.at[n] if ss is None else ss,
                recv_sem=recv_sem.at[n] if rs is None else rs,
                device_id=dev, device_id_type=MESH)

        def same(ref, dev, **k):
            return one(ref, ref, dev, **k)

        if kind == "kv":
            j = name[1]
            dev = ((c + j) % 64, t)
            to = pl.ds((BACK - j) * TOK, TOK)
            return [(None, one(kbuf.at[own], kbuf.at[to], dev)),
                    (None, one(vbuf.at[own], vbuf.at[to], dev, kv_send.at[j - 1], kv_recv.at[j - 1]))]
        if kind == "tg":
            k = name[1]
            i = "ab".index(k)
            if not incoming:
                return [(owner != t, one(w_hbm.at[w_rows[k]], w_buf[k].at[z, t], (c, owner),
                                         rs=tg_recv.at[i, t]))]
            return [((r == 0) & (t != u),
                     same(w_buf[k].at[z, u], (c, owner), rs=tg_recv.at[i, u])) for u in range(4)]
        if kind in ("at+", "at-", "ar2+", "ar2-", "am"):
            m = name[1]
            rows = pl.ds(m * CHUNK, CHUNK)
            if kind == "am":
                k = name[2]
                d = {"own": 0, "+": -1, "-": 1, "+2": 2, "-2": 2}[k]
                from_core = (1 - core) if incoming else core
                if k == "+2":
                    rows = pl.ds(m * CHUNK, CHUNK // 2)
                if k == "-2":
                    rows = pl.ds(m * CHUNK + CHUNK // 2, CHUNK // 2)
                i = ((x + d + 4) % 4) * 2 + from_core
                return [(None, same(att.at[i, rows], mate))]
            sign = 1 if kind[-1] == "+" else -1
            d = -sign * ((1 if kind[:3] == "ar2" else 0) + (1 if incoming else 0))
            if kind[:3] == "ar2":
                rows = pl.ds(m * CHUNK + (0 if sign > 0 else CHUNK // 2), CHUNK // 2)
            i = ((x + d + 4) % 4) * 2 + core
            return [(None, same(att.at[i, rows], ring(sign)))]
        if kind == "b":
            hop, k = name[1], name[2]
            out = []
            for sign, p in ((1, k), (-1, 3 - k)):
                at_r = (4 - hop) % 4 if sign > 0 else hop % 4
                n = NUMBER[("bs+" if sign > 0 else "bs-", p)]
                ref = wb.at[(z - sign * hop + 8) % 8, p]
                out.append((r == at_r, same(ref, ctx_of(sign, 0, 0))))
            return out
        sign = 1 if kind[2] == "+" else -1
        if kind[:2] in ("ay", "ar"):
            half = name[1]
            ref = wa.at[z, halves(half)]
            if kind[:2] == "ay":
                cond = (r == (3 if sign > 0 else 1)) if incoming else (r == 0)
            else:
                cond = (r == 2) if incoming else (r == (3 if sign > 0 else 1))
            return [(cond, same(ref, ctx_of(0, 0, sign)))]
        if kind[:2] == "az":
            s = name[1]
            zz = (z - sign * (s + (1 if incoming else 0)) + 8) % 8
            ref = wa.at[zz] if s < 3 else wa.at[zz, halves(0 if sign > 0 else 1)]
            return [(None, same(ref, ctx_of(sign, 0, 0)))]
        if kind in ("bs+", "bs-"):
            return [] if incoming else [(r == 0, same(wb.at[z, name[1]], ctx_of(sign, 0, 0)))]
        which, half = name[1], name[2]
        step = (1 if kind[:2] == "bq" else 0) + (1 if incoming else 0)
        zs = slot(which, -sign * step)
        return [(None, same(wb.at[zs, halves(half)], ctx_of(0, 0, sign)))]

    def under(cond, act):
        if cond is None:
            act()
        else:
            pl.when(cond)(act)

    got = set()

    def need(names):
        for name in names:
            if name not in got and name[0] != "att":
                got.add(name)
                if name[0] == "b":
                    continue
                if name[0] == "tg":
                    @pl.when(owner == t)
                    def _(name=name):
                        w_local[name[1]].wait()
                if name[0] == "hop":
                    name = ("b",) + name[1:]
                for cond, cp in copies(name, True):
                    under(cond, cp.wait_recv)

    def send(name):
        need(TASKS[name][2])
        if name[0] == "b":
            need([("hop",) + name[1:]])
        if name[0] in ("by+", "by-"):
            for hop in (1, 2) if name[1] == "N" else (1, 2, 3, 4):
                need([("hop", hop, k) for k in range(4 if hop < 4 else 2)])
        for cond, cp in copies(name, False):
            under(cond, cp.start)

    scale2 = (1.0 / math.sqrt(HD)) * math.log2(math.e)

    def rotate_queries():
        for k in ("q", "cos", "sin", "hot"):
            loads[k].wait()

        def body(hd, carry):
            cols = pl.ds(pl.multiple_of(hd * HD, HD), HD)
            v = q[:, cols].astype(jnp.float32)
            v = v * cos[...] + pltpu.roll(v, HD // 2, 1) * sin[...]
            q[:, cols] = v.astype(jnp.bfloat16)
            return carry

        lax.fori_loop(0, HEADS, body, 0)

    def attend(m, g):
        rows = pl.ds(pl.multiple_of(m * CHUNK, CHUNK), CHUNK)
        keys = pl.ds(pl.multiple_of(m * CHUNK, CHUNK), WINDOW)
        mine = hot[pl.ds(pl.multiple_of(BACK * TOK + m * CHUNK, CHUNK), CHUNK), :]
        heads = []
        for i in range(4):
            qh = q[rows, pl.ds(pl.multiple_of((g * 4 + i) * HD, HD), HD)]
            heads.append(jnp.concatenate([qh, mine], axis=1))
        qs = jnp.concatenate(heads, axis=0)
        other = ((hot[keys, :].astype(jnp.float32) - 1.0) * BIG).astype(jnp.bfloat16)
        ks = jnp.concatenate([kbuf[keys, :], other], axis=1)
        score = lax.dot_general(
            qs, ks, (((1,), (1,)), ((), ())), preferred_element_type=jnp.float32)
        row = lax.broadcasted_iota(jnp.int32, (4 * CHUNK, CHUNK), 0) % CHUNK
        col = lax.broadcasted_iota(jnp.int32, (4 * CHUNK, CHUNK), 1)
        edge = jnp.where(col <= row, score[:, WINDOW - CHUNK:], -BIG)
        score = jnp.concatenate([score[:, :WINDOW - CHUNK], edge], axis=1)
        peak = jnp.max(score, axis=1, keepdims=True)
        prob = jnp.exp2((score - peak) * scale2).astype(jnp.bfloat16)
        vs = jnp.concatenate([vbuf[keys, :], jnp.ones((WINDOW, HD), jnp.bfloat16)], axis=1)
        mixed = jnp.dot(prob, vs, preferred_element_type=jnp.float32)
        result = (mixed[:, :HD] / mixed[:, HD:]).astype(jnp.bfloat16)
        for i in range(4):
            att[me, rows, pl.ds(pl.multiple_of((g * 4 + i) * HD, HD), HD)] = (
                result[i * CHUNK:(i + 1) * CHUNK])

    def c_copy(m, hh, part):
        return pltpu.make_async_remote_copy(
            src_ref=csend.at[m, hh, part], dst_ref=crecv.at[me, part],
            send_sem=c_send.at[m, hh, part], recv_sem=c_recv.at[me, part],
            device_id=(z * 8 + hh * 4 + y, m), device_id_type=MESH)

    def matmul(m, part):
        need(mat_needs(m, part))
        rows = pl.ds(m * CHUNK, CHUNK)
        for pair in range(2):
            total = None
            z0, z1 = [(z + PARTS[part][2 * pair + i] + 8) % 8 for i in range(2)]
            for u in range(4):
                lhs = jnp.concatenate([att[u, rows, :], att[4 + u, rows, :]], axis=0)
                rhs = jnp.concatenate(
                    [jnp.concatenate([wa[z0, u], wb[z0, u]], axis=0),
                     jnp.concatenate([wa[z1, u], wb[z1, u]], axis=0)], axis=1)
                one = jnp.dot(lhs, rhs, preferred_element_type=jnp.float32)
                total = one if total is None else total + one
            total = total.astype(jnp.bfloat16)
            cols = pl.ds(pair * 256, 256)
            for hh in range(2):
                csend[m, hh, part, :, cols] = total[hh * CHUNK:(hh + 1) * CHUNK]
        for hh in range(2):
            mine = (h == hh) & (t == m)

            @pl.when(mine)
            def _(hh=hh):
                crecv[me, part] = csend[m, hh, part]

            pl.when(jnp.logical_not(mine))(c_copy(m, hh, part).start)

    def final(part):
        if part == 0:
            loads["res"].wait()

        def body(s, carry):
            hs, ts = s // 4, s % 4
            cp = pltpu.make_async_remote_copy(
                src_ref=csend.at[0, 0, part], dst_ref=crecv.at[s, part],
                send_sem=c_send.at[0, 0, part], recv_sem=c_recv.at[s, part],
                device_id=mate, device_id_type=MESH)
            pl.when(s != me)(cp.wait_recv)
            for i, dz in enumerate(PARTS[part]):
                zs = (z + dz + 8) % 8
                col = (zs * 8 + hs * 4 + (ts - zs + 8) % 4) * HD
                wide = pl.ds(pl.multiple_of(col, HD), HD)
                got_c = crecv[s, part, :, i * HD:(i + 1) * HD].astype(jnp.float32)
                out_ref[:, wide] = (got_c + res[:, wide].astype(jnp.float32)).astype(jnp.bfloat16)
            return carry

        lax.fori_loop(0, 8, body, 0)

    items = list(ORDER)
    first = next(i for i, it in enumerate(items) if it[0] == "step")
    last = max(i for i, it in enumerate(items) if it[0] == "step")
    rotated = False
    for it in items[:first]:
        if not rotated and it[1][0] not in ("tg", "kv"):
            rotated = True
            with jax.named_scope("rotq"):
                rotate_queries()
        with jax.named_scope("s_" + "_".join(map(str, it[1])).replace("+", "p").replace("-", "m")):
            send(it[1])
    need([("kv", j) for j in range(1, BACK + 1)])
    slots, at_step = {}, -1
    for it in items[first:last + 1]:
        if it[0] == "step":
            at_step += 1
        else:
            slots.setdefault(at_step, []).append(it[1])

    def step(i, carry):
        with jax.named_scope("attend"):
            attend(i // 2, i % 2)
        for k, names in slots.items():
            def issue(names=names):
                for name in names:
                    send(name)
            pl.when(i == k)(issue)
        return carry

    lax.fori_loop(0, 8, step, 0)
    for it in items[last + 1:]:
        if it[0] == "send":
            with jax.named_scope("s_" + "_".join(map(str, it[1])).replace("+", "p").replace("-", "m")):
                send(it[1])
        elif it[0] == "M":
            with jax.named_scope("M%d%d" % it[1:]):
                matmul(*it[1:])
        else:
            with jax.named_scope("F%d" % it[1]):
                final(it[1])
    for name in NAMES:
        need([name])
        for cond, cp in copies(name, False):
            under(cond, cp.wait_send)
    for m in range(4):
        for hh in range(2):
            for part in range(2):
                pl.when(jnp.logical_not((h == hh) & (t == m)))(c_copy(m, hh, part).wait_send)


def rotary_tables(positions):
    half_dim = HD // 2
    freq_index = jnp.arange(half_dim)
    inv_freq = theta_base ** (-2.0 * freq_index.astype(jnp.float32) / HD)
    first_end = HD // 8
    second_end = first_end + 3 * HD // 16
    place = positions.astype(jnp.float32)
    chosen = jnp.where(
        freq_index[None, :] < first_end,
        place[0][:, None],
        jnp.where(freq_index[None, :] < second_end, place[1][:, None], place[2][:, None]),
    )
    angle = chosen * inv_freq[None, :]
    return (jnp.cos(angle), jnp.sin(angle))


def on_device(queries, keys, values, positions, segment_ids, out_weight, residual):
    cosine, sine = rotary_tables(positions)
    cos2 = jnp.concatenate([cosine, cosine], axis=1)
    sin2 = jnp.concatenate([-sine, sine], axis=1)
    kf = keys.astype(jnp.float32)
    swapped = jnp.concatenate([kf[:, HD // 2:], kf[:, :HD // 2]], axis=1)
    rot_k = (kf * cos2 + swapped * sin2).astype(jnp.bfloat16)
    my = lax.axis_index("ctx")
    wrapped = jnp.concatenate([segment_ids[-BACK * TOK:], segment_ids])
    window = lax.dynamic_slice_in_dim(wrapped, my * TOK, SPAN, 0)
    hot = (window[:, None] == jnp.arange(HD, dtype=jnp.int32)[None, :]).astype(jnp.bfloat16)
    anyspec = pl.BlockSpec(memory_space=pl.ANY)
    nt = len(NAMES)
    bf, f32 = jnp.bfloat16, jnp.float32
    dma = pltpu.SemaphoreType.DMA
    return pl.pallas_call(
        kernel,
        out_shape=jax.ShapeDtypeStruct((CHUNK, 8192), bf),
        in_specs=[anyspec] * 8,
        out_specs=pl.BlockSpec(memory_space=pltpu.VMEM),
        scratch_shapes=[
            pltpu.VMEM((8, 4, ROWS_A, HD), bf),
            pltpu.VMEM((8, 4, ROWS_B, HD), bf),
            pltpu.VMEM((TOK, 1024), bf),
            pltpu.VMEM((TOK, HD), f32),
            pltpu.VMEM((TOK, HD), f32),
            pltpu.VMEM((SPAN, HD), bf),
            pltpu.VMEM((SPAN, HD), bf),
            pltpu.VMEM((SPAN, HD), bf),
            pltpu.VMEM((8, TOK, 1024), bf),
            pltpu.VMEM((4, 2, 2, CHUNK, 512), bf),
            pltpu.VMEM((8, 2, CHUNK, 512), bf),
            pltpu.VMEM((CHUNK, 8192), bf),
            dma((nt,)),
            dma((nt,)),
            dma((BACK,)),
            dma((BACK,)),
            dma((2, 4)),
            dma((4, 2, 2)),
            dma((8, 2)),
            dma((9,)),
        ],
        compiler_params=pltpu.CompilerParams(
            collective_id=0, has_side_effects=True, vmem_limit_bytes=62 * 1024 * 1024),
    )(queries, rot_k, values, cos2, sin2, hot, out_weight, residual)


def solution(mesh):
    return jax.shard_map(
        on_device,
        mesh=mesh,
        in_specs=(
            P("ctx", "tp"),
            P("ctx", "tp"),
            P("ctx", "tp"),
            P(None, "ctx"),
            P(),
            P("tp", "ctx"),
            P(("ctx", "tp"), None),
        ),
        out_specs=P(("ctx", "tp"), None),
        check_vma=False,
    )
```

```python
import math

import jax
import jax.numpy as jnp
from jax import lax
from jax.experimental import pallas as pl
from jax.experimental.pallas import tpu as pltpu
from jax.sharding import PartitionSpec as P

HD = 128
HEADS = 8
TOK = 512
CHUNK = 128
BACK = 4
SPAN = (BACK + 1) * TOK
WINDOW = BACK * TOK + CHUNK
ROWS_A = 512
ROWS_B = 1024 - ROWS_A
RATE = 43.0
HOP = 2.0
STEP = 2.9
AHEAD = 6.0
BIG = 2.0**100
theta_base = 1000000.0
MESH = pl.DeviceIdType.MESH
ORDERED = (0, 1, -1, 2, -2, 3, -3, 4)
PARTS = ((0, 4), (4, 3), (7, 1))
DEPTH = (2, 3, 4)


def build_tasks():
    t = {}
    ra, rb = float(ROWS_A), float(ROWS_B)
    t[("kv", 4)] = ("x+", 256.0, (), 2.0)
    t[("tg", "b")] = ("x-", rb / 4, (), 3.0)
    t[("tg", "a")] = ("x-", ra / 4, (), 3.0)
    for j, link in ((1, "y+"), (3, "y-"), (2, "y+")):
        t[("kv", j)] = (link, 128.0, (), 0.0)
    for j, link in ((1, "y+"), (3, "y-"), (2, "y+")):
        t[("kw", j)] = (link, 128.0, (("kv", 4),), 2.0)
    t[("ay", 1)] = ("y+", ra / 4, (("tg", "a"),), 2.0)
    t[("ay", -1)] = ("y-", ra / 4, (("tg", "a"),), 2.0)
    t[("ay", 2)] = ("y+", ra / 4, (("tg", "a"),), 4.0)
    for p in range(4):
        for d in (1, -1, -2):
            t[("bs", d, p)] = ("z+" if d > 0 else "z-", rb / 8 if d != -2 else rb / 8, (("tg", "b"),), 1.0)
    far = {
        1: (("bs", 1), ("bs", -2)),
        2: (("bf", 1),),
        3: (("bf", 2), ("bf", 1)),
    }
    for stage in (1, 2, 3):
        for p in range(4):
            t[("bf", stage, p)] = (
                "z+", 1.0, tuple(k + (p,) for k in far[stage]), rb / 4 / RATE)
    column = (("tg", "a"), ("ay", 1), ("ay", -1), ("ay", 2))
    for s in range(4):
        size = ra if s < 3 else ra / 2
        t[("az+", s)] = ("z+", size, column if s == 0 else (("az+", s - 1),), 0.0)
        t[("az-", s)] = ("z-", size, column if s == 0 else (("az-", s - 1),), 0.0)
    for slot in "NF":
        for half in (0, 1):
            pieces = (2 * half, 2 * half + 1)
            need = (("tg", "b"),)
            if slot == "N":
                need += tuple(("bs", d, p) for d in (1, -1, -2) for p in pieces)
            else:
                need += tuple(("bf", stage, p) for stage in (1, 2, 3) for p in pieces)
            t[("by+", slot, half)] = ("y+", rb / 2, need, 0.0)
            t[("by-", slot, half)] = ("y-", rb / 2, need, 0.0)
        t[("bq+", slot, 0)] = ("y+", rb / 2, (("by+", slot, 0),), 0.0)
        t[("bq-", slot, 1)] = ("y-", rb / 2, (("by-", slot, 1),), 0.0)
    for m in range(4):
        for s in "+-":
            t[("at" + s, m)] = ("x" + s, 256.0, (("att", m),), 0.0)
            t[("ar2" + s, m)] = ("x" + s, 128.0, (("at" + s, m),), 0.0)
        t[("am", m, "own")] = ("d", 256.0 / 12, (("att", m),), 0.0)
        for s in "+-":
            t[("am", m, s)] = ("d", 256.0 / 12, (("at" + s, m),), 0.0)
            t[("am", m, s + "2")] = ("d", 128.0 / 12, (("ar2" + s, m),), 0.0)
    return t


def b_names(slots):
    out = []
    for slot in slots:
        for half in (0, 1):
            out += [("by+", slot, half), ("by-", slot, half)]
        out += [("bq+", slot, 0), ("bq-", slot, 1)]
    return out


def mat_needs(m, part):
    need = [("am", m, k) for k in ("own", "+", "-", "+2", "-2")]
    need += [("at+", m), ("at-", m), ("ar2+", m), ("ar2-", m)]
    need += b_names("N" if part == 0 else "NF")
    for s in range(DEPTH[part]):
        need += [("az+", s), ("az-", s)]
    return tuple(need)


def plan(t):
    rank = {}
    for n, name in enumerate(t):
        k = name[0]
        if k == "kv":
            r = 0
        elif k == "kw":
            r = 0.55
        elif k == "tg":
            r = 0
        elif k == "ay":
            r = 0.6
        elif k == "bs":
            r = 0.5
        elif k == "bf":
            r = 3
        elif k in ("az+", "az-"):
            r = 6
        elif k in ("at+", "at-"):
            r = 4
        elif k in ("ar2+", "ar2-"):
            r = 3
        elif k == "am":
            r = 4
        else:
            r = 5 if name[1] == "N" else 7
        rank[name] = (r, n)
    link_free, arrive = {}, {}
    pending = sorted(t, key=lambda k: rank[k])
    order, now = [], 0.0
    steps = [(m, g) for m in range(4) for g in range(2)]
    mats = [(m, part) for part in range(len(PARTS)) for m in range(4)]
    finals = []
    sent = {part: [] for part in range(len(PARTS))}

    def ready(names):
        return all(arrive.get(n, 1e9) <= now for n in names)

    def send(name, link, size, extra):
        start = max(now, link_free.get(link, 0.0))
        link_free[link] = start + size / RATE
        arrive[name] = link_free[link] + HOP + extra

    while pending or steps or mats or finals:
        for n in list(pending):
            if len(steps) == 8 and n[0] not in ("tg", "kv", "kw", "ay", "bs"):
                continue
            if ready(t[n][2]) and link_free.get(t[n][0], 0.0) - now < AHEAD:
                order.append(("send", n))
                send(n, *[t[n][i] for i in (0, 1, 3)])
                pending.remove(n)
        if steps:
            if ready([("kv", j) for j in range(1, BACK + 1)] + [("kw", j) for j in (1, 2, 3)]):
                m, g = steps.pop(0)
                order.append(("step", m, g))
                now += STEP
                if g == 1:
                    arrive[("att", m)] = now
                continue
        elif mats:
            ok = [c for c in mats if ready(mat_needs(*c))]
            if ok:
                m, part = ok[0]
                mats.remove(ok[0])
                order.append(("M", m, part))
                now += 0.35 * PARTS[part][1]
                send(("c", m, part), "x+", 35.0 * PARTS[part][1], 1.0)
                sent[part].append(("c", m, part))
                if len(sent[part]) == 4:
                    finals.append(part)
                continue
        if finals and not steps and ready(sent[finals[0]]):
            order.append(("F", finals.pop(0)))
            now += 1.0
            continue
        later = [a for a in arrive.values() if a > now]
        later += [f - AHEAD for f in link_free.values() if f - AHEAD > now]
        assert later, "stuck"
        now = min(later) + 1e-6
    return order, now, arrive


TASKS = build_tasks()
ORDER, MODEL_US, ARRIVE = plan(TASKS)
NAMES = list(TASKS)
NUMBER = {n: i for i, n in enumerate(NAMES)}


def kernel(
    q_hbm, k_hbm, v_hbm, cos_hbm, sin_hbm, hot_hbm, w_hbm, res_hbm, out_ref,
    wa, wb, q, cos, sin, kbuf, vbuf, hot, att, csend, crecv, res,
    send_sem, recv_sem, kv_send, kv_recv, tg_recv, c_send, c_recv, local,
):
    c = lax.axis_index("ctx")
    t = lax.axis_index("tp")
    z, h, y = c // 8, (c // 4) % 2, c % 4
    core = t % 2
    chip = t // 2
    x = h * 2 + chip
    owner = (z + y) % 4
    r = (t - z - y + 16) % 4
    me = h * 4 + t

    def ctx_of(dz, dh, dy):
        return (((z + dz + 8) % 8) * 8 + ((h + dh) % 2) * 4 + (y + dy + 4) % 4, t)

    def ring(d):
        other = (x + d + 4) % 4
        return (z * 8 + (other // 2) * 4 + y, (other % 2) * 2 + core)

    mate = (c, chip * 2 + (1 - core))
    barrier = pltpu.get_barrier_semaphore()
    partners = [ctx_of(1, 0, 0), ctx_of(-1, 0, 0), ctx_of(0, 0, 1), ctx_of(0, 0, -1), ctx_of(0, 0, 2), ctx_of(2, 0, 0), ctx_of(-2, 0, 0)]
    for d in range(4):
        for k in range(2):
            other = (x + d) % 4
            who = (z * 8 + (other // 2) * 4 + y, (other % 2) * 2 + (core + k) % 2)
            if d or k:
                partners.append(who)
    for j in (BACK, 64 - BACK):
        partners.append(((c + j) % 64, t))
    for d in partners:
        pl.semaphore_signal(barrier, inc=1, device_id=d, device_id_type=MESH)

    own = pl.ds(BACK * TOK, TOK)
    loads = {
        "k": pltpu.make_async_copy(k_hbm, kbuf.at[own], local.at[0]),
        "v": pltpu.make_async_copy(v_hbm, vbuf.at[own], local.at[1]),
        "q": pltpu.make_async_copy(q_hbm, q, local.at[2]),
        "cos": pltpu.make_async_copy(cos_hbm, cos, local.at[3]),
        "sin": pltpu.make_async_copy(sin_hbm, sin, local.at[4]),
        "hot": pltpu.make_async_copy(hot_hbm, hot, local.at[5]),
        "res": pltpu.make_async_copy(res_hbm, res, local.at[6]),
    }
    for cp in loads.values():
        cp.start()
    w_rows = {"a": pl.ds(0, ROWS_A), "b": pl.ds(ROWS_A, ROWS_B)}
    w_buf = {"a": wa, "b": wb}
    w_local = {
        k: pltpu.make_async_copy(w_hbm.at[w_rows[k]], w_buf[k].at[z, t], local.at[7 + i])
        for i, k in enumerate("ab")
    }

    @pl.when(owner == t)
    def _():
        for k in "ab":
            w_local[k].start()

    with jax.named_scope("barrier"):
        pl.semaphore_wait(barrier, len(partners))
    with jax.named_scope("kvload"):
        loads["k"].wait()
        loads["v"].wait()

    def slot(which, dy):
        rr = (r - dy + 8) % 4
        near = jnp.where(rr == 3, -1, rr)
        return (z + near + (8 if which == "N" else 12)) % 8

    def halves(half):
        return pl.ds(2 * half, 2)

    def copies(name, incoming):
        kind = name[0]
        n = NUMBER.get(name)

        def one(src, dst, dev, ss=None, rs=None):
            return pltpu.make_async_remote_copy(
                src_ref=src, dst_ref=dst,
                send_sem=send_sem.at[n] if ss is None else ss,
                recv_sem=recv_sem.at[n] if rs is None else rs,
                device_id=dev, device_id_type=MESH)

        def same(ref, dev, **k):
            return one(ref, ref, dev, **k)

        if kind in ("kv", "kw"):
            j = name[1]
            to = pl.ds((BACK - j) * TOK, TOK)
            n = NUMBER[("kv", j)]
            wrap = y + j >= 4
            dev = ((c + 4) % 64, t) if j == 4 else ctx_of(0, 0, j)
            cond = None if j == 4 else (wrap if kind == "kw" else jnp.logical_not(wrap))
            at = own if kind == "kv" else pl.ds(0, TOK)
            if incoming:
                if kind == "kw":
                    return []
                cond = None
            return [(cond, one(kbuf.at[at], kbuf.at[to], dev)),
                    (cond, one(vbuf.at[at], vbuf.at[to], dev, kv_send.at[j - 1], kv_recv.at[j - 1]))]
        if kind == "tg":
            k = name[1]
            i = "ab".index(k)
            if not incoming:
                return [(owner != t, one(w_hbm.at[w_rows[k]], w_buf[k].at[z, t], (c, owner),
                                         rs=tg_recv.at[i, t]))]
            return [((r == 0) & (t != u),
                     same(w_buf[k].at[z, u], (c, owner), rs=tg_recv.at[i, u])) for u in range(4)]
        if kind in ("at+", "at-", "ar2+", "ar2-", "am"):
            m = name[1]
            rows = pl.ds(m * CHUNK, CHUNK)
            if kind == "am":
                k = name[2]
                d = {"own": 0, "+": -1, "-": 1, "+2": 2, "-2": 2}[k]
                from_core = (1 - core) if incoming else core
                if k == "+2":
                    rows = pl.ds(m * CHUNK, CHUNK // 2)
                if k == "-2":
                    rows = pl.ds(m * CHUNK + CHUNK // 2, CHUNK // 2)
                i = ((x + d + 4) % 4) * 2 + from_core
                return [(None, same(att.at[i, rows], mate))]
            sign = 1 if kind[-1] == "+" else -1
            d = -sign * ((1 if kind[:3] == "ar2" else 0) + (1 if incoming else 0))
            if kind[:3] == "ar2":
                rows = pl.ds(m * CHUNK + (0 if sign > 0 else CHUNK // 2), CHUNK // 2)
            i = ((x + d + 4) % 4) * 2 + core
            return [(None, same(att.at[i, rows], ring(sign)))]
        if kind == "ay":
            d = name[1]
            cond = (r == (4 - d) % 4) if incoming else (r == 0)
            return [(cond, same(wa.at[z], ctx_of(0, 0, d)))]
        if kind == "bs":
            d, p = name[1], name[2]
            zs = (z - (d if incoming else 0) + 8) % 8
            cond = (r == (4 - d) % 4) if incoming else (r == 0)
            return [(cond, same(wb.at[zs, p], ctx_of(d, 0, 0)))]
        if kind == "bf":
            stage, p = name[1], name[2]
            out = []
            for sign, sender, carried in {
                1: ((1, 3, 1), (-1, 2, 2)),
                2: ((1, 2, 2),),
                3: ((1, 1, 3), (-1, 3, 3)),
            }[stage]:
                if stage == 3 and (p < 2) != (sign > 0):
                    continue
                rr = (sender - sign + 4) % 4 if incoming else sender
                zs = (z - sign * (carried + (1 if incoming else 0)) + 8) % 8
                out.append((r == rr, same(wb.at[zs, p], ctx_of(sign, 0, 0))))
            return out
        sign = 1 if kind[2] == "+" else -1
        if kind[:2] == "az":
            s = name[1]
            zz = (z - sign * (s + (1 if incoming else 0)) + 8) % 8
            ref = wa.at[zz] if s < 3 else wa.at[zz, halves(0 if sign > 0 else 1)]
            return [(None, same(ref, ctx_of(sign, 0, 0)))]
        which, half = name[1], name[2]
        step = (1 if kind[:2] == "bq" else 0) + (1 if incoming else 0)
        zs = slot(which, -sign * step)
        return [(None, same(wb.at[zs, halves(half)], ctx_of(0, 0, sign)))]

    def under(cond, act):
        if cond is None:
            act()
        else:
            pl.when(cond)(act)

    got = set()

    def need(names):
        for name in names:
            if name not in got and name[0] != "att":
                got.add(name)
                if name[0] == "tg":
                    @pl.when(owner == t)
                    def _(name=name):
                        w_local[name[1]].wait()
                for cond, cp in copies(name, True):
                    under(cond, cp.wait_recv)

    def send(name):
        need(TASKS[name][2])
        for cond, cp in copies(name, False):
            under(cond, cp.start)

    scale2 = (1.0 / math.sqrt(HD)) * math.log2(math.e)

    def rotate_queries():
        for k in ("q", "cos", "sin", "hot"):
            loads[k].wait()

        def body(hd, carry):
            cols = pl.ds(pl.multiple_of(hd * HD, HD), HD)
            v = q[:, cols].astype(jnp.float32)
            v = v * cos[...] + pltpu.roll(v, HD // 2, 1) * sin[...]
            q[:, cols] = v.astype(jnp.bfloat16)
            return carry

        lax.fori_loop(0, HEADS, body, 0)

    def attend(m, g):
        rows = pl.ds(pl.multiple_of(m * CHUNK, CHUNK), CHUNK)
        keys = pl.ds(pl.multiple_of(m * CHUNK, CHUNK), WINDOW)
        mine = hot[pl.ds(pl.multiple_of(BACK * TOK + m * CHUNK, CHUNK), CHUNK), :]
        heads = []
        for i in range(4):
            qh = q[rows, pl.ds(pl.multiple_of((g * 4 + i) * HD, HD), HD)]
            heads.append(jnp.concatenate([qh, mine], axis=1))
        qs = jnp.concatenate(heads, axis=0)
        other = ((hot[keys, :].astype(jnp.float32) - 1.0) * BIG).astype(jnp.bfloat16)
        ks = jnp.concatenate([kbuf[keys, :], other], axis=1)
        score = lax.dot_general(
            qs, ks, (((1,), (1,)), ((), ())), preferred_element_type=jnp.float32)
        row = lax.broadcasted_iota(jnp.int32, (4 * CHUNK, CHUNK), 0) % CHUNK
        col = lax.broadcasted_iota(jnp.int32, (4 * CHUNK, CHUNK), 1)
        edge = jnp.where(col <= row, score[:, WINDOW - CHUNK:], -BIG)
        score = jnp.concatenate([score[:, :WINDOW - CHUNK], edge], axis=1)
        peak = jnp.max(score, axis=1, keepdims=True)
        prob = jnp.exp2((score - peak) * scale2).astype(jnp.bfloat16)
        vs = jnp.concatenate([vbuf[keys, :], jnp.ones((WINDOW, HD), jnp.bfloat16)], axis=1)
        mixed = jnp.dot(prob, vs, preferred_element_type=jnp.float32)
        result = (mixed[:, :HD] / mixed[:, HD:]).astype(jnp.bfloat16)
        for i in range(4):
            att[me, rows, pl.ds(pl.multiple_of((g * 4 + i) * HD, HD), HD)] = (
                result[i * CHUNK:(i + 1) * CHUNK])

    def part_cols(part):
        return pl.ds(PARTS[part][0] * HD, PARTS[part][1] * HD)

    def c_copy(m, hh, part):
        return pltpu.make_async_remote_copy(
            src_ref=csend.at[m, hh, :, part_cols(part)], dst_ref=crecv.at[me, :, part_cols(part)],
            send_sem=c_send.at[m, hh, part], recv_sem=c_recv.at[me, part],
            device_id=(z * 8 + hh * 4 + y, m), device_id_type=MESH)

    def matmul(m, part):
        need(mat_needs(m, part))
        rows = pl.ds(m * CHUNK, CHUNK)
        begin, count = PARTS[part]
        for at in range(begin, begin + count, 2):
            total = None
            wide = range(at, min(at + 2, begin + count))
            zs = [(z + ORDERED[i] + 8) % 8 for i in wide]
            for u in range(4):
                lhs = jnp.concatenate([att[u, rows, :], att[4 + u, rows, :]], axis=0)
                rhs = [jnp.concatenate([wa[i, u], wb[i, u]], axis=0) for i in zs]
                rhs = jnp.concatenate(rhs, axis=1) if len(rhs) > 1 else rhs[0]
                one = jnp.dot(lhs, rhs, preferred_element_type=jnp.float32)
                total = one if total is None else total + one
            total = total.astype(jnp.bfloat16)
            cols = pl.ds(at * HD, len(wide) * HD)
            for hh in range(2):
                csend[m, hh, :, cols] = total[hh * CHUNK:(hh + 1) * CHUNK]
        for hh in range(2):
            mine = (h == hh) & (t == m)

            @pl.when(mine)
            def _(hh=hh):
                crecv[me, :, part_cols(part)] = csend[m, hh, :, part_cols(part)]

            pl.when(jnp.logical_not(mine))(c_copy(m, hh, part).start)

    def final(part):
        if part == 0:
            loads["res"].wait()

        def body(s, carry):
            hs, ts = s // 4, s % 4
            cp = pltpu.make_async_remote_copy(
                src_ref=csend.at[0, 0, :, part_cols(part)], dst_ref=crecv.at[s, :, part_cols(part)],
                send_sem=c_send.at[0, 0, part], recv_sem=c_recv.at[s, part],
                device_id=mate, device_id_type=MESH)
            pl.when(s != me)(cp.wait_recv)
            for i in range(PARTS[part][0], sum(PARTS[part])):
                zs = (z + ORDERED[i] + 8) % 8
                col = (zs * 8 + hs * 4 + (ts - zs + 8) % 4) * HD
                wide = pl.ds(pl.multiple_of(col, HD), HD)
                got_c = crecv[s, :, i * HD:(i + 1) * HD].astype(jnp.float32)
                out_ref[:, wide] = (got_c + res[:, wide].astype(jnp.float32)).astype(jnp.bfloat16)
            return carry

        lax.fori_loop(0, 8, body, 0)

    items = list(ORDER)
    first = next(i for i, it in enumerate(items) if it[0] == "step")
    last = max(i for i, it in enumerate(items) if it[0] == "step")
    rotated = False
    for it in items[:first]:
        if not rotated and it[1][0] != "tg" and it[1][0] != "kv":
            rotated = True
            with jax.named_scope("rotq"):
                rotate_queries()
        with jax.named_scope("s_" + "_".join(map(str, it[1])).replace("+", "p").replace("-", "m")):
            send(it[1])
    need([("kv", j) for j in range(1, BACK + 1)])
    slots, at_step = {}, -1
    for it in items[first:last + 1]:
        if it[0] == "step":
            at_step += 1
        else:
            slots.setdefault(at_step, []).append(it[1])

    def step(i, carry):
        with jax.named_scope("attend"):
            attend(i // 2, i % 2)
        for k, names in slots.items():
            def issue(names=names):
                for name in names:
                    send(name)
            pl.when(i == k)(issue)
        return carry

    lax.fori_loop(0, 8, step, 0)
    for it in items[last + 1:]:
        if it[0] == "send":
            with jax.named_scope("s_" + "_".join(map(str, it[1])).replace("+", "p").replace("-", "m")):
                send(it[1])
        elif it[0] == "M":
            with jax.named_scope("M%d%d" % it[1:]):
                matmul(*it[1:])
        else:
            with jax.named_scope("F%d" % it[1]):
                final(it[1])
    for name in NAMES:
        need([name])
        for cond, cp in copies(name, False):
            under(cond, cp.wait_send)
    for m in range(4):
        for hh in range(2):
            for part in range(len(PARTS)):
                pl.when(jnp.logical_not((h == hh) & (t == m)))(c_copy(m, hh, part).wait_send)


def rotary_tables(positions):
    half_dim = HD // 2
    freq_index = jnp.arange(half_dim)
    inv_freq = theta_base ** (-2.0 * freq_index.astype(jnp.float32) / HD)
    first_end = HD // 8
    second_end = first_end + 3 * HD // 16
    place = positions.astype(jnp.float32)
    chosen = jnp.where(
        freq_index[None, :] < first_end,
        place[0][:, None],
        jnp.where(freq_index[None, :] < second_end, place[1][:, None], place[2][:, None]),
    )
    angle = chosen * inv_freq[None, :]
    return (jnp.cos(angle), jnp.sin(angle))


def on_device(queries, keys, values, positions, segment_ids, out_weight, residual):
    cosine, sine = rotary_tables(positions)
    cos2 = jnp.concatenate([cosine, cosine], axis=1)
    sin2 = jnp.concatenate([-sine, sine], axis=1)
    kf = keys.astype(jnp.float32)
    swapped = jnp.concatenate([kf[:, HD // 2:], kf[:, :HD // 2]], axis=1)
    rot_k = (kf * cos2 + swapped * sin2).astype(jnp.bfloat16)
    my = lax.axis_index("ctx")
    wrapped = jnp.concatenate([segment_ids[-BACK * TOK:], segment_ids])
    window = lax.dynamic_slice_in_dim(wrapped, my * TOK, SPAN, 0)
    hot = (window[:, None] == jnp.arange(HD, dtype=jnp.int32)[None, :]).astype(jnp.bfloat16)
    anyspec = pl.BlockSpec(memory_space=pl.ANY)
    nt = len(NAMES)
    bf, f32 = jnp.bfloat16, jnp.float32
    dma = pltpu.SemaphoreType.DMA
    return pl.pallas_call(
        kernel,
        out_shape=jax.ShapeDtypeStruct((CHUNK, 8192), bf),
        in_specs=[anyspec] * 8,
        out_specs=pl.BlockSpec(memory_space=pltpu.VMEM),
        scratch_shapes=[
            pltpu.VMEM((8, 4, ROWS_A, HD), bf),
            pltpu.VMEM((8, 4, ROWS_B, HD), bf),
            pltpu.VMEM((TOK, 1024), bf),
            pltpu.VMEM((TOK, HD), f32),
            pltpu.VMEM((TOK, HD), f32),
            pltpu.VMEM((SPAN, HD), bf),
            pltpu.VMEM((SPAN, HD), bf),
            pltpu.VMEM((SPAN, HD), bf),
            pltpu.VMEM((8, TOK, 1024), bf),
            pltpu.VMEM((4, 2, CHUNK, 1024), bf),
            pltpu.VMEM((8, CHUNK, 1024), bf),
            pltpu.VMEM((CHUNK, 8192), bf),
            dma((nt,)),
            dma((nt,)),
            dma((BACK,)),
            dma((BACK,)),
            dma((2, 4)),
            dma((4, 2, len(PARTS))),
            dma((8, len(PARTS))),
            dma((9,)),
        ],
        compiler_params=pltpu.CompilerParams(
            collective_id=0, has_side_effects=True, vmem_limit_bytes=62 * 1024 * 1024),
    )(queries, rot_k, values, cos2, sin2, hot, out_weight, residual)


def solution(mesh):
    return jax.shard_map(
        on_device,
        mesh=mesh,
        in_specs=(
            P("ctx", "tp"),
            P("ctx", "tp"),
            P("ctx", "tp"),
            P(None, "ctx"),
            P(),
            P("tp", "ctx"),
            P(("ctx", "tp"), None),
        ),
        out_specs=P(("ctx", "tp"), None),
        check_vma=False,
    )
```

```python
import math

import jax
import jax.numpy as jnp
from jax import lax
from jax.experimental import pallas as pl
from jax.experimental.pallas import tpu as pltpu
from jax.sharding import PartitionSpec as P

HD = 128
HEADS = 8
TOK = 512
CHUNK = 128
BACK = 4
SPAN = (BACK + 1) * TOK
WINDOW = BACK * TOK + CHUNK
ROWS_A = 384
ROWS_B = 1024 - ROWS_A
RATE = 43.0
HOP = 2.0
STEP = 2.9
AHEAD = 6.0
BIG = 2.0**100
theta_base = 1000000.0
MESH = pl.DeviceIdType.MESH
ORDERED = (0, 1, -1, 2, -2, 3, -3, 4)
PARTS = ((0, 4), (4, 3), (7, 1))
DEPTH = (2, 3, 4)


def build_tasks():
    t = {}
    ra, rb = float(ROWS_A), float(ROWS_B)
    t[("kv", 4)] = ("x+", 256.0, (), 2.0)
    t[("tg", "b")] = ("x-", rb / 4, (), 3.0)
    t[("tg", "a")] = ("x-", ra / 4, (), 3.0)
    for j, link in ((1, "y+"), (3, "y-"), (2, "y+")):
        t[("kv", j)] = (link, 128.0, (), 0.0)
    for j, link in ((1, "y+"), (3, "y-"), (2, "y+")):
        t[("kw", j)] = (link, 128.0, (("kv", 4),), 2.0)
    t[("ay", 1)] = ("y+", ra / 4, (("tg", "a"),), 10.0)
    t[("ay", -1)] = ("y-", ra / 4, (("tg", "a"),), 10.0)
    t[("ay", 2)] = ("y+", ra / 4, (("tg", "a"),), 10.0)
    for p in range(4):
        for d in (1, -1, -2):
            t[("bs", d, p)] = ("z+" if d > 0 else "z-", rb / 8 if d != -2 else rb / 8, (("tg", "b"),), 1.0)
    far = {
        1: (("bs", 1), ("bs", -2)),
        2: (("bf", 1),),
        3: (("bf", 2), ("bf", 1)),
    }
    for stage in (1, 2, 3):
        for p in range(4):
            t[("bf", stage, p)] = (
                "z+", 1.0, tuple(k + (p,) for k in far[stage]), rb / 4 / RATE)
    column = (("tg", "a"), ("ay", 1), ("ay", -1), ("ay", 2))
    for s in range(4):
        size = ra if s < 3 else ra / 2
        t[("az+", s)] = ("z+", size, column if s == 0 else (("az+", s - 1),), 0.0)
        t[("az-", s)] = ("z-", size, column if s == 0 else (("az-", s - 1),), 0.0)
    for slot in "NF":
        for half in (0, 1):
            pieces = (2 * half, 2 * half + 1)
            need = (("tg", "b"),)
            if slot == "N":
                need += tuple(("bs", d, p) for d in (1, -1, -2) for p in pieces)
            else:
                need += tuple(("bf", stage, p) for stage in (1, 2, 3) for p in pieces)
            t[("by+", slot, half)] = ("y+", rb / 2, need, 0.0)
            t[("by-", slot, half)] = ("y-", rb / 2, need, 0.0)
        t[("bq+", slot, 0)] = ("y+", rb / 2, (("by+", slot, 0),), 0.0)
        t[("bq-", slot, 1)] = ("y-", rb / 2, (("by-", slot, 1),), 0.0)
    for m in range(4):
        for s in "+-":
            t[("at" + s, m)] = ("x" + s, 256.0, (("att", m),), 0.0)
            t[("ar2" + s, m)] = ("x" + s, 128.0, (("at" + s, m),), 0.0)
        t[("am", m, "own")] = ("d", 256.0 / 12, (("att", m),), 0.0)
        for s in "+-":
            t[("am", m, s)] = ("d", 256.0 / 12, (("at" + s, m),), 0.0)
            t[("am", m, s + "2")] = ("d", 128.0 / 12, (("ar2" + s, m),), 0.0)
    return t


def b_names(slots):
    out = []
    for slot in slots:
        for half in (0, 1):
            out += [("by+", slot, half), ("by-", slot, half)]
        out += [("bq+", slot, 0), ("bq-", slot, 1)]
    return out


def mat_needs(m, part):
    need = [("am", m, k) for k in ("own", "+", "-", "+2", "-2")]
    need += [("at+", m), ("at-", m), ("ar2+", m), ("ar2-", m)]
    need += b_names("N" if part == 0 else "NF")
    for s in range(DEPTH[part]):
        need += [("az+", s), ("az-", s)]
    return tuple(need)


def plan(t):
    rank = {}
    for n, name in enumerate(t):
        k = name[0]
        if k == "kv":
            r = 0
        elif k == "kw":
            r = 0.55
        elif k == "tg":
            r = 0
        elif k == "ay":
            r = 0.6
        elif k == "bs":
            r = 0.5
        elif k == "bf":
            r = 3
        elif k in ("az+", "az-"):
            r = 6
        elif k in ("at+", "at-"):
            r = 4
        elif k in ("ar2+", "ar2-"):
            r = 3
        elif k == "am":
            r = 4
        else:
            r = 5 if name[1] == "N" else 7
        rank[name] = (r, n)
    link_free, arrive = {}, {}
    pending = sorted(t, key=lambda k: rank[k])
    order, now = [], 0.0
    steps = [(m, g) for m in range(4) for g in range(2)]
    mats = [(m, part) for part in range(len(PARTS)) for m in range(4)]
    finals = []
    sent = {part: [] for part in range(len(PARTS))}

    def ready(names):
        return all(arrive.get(n, 1e9) <= now for n in names)

    def send(name, link, size, extra):
        start = max(now, link_free.get(link, 0.0))
        link_free[link] = start + size / RATE
        arrive[name] = link_free[link] + HOP + extra

    while pending or steps or mats or finals:
        for n in list(pending):
            if len(steps) == 8 and n[0] not in ("tg", "kv", "kw", "ay", "bs"):
                continue
            if ready(t[n][2]) and link_free.get(t[n][0], 0.0) - now < AHEAD:
                order.append(("send", n))
                send(n, *[t[n][i] for i in (0, 1, 3)])
                pending.remove(n)
        if steps:
            if ready([("kv", j) for j in range(1, BACK + 1)] + [("kw", j) for j in (1, 2, 3)]):
                m, g = steps.pop(0)
                order.append(("step", m, g))
                now += STEP
                if g == 1:
                    arrive[("att", m)] = now
                continue
        elif mats:
            ok = [c for c in mats if ready(mat_needs(*c))]
            if ok:
                m, part = ok[0]
                mats.remove(ok[0])
                order.append(("M", m, part))
                now += 0.35 * PARTS[part][1]
                send(("c", m, part), "x+", 35.0 * PARTS[part][1], 1.0)
                sent[part].append(("c", m, part))
                if len(sent[part]) == 4:
                    finals.append(part)
                continue
        if finals and not steps and ready(sent[finals[0]]):
            order.append(("F", finals.pop(0)))
            now += 1.0
            continue
        later = [a for a in arrive.values() if a > now]
        later += [f - AHEAD for f in link_free.values() if f - AHEAD > now]
        assert later, "stuck"
        now = min(later) + 1e-6
    return order, now, arrive


TASKS = build_tasks()
ORDER, MODEL_US, ARRIVE = plan(TASKS)
NAMES = list(TASKS)
NUMBER = {n: i for i, n in enumerate(NAMES)}


def cos_sin(angle):
    turns = jnp.floor(angle * (2.0 / math.pi) + 0.5)
    a = angle - turns * 1.5703125
    a = a - turns * 4.837512969970703125e-4
    a = a - turns * 7.549789948768648e-8
    quarter = turns - 4.0 * jnp.floor(turns * 0.25)
    s = a * a
    sine = a + a * s * (-1.6666654611e-1 + s * (8.3321608736e-3 - s * 1.9515295891e-4))
    cosine = 1.0 - 0.5 * s + s * s * (
        4.166664568298827e-2 + s * (-1.388731625493765e-3 + s * 2.443315711809948e-5))
    odd = (quarter == 1.0) | (quarter == 3.0)
    low_c = (quarter == 1.0) | (quarter == 2.0)
    c = jnp.where(odd, sine, cosine)
    d = jnp.where(odd, cosine, sine)
    return jnp.where(low_c, -c, c), jnp.where(quarter >= 2.0, -d, d)


def kernel(
    q_hbm, k_hbm, v_hbm, pos_hbm, seg_hbm, freq_ref, w_hbm, res_hbm, out_ref,
    wa, wb, q, cos, sin, kraw, kbuf, vbuf, hot, pos, seg, att, csend, crecv, res,
    send_sem, recv_sem, kv_send, kv_recv, tg_recv, c_send, c_recv, local,
):
    c = lax.axis_index("ctx")
    t = lax.axis_index("tp")
    z, h, y = c // 8, (c // 4) % 2, c % 4
    core = t % 2
    chip = t // 2
    x = h * 2 + chip
    owner = (z + y) % 4
    r = (t - z - y + 16) % 4
    me = h * 4 + t

    def ctx_of(dz, dh, dy):
        return (((z + dz + 8) % 8) * 8 + ((h + dh) % 2) * 4 + (y + dy + 4) % 4, t)

    def ring(d):
        other = (x + d + 4) % 4
        return (z * 8 + (other // 2) * 4 + y, (other % 2) * 2 + core)

    mate = (c, chip * 2 + (1 - core))
    barrier = pltpu.get_barrier_semaphore()
    partners = [ctx_of(1, 0, 0), ctx_of(-1, 0, 0), ctx_of(0, 0, 1), ctx_of(0, 0, -1), ctx_of(0, 0, 2), ctx_of(2, 0, 0), ctx_of(-2, 0, 0)]
    for d in range(4):
        for k in range(2):
            other = (x + d) % 4
            who = (z * 8 + (other // 2) * 4 + y, (other % 2) * 2 + (core + k) % 2)
            if d or k:
                partners.append(who)
    for j in (BACK, 64 - BACK):
        partners.append(((c + j) % 64, t))
    for d in partners:
        pl.semaphore_signal(barrier, inc=1, device_id=d, device_id_type=MESH)

    own = pl.ds(BACK * TOK, TOK)
    loads = {
        "pos": pltpu.make_async_copy(pos_hbm, pos.at[pl.ds(0, 3)], local.at[3]),
        "k": pltpu.make_async_copy(k_hbm, kraw, local.at[0]),
        "seg": pltpu.make_async_copy(seg_hbm, seg, local.at[4]),
        "v": pltpu.make_async_copy(v_hbm, vbuf.at[own], local.at[1]),
        "q": pltpu.make_async_copy(q_hbm, q, local.at[2]),
        "res": pltpu.make_async_copy(res_hbm, res, local.at[6]),
    }
    for cp in loads.values():
        cp.start()
    w_rows = {"a": pl.ds(0, ROWS_A), "b": pl.ds(ROWS_A, ROWS_B)}
    w_buf = {"a": wa, "b": wb}
    w_local = {
        k: pltpu.make_async_copy(w_hbm.at[w_rows[k]], w_buf[k].at[z, t], local.at[7 + i])
        for i, k in enumerate("ab")
    }

    @pl.when(owner == t)
    def _():
        for k in "ab":
            w_local[k].start()

    with jax.named_scope("tables"):
        pos[3:8, :] = jnp.zeros((5, TOK), jnp.int32)
        loads["pos"].wait()
        place = jnp.transpose(pos[...].astype(jnp.float32))
        lane = lax.broadcasted_iota(jnp.int32, (TOK, HD), 1) % (HD // 2)
        chosen = jnp.where(
            lane < HD // 8, place[:, 0:1],
            jnp.where(lane < HD // 8 + 3 * HD // 16, place[:, 1:2], place[:, 2:3]))
        cosine, sine = cos_sin(chosen * freq_ref[0:1, :])
        upper = lax.broadcasted_iota(jnp.int32, (TOK, HD), 1) < HD // 2
        cos[...] = cosine
        sin[...] = jnp.where(upper, -sine, sine)
        loads["k"].wait()
        kf = kraw[...].astype(jnp.float32)
        kbuf[own, :] = (kf * cos[...] + pltpu.roll(kf, HD // 2, 1) * sin[...]).astype(jnp.bfloat16)
        loads["v"].wait()
        loads["seg"].wait()
        for j in range(BACK + 1):
            rows = seg[pl.ds(((c - BACK + j + 64) % 64) * 4, 4), :].astype(jnp.float32)
            turned = jnp.transpose(jnp.concatenate([rows, rows], axis=0))
            ids = lax.broadcasted_iota(jnp.int32, (HD, HD), 1).astype(jnp.float32)
            for i in range(4):
                hot[pl.ds(j * TOK + i * HD, HD), :] = (
                    turned[:, i:i + 1] == ids).astype(jnp.float32).astype(jnp.bfloat16)
    with jax.named_scope("barrier"):
        pl.semaphore_wait(barrier, len(partners))

    def slot(which, dy):
        rr = (r - dy + 8) % 4
        near = jnp.where(rr == 3, -1, rr)
        return (z + near + (8 if which == "N" else 12)) % 8

    def halves(half):
        return pl.ds(2 * half, 2)

    def copies(name, incoming):
        kind = name[0]
        n = NUMBER.get(name)

        def one(src, dst, dev, ss=None, rs=None):
            return pltpu.make_async_remote_copy(
                src_ref=src, dst_ref=dst,
                send_sem=send_sem.at[n] if ss is None else ss,
                recv_sem=recv_sem.at[n] if rs is None else rs,
                device_id=dev, device_id_type=MESH)

        def same(ref, dev, **k):
            return one(ref, ref, dev, **k)

        if kind in ("kv", "kw"):
            j = name[1]
            to = pl.ds((BACK - j) * TOK, TOK)
            n = NUMBER[("kv", j)]
            wrap = y + j >= 4
            dev = ((c + 4) % 64, t) if j == 4 else ctx_of(0, 0, j)
            cond = None if j == 4 else (wrap if kind == "kw" else jnp.logical_not(wrap))
            at = own if kind == "kv" else pl.ds(0, TOK)
            if incoming:
                if kind == "kw":
                    return []
                cond = None
            return [(cond, one(vbuf.at[at], vbuf.at[to], dev, kv_send.at[j - 1], kv_recv.at[j - 1])),
                    (cond, one(kbuf.at[at], kbuf.at[to], dev))]
        if kind == "tg":
            k = name[1]
            i = "ab".index(k)
            if not incoming:
                return [(owner != t, one(w_hbm.at[w_rows[k]], w_buf[k].at[z, t], (c, owner),
                                         rs=tg_recv.at[i, t]))]
            return [((r == 0) & (t != u),
                     same(w_buf[k].at[z, u], (c, owner), rs=tg_recv.at[i, u])) for u in range(4)]
        if kind in ("at+", "at-", "ar2+", "ar2-", "am"):
            m = name[1]
            rows = pl.ds(m * CHUNK, CHUNK)
            if kind == "am":
                k = name[2]
                d = {"own": 0, "+": -1, "-": 1, "+2": 2, "-2": 2}[k]
                from_core = (1 - core) if incoming else core
                if k == "+2":
                    rows = pl.ds(m * CHUNK, CHUNK // 2)
                if k == "-2":
                    rows = pl.ds(m * CHUNK + CHUNK // 2, CHUNK // 2)
                i = ((x + d + 4) % 4) * 2 + from_core
                return [(None, same(att.at[i, rows], mate))]
            sign = 1 if kind[-1] == "+" else -1
            d = -sign * ((1 if kind[:3] == "ar2" else 0) + (1 if incoming else 0))
            if kind[:3] == "ar2":
                rows = pl.ds(m * CHUNK + (0 if sign > 0 else CHUNK // 2), CHUNK // 2)
            i = ((x + d + 4) % 4) * 2 + core
            return [(None, same(att.at[i, rows], ring(sign)))]
        if kind == "ay":
            d = name[1]
            cond = (r == (4 - d) % 4) if incoming else (r == 0)
            return [(cond, same(wa.at[z], ctx_of(0, 0, d)))]
        if kind == "bs":
            d, p = name[1], name[2]
            zs = (z - (d if incoming else 0) + 8) % 8
            cond = (r == (4 - d) % 4) if incoming else (r == 0)
            return [(cond, same(wb.at[zs, p], ctx_of(d, 0, 0)))]
        if kind == "bf":
            stage, p = name[1], name[2]
            out = []
            for sign, sender, carried in {
                1: ((1, 3, 1), (-1, 2, 2)),
                2: ((1, 2, 2),),
                3: ((1, 1, 3), (-1, 3, 3)),
            }[stage]:
                if stage == 3 and (p < 2) != (sign > 0):
                    continue
                rr = (sender - sign + 4) % 4 if incoming else sender
                zs = (z - sign * (carried + (1 if incoming else 0)) + 8) % 8
                out.append((r == rr, same(wb.at[zs, p], ctx_of(sign, 0, 0))))
            return out
        sign = 1 if kind[2] == "+" else -1
        if kind[:2] == "az":
            s = name[1]
            zz = (z - sign * (s + (1 if incoming else 0)) + 8) % 8
            ref = wa.at[zz] if s < 3 else wa.at[zz, halves(0 if sign > 0 else 1)]
            return [(None, same(ref, ctx_of(sign, 0, 0)))]
        which, half = name[1], name[2]
        step = (1 if kind[:2] == "bq" else 0) + (1 if incoming else 0)
        zs = slot(which, -sign * step)
        return [(None, same(wb.at[zs, halves(half)], ctx_of(0, 0, sign)))]

    def under(cond, act):
        if cond is None:
            act()
        else:
            pl.when(cond)(act)

    got = set()

    def need(names):
        for name in names:
            if name not in got and name[0] != "att":
                got.add(name)
                if name[0] == "tg":
                    @pl.when(owner == t)
                    def _(name=name):
                        w_local[name[1]].wait()
                for cond, cp in copies(name, True):
                    under(cond, cp.wait_recv)

    def send(name):
        need(TASKS[name][2])
        for cond, cp in copies(name, False):
            under(cond, cp.start)

    scale2 = (1.0 / math.sqrt(HD)) * math.log2(math.e)

    def rotate_queries():
        loads["q"].wait()

        def body(hd, carry):
            cols = pl.ds(pl.multiple_of(hd * HD, HD), HD)
            v = q[:, cols].astype(jnp.float32)
            v = v * cos[...] + pltpu.roll(v, HD // 2, 1) * sin[...]
            q[:, cols] = v.astype(jnp.bfloat16)
            return carry

        lax.fori_loop(0, HEADS, body, 0)

    def attend(m, g):
        rows = pl.ds(pl.multiple_of(m * CHUNK, CHUNK), CHUNK)
        keys = pl.ds(pl.multiple_of(m * CHUNK, CHUNK), WINDOW)
        mine = hot[pl.ds(pl.multiple_of(BACK * TOK + m * CHUNK, CHUNK), CHUNK), :]
        heads = []
        for i in range(4):
            qh = q[rows, pl.ds(pl.multiple_of((g * 4 + i) * HD, HD), HD)]
            heads.append(jnp.concatenate([qh, mine], axis=1))
        qs = jnp.concatenate(heads, axis=0)
        other = ((hot[keys, :].astype(jnp.float32) - 1.0) * BIG).astype(jnp.bfloat16)
        ks = jnp.concatenate([kbuf[keys, :], other], axis=1)
        score = lax.dot_general(
            qs, ks, (((1,), (1,)), ((), ())), preferred_element_type=jnp.float32)
        row = lax.broadcasted_iota(jnp.int32, (4 * CHUNK, CHUNK), 0) % CHUNK
        col = lax.broadcasted_iota(jnp.int32, (4 * CHUNK, CHUNK), 1)
        edge = jnp.where(col <= row, score[:, WINDOW - CHUNK:], -BIG)
        score = jnp.concatenate([score[:, :WINDOW - CHUNK], edge], axis=1)
        peak = jnp.max(score, axis=1, keepdims=True)
        prob = jnp.exp2((score - peak) * scale2).astype(jnp.bfloat16)
        vs = jnp.concatenate([vbuf[keys, :], jnp.ones((WINDOW, HD), jnp.bfloat16)], axis=1)
        mixed = jnp.dot(prob, vs, preferred_element_type=jnp.float32)
        result = (mixed[:, :HD] / mixed[:, HD:]).astype(jnp.bfloat16)
        for i in range(4):
            att[me, rows, pl.ds(pl.multiple_of((g * 4 + i) * HD, HD), HD)] = (
                result[i * CHUNK:(i + 1) * CHUNK])

    def part_cols(part):
        return pl.ds(PARTS[part][0] * HD, PARTS[part][1] * HD)

    def c_copy(m, hh, part):
        return pltpu.make_async_remote_copy(
            src_ref=csend.at[m, hh, :, part_cols(part)], dst_ref=crecv.at[me, :, part_cols(part)],
            send_sem=c_send.at[m, hh, part], recv_sem=c_recv.at[me, part],
            device_id=(z * 8 + hh * 4 + y, m), device_id_type=MESH)

    def matmul(m, part):
        need(mat_needs(m, part))
        rows = pl.ds(m * CHUNK, CHUNK)
        begin, count = PARTS[part]
        for at in range(begin, begin + count, 2):
            total = None
            wide = range(at, min(at + 2, begin + count))
            zs = [(z + ORDERED[i] + 8) % 8 for i in wide]
            for u in range(4):
                lhs = jnp.concatenate([att[u, rows, :], att[4 + u, rows, :]], axis=0)
                rhs = [jnp.concatenate([wa[i, u], wb[i, u]], axis=0) for i in zs]
                rhs = jnp.concatenate(rhs, axis=1) if len(rhs) > 1 else rhs[0]
                one = jnp.dot(lhs, rhs, preferred_element_type=jnp.float32)
                total = one if total is None else total + one
            total = total.astype(jnp.bfloat16)
            cols = pl.ds(at * HD, len(wide) * HD)
            for hh in range(2):
                csend[m, hh, :, cols] = total[hh * CHUNK:(hh + 1) * CHUNK]
        for hh in range(2):
            mine = (h == hh) & (t == m)

            @pl.when(mine)
            def _(hh=hh):
                crecv[me, :, part_cols(part)] = csend[m, hh, :, part_cols(part)]

            pl.when(jnp.logical_not(mine))(c_copy(m, hh, part).start)

    def final(part):
        if part == 0:
            loads["res"].wait()

        def body(s, carry):
            hs, ts = s // 4, s % 4
            cp = pltpu.make_async_remote_copy(
                src_ref=csend.at[0, 0, :, part_cols(part)], dst_ref=crecv.at[s, :, part_cols(part)],
                send_sem=c_send.at[0, 0, part], recv_sem=c_recv.at[s, part],
                device_id=mate, device_id_type=MESH)
            pl.when(s != me)(cp.wait_recv)
            for i in range(PARTS[part][0], sum(PARTS[part])):
                zs = (z + ORDERED[i] + 8) % 8
                col = (zs * 8 + hs * 4 + (ts - zs + 8) % 4) * HD
                wide = pl.ds(pl.multiple_of(col, HD), HD)
                got_c = crecv[s, :, i * HD:(i + 1) * HD].astype(jnp.float32)
                out_ref[:, wide] = (got_c + res[:, wide].astype(jnp.float32)).astype(jnp.bfloat16)
            return carry

        lax.fori_loop(0, 8, body, 0)

    items = list(ORDER)
    first = next(i for i, it in enumerate(items) if it[0] == "step")
    last = max(i for i, it in enumerate(items) if it[0] == "step")
    rotated = False
    for it in items[:first]:
        if not rotated and it[1][0] != "tg" and it[1][0] != "kv":
            rotated = True
            with jax.named_scope("rotq"):
                rotate_queries()
        with jax.named_scope("s_" + "_".join(map(str, it[1])).replace("+", "p").replace("-", "m")):
            send(it[1])
    need([("kv", j) for j in range(1, BACK + 1)])
    slots, at_step = {}, -1
    for it in items[first:last + 1]:
        if it[0] == "step":
            at_step += 1
        else:
            slots.setdefault(at_step, []).append(it[1])

    def step(i, carry):
        with jax.named_scope("attend"):
            attend(i // 2, i % 2)
        for k, names in slots.items():
            def issue(names=names):
                for name in names:
                    send(name)
            pl.when(i == k)(issue)
        return carry

    lax.fori_loop(0, 8, step, 0)
    for it in items[last + 1:]:
        if it[0] == "send":
            with jax.named_scope("s_" + "_".join(map(str, it[1])).replace("+", "p").replace("-", "m")):
                send(it[1])
        elif it[0] == "M":
            with jax.named_scope("M%d%d" % it[1:]):
                matmul(*it[1:])
        else:
            with jax.named_scope("F%d" % it[1]):
                final(it[1])
    for name in NAMES:
        need([name])
        for cond, cp in copies(name, False):
            under(cond, cp.wait_send)
    for m in range(4):
        for hh in range(2):
            for part in range(len(PARTS)):
                pl.when(jnp.logical_not((h == hh) & (t == m)))(c_copy(m, hh, part).wait_send)


def on_device(queries, keys, values, positions, segment_ids, out_weight, residual):
    half = jnp.arange(HD // 2).astype(jnp.float32)
    freq = theta_base ** (-2.0 * half / HD)
    freq = jnp.broadcast_to(jnp.concatenate([freq, freq])[None], (8, HD))
    anyspec = pl.BlockSpec(memory_space=pl.ANY)
    nt = len(NAMES)
    bf, f32 = jnp.bfloat16, jnp.float32
    dma = pltpu.SemaphoreType.DMA
    return pl.pallas_call(
        kernel,
        out_shape=jax.ShapeDtypeStruct((CHUNK, 8192), bf),
        in_specs=[anyspec] * 5 + [pl.BlockSpec(memory_space=pltpu.VMEM)] + [anyspec] * 2,
        out_specs=pl.BlockSpec(memory_space=pltpu.VMEM),
        scratch_shapes=[
            pltpu.VMEM((8, 4, ROWS_A, HD), bf),
            pltpu.VMEM((8, 4, ROWS_B, HD), bf),
            pltpu.VMEM((TOK, 1024), bf),
            pltpu.VMEM((TOK, HD), f32),
            pltpu.VMEM((TOK, HD), f32),
            pltpu.VMEM((TOK, HD), bf),
            pltpu.VMEM((SPAN, HD), bf),
            pltpu.VMEM((SPAN, HD), bf),
            pltpu.VMEM((SPAN, HD), bf),
            pltpu.VMEM((8, TOK), jnp.int32),
            pltpu.VMEM((256, HD), jnp.int32),
            pltpu.VMEM((8, TOK, 1024), bf),
            pltpu.VMEM((4, 2, CHUNK, 1024), bf),
            pltpu.VMEM((8, CHUNK, 1024), bf),
            pltpu.VMEM((CHUNK, 8192), bf),
            dma((nt,)),
            dma((nt,)),
            dma((BACK,)),
            dma((BACK,)),
            dma((2, 4)),
            dma((4, 2, len(PARTS))),
            dma((8, len(PARTS))),
            dma((9,)),
        ],
        compiler_params=pltpu.CompilerParams(
            collective_id=0, has_side_effects=True, vmem_limit_bytes=62 * 1024 * 1024),
    )(queries, keys, values, positions, segment_ids.reshape(256, HD), freq, out_weight, residual)


def solution(mesh):
    return jax.shard_map(
        on_device,
        mesh=mesh,
        in_specs=(
            P("ctx", "tp"),
            P("ctx", "tp"),
            P("ctx", "tp"),
            P(None, "ctx"),
            P(),
            P("tp", "ctx"),
            P(("ctx", "tp"), None),
        ),
        out_specs=P(("ctx", "tp"), None),
        check_vma=False,
    )
```

```python
import math

import jax
import jax.numpy as jnp
from jax import lax
from jax.experimental import pallas as pl
from jax.experimental.pallas import tpu as pltpu
from jax.sharding import PartitionSpec as P

HD = 128
HEADS = 8
TOK = 512
CHUNK = 128
BACK = 4
SPAN = (BACK + 1) * TOK
WINDOW = BACK * TOK + CHUNK
ROWS_A = 384
ROWS_B = 1024 - ROWS_A
RATE = 43.0
HOP = 2.0
STEP = 2.9
AHEAD = 6.0
BIG = 2.0**100
theta_base = 1000000.0
MESH = pl.DeviceIdType.MESH
ORDERED = (0, 1, -1, 2, -2, 3, -3, 4)
PARTS = ((0, 4), (4, 3), (7, 1))
DEPTH = (2, 3, 4)


def build_tasks():
    t = {}
    ra, rb = float(ROWS_A), float(ROWS_B)
    t[("kv", 4)] = ("x+", 256.0, (), 2.0)
    t[("tg", "b")] = ("x-", rb / 4, (), 3.0)
    t[("tg", "a")] = ("x-", ra / 4, (), 3.0)
    for j, link in ((2, "y-"), (1, "y+"), (3, "y-")):
        t[("kv", j)] = (link, 128.0, (), 0.0)
    for j, link in ((2, "y-"), (1, "y+"), (3, "y-")):
        t[("kw", j)] = (link, 128.0, (("kv", 4),), 2.0)
    t[("ay", 1)] = ("y+", ra / 4, (("tg", "a"),), 10.0)
    t[("ay", -1)] = ("y-", ra / 4, (("tg", "a"),), 10.0)
    t[("ay", 2)] = ("y+", ra / 4, (("tg", "a"),), 10.0)
    for p in range(4):
        for d in (1, -1, -2):
            t[("bs", d, p)] = ("z+" if d > 0 else "z-", rb / 8 if d != -2 else rb / 8, (("tg", "b"),), 1.0)
    far = {
        1: (("bs", 1), ("bs", -2)),
        2: (("bf", 1),),
        3: (("bf", 2), ("bf", 1)),
    }
    for stage in (1, 2, 3):
        for p in range(4):
            t[("bf", stage, p)] = (
                "z+", 1.0, tuple(k + (p,) for k in far[stage]), rb / 4 / RATE)
    column = (("tg", "a"), ("ay", 1), ("ay", -1), ("ay", 2))
    for s in range(4):
        size = ra if s < 3 else ra / 2
        t[("az+", s)] = ("z+", size, column if s == 0 else (("az+", s - 1),), 0.0)
        t[("az-", s)] = ("z-", size, column if s == 0 else (("az-", s - 1),), 0.0)
    for slot in "NF":
        for half in (0, 1):
            pieces = (2 * half, 2 * half + 1)
            need = (("tg", "b"),)
            if slot == "N":
                need += tuple(("bs", d, p) for d in (1, -1, -2) for p in pieces)
            else:
                need += tuple(("bf", stage, p) for stage in (1, 2, 3) for p in pieces)
            t[("by+", slot, half)] = ("y+", rb / 2, need, 0.0)
            t[("by-", slot, half)] = ("y-", rb / 2, need, 0.0)
        t[("bq+", slot, 0)] = ("y+", rb / 2, (("by+", slot, 0),), 0.0)
        t[("bq-", slot, 1)] = ("y-", rb / 2, (("by-", slot, 1),), 0.0)
    for m in range(4):
        for s in "+-":
            t[("at" + s, m)] = ("x" + s, 256.0, (("att", m),), 0.0)
            t[("ar2" + s, m)] = ("x" + s, 128.0, (("at" + s, m),), 0.0)
        t[("am", m, "own")] = ("d", 256.0 / 12, (("att", m),), 0.0)
        for s in "+-":
            t[("am", m, s)] = ("d", 256.0 / 12, (("at" + s, m),), 0.0)
            t[("am", m, s + "2")] = ("d", 128.0 / 12, (("ar2" + s, m),), 0.0)
    return t


def b_names(slots):
    out = []
    for slot in slots:
        for half in (0, 1):
            out += [("by+", slot, half), ("by-", slot, half)]
        out += [("bq+", slot, 0), ("bq-", slot, 1)]
    return out


def mat_needs(m, part):
    need = [("am", m, k) for k in ("own", "+", "-", "+2", "-2")]
    need += [("at+", m), ("at-", m), ("ar2+", m), ("ar2-", m)]
    need += b_names("N" if part == 0 else "NF")
    for s in range(DEPTH[part]):
        need += [("az+", s), ("az-", s)]
    return tuple(need)


def plan(t):
    rank = {}
    for n, name in enumerate(t):
        k = name[0]
        if k == "kv":
            r = 0
        elif k == "kw":
            r = 0.55
        elif k == "tg":
            r = 0
        elif k == "ay":
            r = 0.6
        elif k == "bs":
            r = 0.5
        elif k == "bf":
            r = 3
        elif k in ("az+", "az-"):
            r = 6
        elif k in ("at+", "at-"):
            r = 4
        elif k in ("ar2+", "ar2-"):
            r = 3
        elif k == "am":
            r = 4
        else:
            r = 5 if name[1] == "N" else 7
        rank[name] = (r, n)
    link_free, arrive = {}, {}
    pending = sorted(t, key=lambda k: rank[k])
    order, now = [], 0.0
    steps = [(m, g) for m in range(4) for g in range(2)]
    mats = [(m, part) for part in range(len(PARTS)) for m in range(4)]
    finals = []
    sent = {part: [] for part in range(len(PARTS))}

    def ready(names):
        return all(arrive.get(n, 1e9) <= now for n in names)

    def send(name, link, size, extra):
        start = max(now, link_free.get(link, 0.0))
        link_free[link] = start + size / RATE
        arrive[name] = link_free[link] + HOP + extra

    while pending or steps or mats or finals:
        for n in list(pending):
            if len(steps) == 8 and n[0] not in ("tg", "kv", "kw", "ay", "bs"):
                continue
            if ready(t[n][2]) and link_free.get(t[n][0], 0.0) - now < AHEAD:
                order.append(("send", n))
                send(n, *[t[n][i] for i in (0, 1, 3)])
                pending.remove(n)
        if steps:
            if ready([("kv", j) for j in range(1, BACK + 1)] + [("kw", j) for j in (1, 2, 3)]):
                m, g = steps.pop(0)
                order.append(("step", m, g))
                now += STEP
                if g == 1:
                    arrive[("att", m)] = now
                continue
        elif mats:
            ok = [c for c in mats if ready(mat_needs(*c))]
            if ok:
                m, part = ok[0]
                mats.remove(ok[0])
                order.append(("M", m, part))
                now += 0.35 * PARTS[part][1]
                send(("c", m, part), "x+", 35.0 * PARTS[part][1], 1.0)
                sent[part].append(("c", m, part))
                if len(sent[part]) == 4:
                    finals.append(part)
                continue
        if finals and not steps and ready(sent[finals[0]]):
            order.append(("F", finals.pop(0)))
            now += 1.0
            continue
        later = [a for a in arrive.values() if a > now]
        later += [f - AHEAD for f in link_free.values() if f - AHEAD > now]
        assert later, "stuck"
        now = min(later) + 1e-6
    return order, now, arrive


TASKS = build_tasks()
ORDER, MODEL_US, ARRIVE = plan(TASKS)


def tail_order(head):
    both = lambda kind, *rest: [("send", (kind + s,) + rest) for s in "+-"]
    got = lambda m, far: [("send", ("am", m, s + far)) for s in "+-"]
    out = both("at", 3) + [("send", ("am", 3, "own"))] + both("ar2", 1)
    out += [("send", ("bf", 3, p)) for p in (2, 3)] + both("by", "F", 0)
    out += got(0, "2") + both("by", "F", 1) + both("ar2", 2) + got(2, "") + both("az", 1)
    out += got(1, "2") + [("send", ("bq+", "F", 0))] + both("ar2", 3) + got(3, "")
    out += both("az", 2) + [("M", 0, 0)] + got(2, "2") + [("M", 1, 0), ("send", ("bq-", "F", 1))]
    out += got(3, "2") + [("M", 2, 0)] + both("az", 3) + [("M", 3, 0)]
    out += [("M", m, part) for part in (1, 2) for m in range(4)]
    out += [("F", part) for part in range(3)]
    rest = [o for o in ORDER if o not in head and o not in out]
    assert not rest, rest
    return [o for o in out if o not in head]


LAST = max(i for i, o in enumerate(ORDER) if o[0] == "step")
LATE = [("send", n) for n in (("by+", "F", 0), ("bf", 3, 2), ("bf", 3, 3))]
HEAD = [o for o in ORDER[:LAST] if o not in LATE]
HEAD += [("send", ("ar2+", 1)), ("send", ("ar2-", 1)), ORDER[LAST]]
ORDER = HEAD + tail_order(HEAD)
NAMES = list(TASKS)
NUMBER = {n: i for i, n in enumerate(NAMES)}


def cos_sin(angle):
    turns = jnp.floor(angle * (2.0 / math.pi) + 0.5)
    a = angle - turns * 1.5703125
    a = a - turns * 4.837512969970703125e-4
    a = a - turns * 7.549789948768648e-8
    quarter = turns - 4.0 * jnp.floor(turns * 0.25)
    s = a * a
    sine = a + a * s * (-1.6666654611e-1 + s * (8.3321608736e-3 - s * 1.9515295891e-4))
    cosine = 1.0 - 0.5 * s + s * s * (
        4.166664568298827e-2 + s * (-1.388731625493765e-3 + s * 2.443315711809948e-5))
    odd = (quarter == 1.0) | (quarter == 3.0)
    low_c = (quarter == 1.0) | (quarter == 2.0)
    c = jnp.where(odd, sine, cosine)
    d = jnp.where(odd, cosine, sine)
    return jnp.where(low_c, -c, c), jnp.where(quarter >= 2.0, -d, d)


def kernel(
    q_hbm, k_hbm, v_hbm, pos_hbm, seg_hbm, freq_ref, w_hbm, res_hbm, out_ref,
    wa, wb, q, cos, sin, kraw, kbuf, vbuf, hot, pos, seg, att, csend, crecv, res,
    send_sem, recv_sem, kv_send, kv_recv, tg_recv, c_send, c_recv, local,
):
    c = lax.axis_index("ctx")
    t = lax.axis_index("tp")
    z, h, y = c // 8, (c // 4) % 2, c % 4
    core = t % 2
    chip = t // 2
    x = h * 2 + chip
    owner = (z + y) % 4
    r = (t - z - y + 16) % 4
    me = h * 4 + t

    def ctx_of(dz, dh, dy):
        return (((z + dz + 8) % 8) * 8 + ((h + dh) % 2) * 4 + (y + dy + 4) % 4, t)

    def ring(d):
        other = (x + d + 4) % 4
        return (z * 8 + (other // 2) * 4 + y, (other % 2) * 2 + core)

    mate = (c, chip * 2 + (1 - core))
    barrier = pltpu.get_barrier_semaphore()
    partners = [ctx_of(1, 0, 0), ctx_of(-1, 0, 0), ctx_of(0, 0, 1), ctx_of(0, 0, -1), ctx_of(0, 0, 2), ctx_of(2, 0, 0), ctx_of(-2, 0, 0)]
    for d in range(4):
        for k in range(2):
            other = (x + d) % 4
            who = (z * 8 + (other // 2) * 4 + y, (other % 2) * 2 + (core + k) % 2)
            if d or k:
                partners.append(who)
    for j in (BACK, 64 - BACK):
        partners.append(((c + j) % 64, t))
    for d in partners:
        pl.semaphore_signal(barrier, inc=1, device_id=d, device_id_type=MESH)

    own = pl.ds(BACK * TOK, TOK)
    loads = {
        "pos": pltpu.make_async_copy(pos_hbm, pos.at[pl.ds(0, 3)], local.at[3]),
        "k": pltpu.make_async_copy(k_hbm, kraw, local.at[0]),
        "seg": pltpu.make_async_copy(seg_hbm, seg, local.at[4]),
        "v": pltpu.make_async_copy(v_hbm, vbuf.at[own], local.at[1]),
        "q": pltpu.make_async_copy(q_hbm, q, local.at[2]),
        "res": pltpu.make_async_copy(res_hbm, res, local.at[6]),
    }
    for cp in loads.values():
        cp.start()
    w_rows = {"a": pl.ds(0, ROWS_A), "b": pl.ds(ROWS_A, ROWS_B)}
    w_buf = {"a": wa, "b": wb}
    w_local = {
        k: pltpu.make_async_copy(w_hbm.at[w_rows[k]], w_buf[k].at[z, t], local.at[7 + i])
        for i, k in enumerate("ab")
    }

    @pl.when(owner == t)
    def _():
        for k in "ab":
            w_local[k].start()

    with jax.named_scope("tables"):
        pos[3:8, :] = jnp.zeros((5, TOK), jnp.int32)
        loads["pos"].wait()
        place = jnp.transpose(pos[...].astype(jnp.float32))
        lane = lax.broadcasted_iota(jnp.int32, (TOK, HD), 1) % (HD // 2)
        chosen = jnp.where(
            lane < HD // 8, place[:, 0:1],
            jnp.where(lane < HD // 8 + 3 * HD // 16, place[:, 1:2], place[:, 2:3]))
        cosine, sine = cos_sin(chosen * freq_ref[0:1, :])
        upper = lax.broadcasted_iota(jnp.int32, (TOK, HD), 1) < HD // 2
        cos[...] = cosine
        sin[...] = jnp.where(upper, -sine, sine)
        loads["k"].wait()
        kf = kraw[...].astype(jnp.float32)
        kbuf[own, :] = (kf * cos[...] + pltpu.roll(kf, HD // 2, 1) * sin[...]).astype(jnp.bfloat16)
        loads["v"].wait()
        loads["seg"].wait()
        for j in range(BACK + 1):
            rows = seg[pl.ds(((c - BACK + j + 64) % 64) * 4, 4), :].astype(jnp.float32)
            turned = jnp.transpose(jnp.concatenate([rows, rows], axis=0))
            ids = lax.broadcasted_iota(jnp.int32, (HD, HD), 1).astype(jnp.float32)
            for i in range(4):
                hot[pl.ds(j * TOK + i * HD, HD), :] = (
                    turned[:, i:i + 1] == ids).astype(jnp.float32).astype(jnp.bfloat16)
    with jax.named_scope("barrier"):
        pl.semaphore_wait(barrier, len(partners))

    def slot(which, dy):
        rr = (r - dy + 8) % 4
        near = jnp.where(rr == 3, -1, rr)
        return (z + near + (8 if which == "N" else 12)) % 8

    def halves(half):
        return pl.ds(2 * half, 2)

    def copies(name, incoming):
        kind = name[0]
        n = NUMBER.get(name)

        def one(src, dst, dev, ss=None, rs=None):
            return pltpu.make_async_remote_copy(
                src_ref=src, dst_ref=dst,
                send_sem=send_sem.at[n] if ss is None else ss,
                recv_sem=recv_sem.at[n] if rs is None else rs,
                device_id=dev, device_id_type=MESH)

        def same(ref, dev, **k):
            return one(ref, ref, dev, **k)

        if kind in ("kv", "kw"):
            j = name[1]
            to = pl.ds((BACK - j) * TOK, TOK)
            n = NUMBER[("kv", j)]
            wrap = y + j >= 4
            dev = ((c + 4) % 64, t) if j == 4 else ctx_of(0, 0, j)
            cond = None if j == 4 else (wrap if kind == "kw" else jnp.logical_not(wrap))
            at = own if kind == "kv" else pl.ds(0, TOK)
            if incoming:
                if kind == "kw":
                    return []
                cond = None
            return [(cond, one(vbuf.at[at], vbuf.at[to], dev, kv_send.at[j - 1], kv_recv.at[j - 1])),
                    (cond, one(kbuf.at[at], kbuf.at[to], dev))]
        if kind == "tg":
            k = name[1]
            i = "ab".index(k)
            if not incoming:
                return [(owner != t, one(w_hbm.at[w_rows[k]], w_buf[k].at[z, t], (c, owner),
                                         rs=tg_recv.at[i, t]))]
            return [((r == 0) & (t != u),
                     same(w_buf[k].at[z, u], (c, owner), rs=tg_recv.at[i, u])) for u in range(4)]
        if kind in ("at+", "at-", "ar2+", "ar2-", "am"):
            m = name[1]
            rows = pl.ds(m * CHUNK, CHUNK)
            if kind == "am":
                k = name[2]
                d = {"own": 0, "+": -1, "-": 1, "+2": 2, "-2": 2}[k]
                from_core = (1 - core) if incoming else core
                if k == "+2":
                    rows = pl.ds(m * CHUNK, CHUNK // 2)
                if k == "-2":
                    rows = pl.ds(m * CHUNK + CHUNK // 2, CHUNK // 2)
                i = ((x + d + 4) % 4) * 2 + from_core
                return [(None, same(att.at[i, rows], mate))]
            sign = 1 if kind[-1] == "+" else -1
            d = -sign * ((1 if kind[:3] == "ar2" else 0) + (1 if incoming else 0))
            if kind[:3] == "ar2":
                rows = pl.ds(m * CHUNK + (0 if sign > 0 else CHUNK // 2), CHUNK // 2)
            i = ((x + d + 4) % 4) * 2 + core
            return [(None, same(att.at[i, rows], ring(sign)))]
        if kind == "ay":
            d = name[1]
            cond = (r == (4 - d) % 4) if incoming else (r == 0)
            return [(cond, same(wa.at[z], ctx_of(0, 0, d)))]
        if kind == "bs":
            d, p = name[1], name[2]
            zs = (z - (d if incoming else 0) + 8) % 8
            cond = (r == (4 - d) % 4) if incoming else (r == 0)
            return [(cond, same(wb.at[zs, p], ctx_of(d, 0, 0)))]
        if kind == "bf":
            stage, p = name[1], name[2]
            out = []
            for sign, sender, carried in {
                1: ((1, 3, 1), (-1, 2, 2)),
                2: ((1, 2, 2),),
                3: ((1, 1, 3), (-1, 3, 3)),
            }[stage]:
                if stage == 3 and (p < 2) != (sign > 0):
                    continue
                rr = (sender - sign + 4) % 4 if incoming else sender
                zs = (z - sign * (carried + (1 if incoming else 0)) + 8) % 8
                out.append((r == rr, same(wb.at[zs, p], ctx_of(sign, 0, 0))))
            return out
        sign = 1 if kind[2] == "+" else -1
        if kind[:2] == "az":
            s = name[1]
            zz = (z - sign * (s + (1 if incoming else 0)) + 8) % 8
            ref = wa.at[zz] if s < 3 else wa.at[zz, halves(0 if sign > 0 else 1)]
            return [(None, same(ref, ctx_of(sign, 0, 0)))]
        which, half = name[1], name[2]
        step = (1 if kind[:2] == "bq" else 0) + (1 if incoming else 0)
        zs = slot(which, -sign * step)
        return [(None, same(wb.at[zs, halves(half)], ctx_of(0, 0, sign)))]

    def under(cond, act):
        if cond is None:
            act()
        else:
            pl.when(cond)(act)

    got = set()

    def need(names):
        for name in names:
            if name not in got and name[0] != "att":
                got.add(name)
                if name[0] == "tg":
                    @pl.when(owner == t)
                    def _(name=name):
                        w_local[name[1]].wait()
                for cond, cp in copies(name, True):
                    under(cond, cp.wait_recv)

    def send(name):
        need(TASKS[name][2])
        for cond, cp in copies(name, False):
            under(cond, cp.start)

    scale2 = (1.0 / math.sqrt(HD)) * math.log2(math.e)

    def rotate_queries():
        loads["q"].wait()

        def body(hd, carry):
            cols = pl.ds(pl.multiple_of(hd * HD, HD), HD)
            v = q[:, cols].astype(jnp.float32)
            v = v * cos[...] + pltpu.roll(v, HD // 2, 1) * sin[...]
            q[:, cols] = v.astype(jnp.bfloat16)
            return carry

        lax.fori_loop(0, HEADS, body, 0)

    def attend(m, g):
        rows = pl.ds(pl.multiple_of(m * CHUNK, CHUNK), CHUNK)
        keys = pl.ds(pl.multiple_of(m * CHUNK, CHUNK), WINDOW)
        mine = hot[pl.ds(pl.multiple_of(BACK * TOK + m * CHUNK, CHUNK), CHUNK), :]
        heads = []
        for i in range(4):
            qh = q[rows, pl.ds(pl.multiple_of((g * 4 + i) * HD, HD), HD)]
            heads.append(jnp.concatenate([qh, mine], axis=1))
        qs = jnp.concatenate(heads, axis=0)
        other = ((hot[keys, :].astype(jnp.float32) - 1.0) * BIG).astype(jnp.bfloat16)
        ks = jnp.concatenate([kbuf[keys, :], other], axis=1)
        score = lax.dot_general(
            qs, ks, (((1,), (1,)), ((), ())), preferred_element_type=jnp.float32)
        row = lax.broadcasted_iota(jnp.int32, (4 * CHUNK, CHUNK), 0) % CHUNK
        col = lax.broadcasted_iota(jnp.int32, (4 * CHUNK, CHUNK), 1)
        edge = jnp.where(col <= row, score[:, WINDOW - CHUNK:], -BIG)
        score = jnp.concatenate([score[:, :WINDOW - CHUNK], edge], axis=1)
        peak = jnp.max(score, axis=1, keepdims=True)
        prob = jnp.exp2((score - peak) * scale2).astype(jnp.bfloat16)
        vs = jnp.concatenate([vbuf[keys, :], jnp.ones((WINDOW, HD), jnp.bfloat16)], axis=1)
        mixed = jnp.dot(prob, vs, preferred_element_type=jnp.float32)
        result = (mixed[:, :HD] / mixed[:, HD:]).astype(jnp.bfloat16)
        for i in range(4):
            att[me, rows, pl.ds(pl.multiple_of((g * 4 + i) * HD, HD), HD)] = (
                result[i * CHUNK:(i + 1) * CHUNK])

    def part_cols(part):
        return pl.ds(PARTS[part][0] * HD, PARTS[part][1] * HD)

    def c_copy(m, hh, part):
        return pltpu.make_async_remote_copy(
            src_ref=csend.at[m, hh, :, part_cols(part)], dst_ref=crecv.at[me, :, part_cols(part)],
            send_sem=c_send.at[m, hh, part], recv_sem=c_recv.at[me, part],
            device_id=(z * 8 + hh * 4 + y, m), device_id_type=MESH)

    def matmul(m, part):
        need(mat_needs(m, part))
        rows = pl.ds(m * CHUNK, CHUNK)
        begin, count = PARTS[part]
        for at in range(begin, begin + count, 2):
            total = None
            wide = range(at, min(at + 2, begin + count))
            zs = [(z + ORDERED[i] + 8) % 8 for i in wide]
            for u in range(4):
                lhs = jnp.concatenate([att[u, rows, :], att[4 + u, rows, :]], axis=0)
                rhs = [jnp.concatenate([wa[i, u], wb[i, u]], axis=0) for i in zs]
                rhs = jnp.concatenate(rhs, axis=1) if len(rhs) > 1 else rhs[0]
                one = jnp.dot(lhs, rhs, preferred_element_type=jnp.float32)
                total = one if total is None else total + one
            total = total.astype(jnp.bfloat16)
            cols = pl.ds(at * HD, len(wide) * HD)
            for hh in range(2):
                csend[m, hh, :, cols] = total[hh * CHUNK:(hh + 1) * CHUNK]
        for hh in range(2):
            mine = (h == hh) & (t == m)

            @pl.when(mine)
            def _(hh=hh):
                crecv[me, :, part_cols(part)] = csend[m, hh, :, part_cols(part)]

            pl.when(jnp.logical_not(mine))(c_copy(m, hh, part).start)

    def final(part):
        if part == 0:
            loads["res"].wait()

        def body(s, carry):
            hs, ts = s // 4, s % 4
            cp = pltpu.make_async_remote_copy(
                src_ref=csend.at[0, 0, :, part_cols(part)], dst_ref=crecv.at[s, :, part_cols(part)],
                send_sem=c_send.at[0, 0, part], recv_sem=c_recv.at[s, part],
                device_id=mate, device_id_type=MESH)
            pl.when(s != me)(cp.wait_recv)
            for i in range(PARTS[part][0], sum(PARTS[part])):
                zs = (z + ORDERED[i] + 8) % 8
                col = (zs * 8 + hs * 4 + (ts - zs + 8) % 4) * HD
                wide = pl.ds(pl.multiple_of(col, HD), HD)
                got_c = crecv[s, :, i * HD:(i + 1) * HD].astype(jnp.float32)
                out_ref[:, wide] = (got_c + res[:, wide].astype(jnp.float32)).astype(jnp.bfloat16)
            return carry

        lax.fori_loop(0, 8, body, 0)

    items = list(ORDER)
    first = next(i for i, it in enumerate(items) if it[0] == "step")
    last = max(i for i, it in enumerate(items) if it[0] == "step")
    rotated = False
    for it in items[:first]:
        if not rotated and it[1][0] != "tg" and it[1][0] != "kv":
            rotated = True
            with jax.named_scope("rotq"):
                rotate_queries()
        with jax.named_scope("s_" + "_".join(map(str, it[1])).replace("+", "p").replace("-", "m")):
            send(it[1])
    need([("kv", j) for j in range(1, BACK + 1)])
    slots, at_step = {}, -1
    for it in items[first:last + 1]:
        if it[0] == "step":
            at_step += 1
        else:
            slots.setdefault(at_step, []).append(it[1])

    def step(i, carry):
        with jax.named_scope("attend"):
            attend(i // 2, i % 2)
        for k, names in slots.items():
            def issue(names=names):
                for name in names:
                    send(name)
            pl.when(i == k)(issue)
        return carry

    lax.fori_loop(0, 8, step, 0)
    for it in items[last + 1:]:
        if it[0] == "send":
            with jax.named_scope("s_" + "_".join(map(str, it[1])).replace("+", "p").replace("-", "m")):
                send(it[1])
        elif it[0] == "M":
            with jax.named_scope("M%d%d" % it[1:]):
                matmul(*it[1:])
        else:
            with jax.named_scope("F%d" % it[1]):
                final(it[1])
    for name in NAMES:
        need([name])
        for cond, cp in copies(name, False):
            under(cond, cp.wait_send)
    for m in range(4):
        for hh in range(2):
            for part in range(len(PARTS)):
                pl.when(jnp.logical_not((h == hh) & (t == m)))(c_copy(m, hh, part).wait_send)


def on_device(queries, keys, values, positions, segment_ids, out_weight, residual):
    half = jnp.arange(HD // 2).astype(jnp.float32)
    freq = theta_base ** (-2.0 * half / HD)
    freq = jnp.broadcast_to(jnp.concatenate([freq, freq])[None], (8, HD))
    anyspec = pl.BlockSpec(memory_space=pl.ANY)
    nt = len(NAMES)
    bf, f32 = jnp.bfloat16, jnp.float32
    dma = pltpu.SemaphoreType.DMA
    return pl.pallas_call(
        kernel,
        out_shape=jax.ShapeDtypeStruct((CHUNK, 8192), bf),
        in_specs=[anyspec] * 5 + [pl.BlockSpec(memory_space=pltpu.VMEM)] + [anyspec] * 2,
        out_specs=pl.BlockSpec(memory_space=pltpu.VMEM),
        scratch_shapes=[
            pltpu.VMEM((8, 4, ROWS_A, HD), bf),
            pltpu.VMEM((8, 4, ROWS_B, HD), bf),
            pltpu.VMEM((TOK, 1024), bf),
            pltpu.VMEM((TOK, HD), f32),
            pltpu.VMEM((TOK, HD), f32),
            pltpu.VMEM((TOK, HD), bf),
            pltpu.VMEM((SPAN, HD), bf),
            pltpu.VMEM((SPAN, HD), bf),
            pltpu.VMEM((SPAN, HD), bf),
            pltpu.VMEM((8, TOK), jnp.int32),
            pltpu.VMEM((256, HD), jnp.int32),
            pltpu.VMEM((8, TOK, 1024), bf),
            pltpu.VMEM((4, 2, CHUNK, 1024), bf),
            pltpu.VMEM((8, CHUNK, 1024), bf),
            pltpu.VMEM((CHUNK, 8192), bf),
            dma((nt,)),
            dma((nt,)),
            dma((BACK,)),
            dma((BACK,)),
            dma((2, 4)),
            dma((4, 2, len(PARTS))),
            dma((8, len(PARTS))),
            dma((9,)),
        ],
        compiler_params=pltpu.CompilerParams(
            collective_id=0, has_side_effects=True, vmem_limit_bytes=62 * 1024 * 1024),
    )(queries, keys, values, positions, segment_ids.reshape(256, HD), freq, out_weight, residual)


def solution(mesh):
    return jax.shard_map(
        on_device,
        mesh=mesh,
        in_specs=(
            P("ctx", "tp"),
            P("ctx", "tp"),
            P("ctx", "tp"),
            P(None, "ctx"),
            P(),
            P("tp", "ctx"),
            P(("ctx", "tp"), None),
        ),
        out_specs=P(("ctx", "tp"), None),
        check_vma=False,
    )
```

```python
import math

import jax
import jax.numpy as jnp
from jax import lax
from jax.experimental import pallas as pl
from jax.experimental.pallas import tpu as pltpu
from jax.sharding import PartitionSpec as P

HD = 128
HEADS = 8
TOK = 512
CHUNK = 128
BACK = 4
SPAN = (BACK + 1) * TOK
WINDOW = BACK * TOK + CHUNK
ROWS_A = 352
ROWS_B = 1024 - ROWS_A
RATE = 43.0
HOP = 2.0
STEP = 2.9
AHEAD = 6.0
BIG = 2.0**100
theta_base = 1000000.0
MESH = pl.DeviceIdType.MESH
ORDERED = (0, 1, -1, 2, -2, 3, -3, 4)
PARTS = ((0, 4), (4, 3), (7, 1))
DEPTH = (2, 3, 4)


def build_tasks():
    t = {}
    ra, rb = 384.0, 640.0
    t[("kv", 4)] = ("x+", 256.0, (), 2.0)
    t[("tg", "b")] = ("x-", rb / 4, (), 3.0)
    t[("tg", "a")] = ("x-", ra / 4, (), 3.0)
    for j, link in ((2, "y-"), (1, "y+"), (3, "y-")):
        t[("kv", j)] = (link, 128.0, (), 0.0)
    for j, link in ((2, "y-"), (1, "y+"), (3, "y-")):
        t[("kw", j)] = (link, 128.0, (("kv", 4),), 2.0)
    t[("ay", 1)] = ("y+", ra / 4, (("tg", "a"),), 10.0)
    t[("ay", -1)] = ("y-", ra / 4, (("tg", "a"),), 10.0)
    t[("ay", 2)] = ("y+", ra / 4, (("tg", "a"),), 10.0)
    for p in range(4):
        for d in (1, -1, -2):
            t[("bs", d, p)] = ("z+" if d > 0 else "z-", rb / 8 if d != -2 else rb / 8, (("tg", "b"),), 1.0)
    far = {
        1: (("bs", 1), ("bs", -2)),
        2: (("bf", 1),),
        3: (("bf", 2), ("bf", 1)),
    }
    for stage in (1, 2, 3):
        for p in range(4):
            t[("bf", stage, p)] = (
                "z+", 1.0, tuple(k + (p,) for k in far[stage]), rb / 4 / RATE)
    column = (("tg", "a"), ("ay", 1), ("ay", -1), ("ay", 2))
    for s in range(4):
        size = ra if s < 3 else ra / 2
        t[("az+", s)] = ("z+", size, column if s == 0 else (("az+", s - 1),), 0.0)
        t[("az-", s)] = ("z-", size, column if s == 0 else (("az-", s - 1),), 0.0)
    for slot in "NF":
        for half in (0, 1):
            pieces = (2 * half, 2 * half + 1)
            need = (("tg", "b"),)
            if slot == "N":
                need += tuple(("bs", d, p) for d in (1, -1, -2) for p in pieces)
            else:
                need += tuple(("bf", stage, p) for stage in (1, 2, 3) for p in pieces)
            t[("by+", slot, half)] = ("y+", rb / 2, need, 0.0)
            t[("by-", slot, half)] = ("y-", rb / 2, need, 0.0)
        t[("bq+", slot, 0)] = ("y+", rb / 2, (("by+", slot, 0),), 0.0)
        t[("bq-", slot, 1)] = ("y-", rb / 2, (("by-", slot, 1),), 0.0)
    for m in range(4):
        for s in "+-":
            t[("at" + s, m)] = ("x" + s, 256.0, (("att", m),), 0.0)
            t[("ar2" + s, m)] = ("x" + s, 128.0, (("at" + s, m),), 0.0)
        t[("am", m, "own")] = ("d", 256.0 / 12, (("att", m),), 0.0)
        for s in "+-":
            t[("am", m, s)] = ("d", 256.0 / 12, (("at" + s, m),), 0.0)
            t[("am", m, s + "2")] = ("d", 128.0 / 12, (("ar2" + s, m),), 0.0)
    return t


def b_names(slots):
    out = []
    for slot in slots:
        for half in (0, 1):
            out += [("by+", slot, half), ("by-", slot, half)]
        out += [("bq+", slot, 0), ("bq-", slot, 1)]
    return out


def mat_needs(m, part):
    need = [("am", m, k) for k in ("own", "+", "-", "+2", "-2")]
    need += [("at+", m), ("at-", m), ("ar2+", m), ("ar2-", m)]
    need += b_names("N" if part == 0 else "NF")
    for s in range(DEPTH[part]):
        need += [("az+", s), ("az-", s)]
    return tuple(need)


def plan(t):
    rank = {}
    for n, name in enumerate(t):
        k = name[0]
        if k == "kv":
            r = 0
        elif k == "kw":
            r = 0.55
        elif k == "tg":
            r = 0
        elif k == "ay":
            r = 0.6
        elif k == "bs":
            r = 0.5
        elif k == "bf":
            r = 3
        elif k in ("az+", "az-"):
            r = 6
        elif k in ("at+", "at-"):
            r = 4
        elif k in ("ar2+", "ar2-"):
            r = 3
        elif k == "am":
            r = 4
        else:
            r = 5 if name[1] == "N" else 7
        rank[name] = (r, n)
    link_free, arrive = {}, {}
    pending = sorted(t, key=lambda k: rank[k])
    order, now = [], 0.0
    steps = [(m, g) for m in range(4) for g in range(2)]
    mats = [(m, part) for part in range(len(PARTS)) for m in range(4)]
    finals = []
    sent = {part: [] for part in range(len(PARTS))}

    def ready(names):
        return all(arrive.get(n, 1e9) <= now for n in names)

    def send(name, link, size, extra):
        start = max(now, link_free.get(link, 0.0))
        link_free[link] = start + size / RATE
        arrive[name] = link_free[link] + HOP + extra

    while pending or steps or mats or finals:
        for n in list(pending):
            if len(steps) == 8 and n[0] not in ("tg", "kv", "kw", "ay", "bs"):
                continue
            if ready(t[n][2]) and link_free.get(t[n][0], 0.0) - now < AHEAD:
                order.append(("send", n))
                send(n, *[t[n][i] for i in (0, 1, 3)])
                pending.remove(n)
        if steps:
            if ready([("kv", j) for j in range(1, BACK + 1)] + [("kw", j) for j in (1, 2, 3)]):
                m, g = steps.pop(0)
                order.append(("step", m, g))
                now += STEP
                if g == 1:
                    arrive[("att", m)] = now
                continue
        elif mats:
            ok = [c for c in mats if ready(mat_needs(*c))]
            if ok:
                m, part = ok[0]
                mats.remove(ok[0])
                order.append(("M", m, part))
                now += 0.35 * PARTS[part][1]
                send(("c", m, part), "x+", 35.0 * PARTS[part][1], 1.0)
                sent[part].append(("c", m, part))
                if len(sent[part]) == 4:
                    finals.append(part)
                continue
        if finals and not steps and ready(sent[finals[0]]):
            order.append(("F", finals.pop(0)))
            now += 1.0
            continue
        later = [a for a in arrive.values() if a > now]
        later += [f - AHEAD for f in link_free.values() if f - AHEAD > now]
        assert later, "stuck"
        now = min(later) + 1e-6
    return order, now, arrive


TASKS = build_tasks()
ORDER, MODEL_US, ARRIVE = plan(TASKS)


def tail_order(head):
    both = lambda kind, *rest: [("send", (kind + s,) + rest) for s in "+-"]
    got = lambda m, far: [("send", ("am", m, s + far)) for s in "+-"]
    out = both("at", 3) + [("send", ("am", 3, "own"))] + both("ar2", 1)
    out += [("send", ("bf", 3, p)) for p in (2, 3)] + both("by", "F", 0)
    out += got(0, "2") + both("by", "F", 1) + both("ar2", 2) + got(2, "") + both("az", 1)
    out += got(1, "2") + [("send", ("bq+", "F", 0))] + both("ar2", 3) + got(3, "")
    out += both("az", 2) + [("M", 0, 0)] + got(2, "2") + [("M", 1, 0), ("send", ("bq-", "F", 1))]
    out += got(3, "2") + [("M", 2, 0)] + both("az", 3) + [("M", 3, 0)]
    out += [("M", m, part) for part in (1, 2) for m in range(4)]
    out += [("F", part) for part in range(3)]
    rest = [o for o in ORDER if o not in head and o not in out]
    assert not rest, rest
    return [o for o in out if o not in head]


LAST = max(i for i, o in enumerate(ORDER) if o[0] == "step")
LATE = [("send", n) for n in (("by+", "F", 0), ("bf", 3, 2), ("bf", 3, 3))]
HEAD = [o for o in ORDER[:LAST] if o not in LATE]
HEAD += [("send", ("ar2+", 1)), ("send", ("ar2-", 1)), ORDER[LAST]]
ORDER = HEAD + tail_order(HEAD)
NAMES = list(TASKS)
NUMBER = {n: i for i, n in enumerate(NAMES)}


def cos_sin(angle):
    turns = jnp.floor(angle * (2.0 / math.pi) + 0.5)
    a = angle - turns * 1.5703125
    a = a - turns * 4.837512969970703125e-4
    a = a - turns * 7.549789948768648e-8
    quarter = turns - 4.0 * jnp.floor(turns * 0.25)
    s = a * a
    sine = a + a * s * (-1.6666654611e-1 + s * (8.3321608736e-3 - s * 1.9515295891e-4))
    cosine = 1.0 - 0.5 * s + s * s * (
        4.166664568298827e-2 + s * (-1.388731625493765e-3 + s * 2.443315711809948e-5))
    odd = (quarter == 1.0) | (quarter == 3.0)
    low_c = (quarter == 1.0) | (quarter == 2.0)
    c = jnp.where(odd, sine, cosine)
    d = jnp.where(odd, cosine, sine)
    return jnp.where(low_c, -c, c), jnp.where(quarter >= 2.0, -d, d)


def kernel(
    q_hbm, k_hbm, v_hbm, pos_hbm, seg_hbm, freq_ref, w_hbm, res_hbm, out_ref,
    wa, wb, q, cos, sin, kraw, kbuf, vbuf, hot, pos, seg, att, csend, crecv, res,
    send_sem, recv_sem, kv_send, kv_recv, tg_recv, c_send, c_recv, local,
):
    c = lax.axis_index("ctx")
    t = lax.axis_index("tp")
    z, h, y = c // 8, (c // 4) % 2, c % 4
    core = t % 2
    chip = t // 2
    x = h * 2 + chip
    owner = (z + y) % 4
    r = (t - z - y + 16) % 4
    me = h * 4 + t

    def ctx_of(dz, dh, dy):
        return (((z + dz + 8) % 8) * 8 + ((h + dh) % 2) * 4 + (y + dy + 4) % 4, t)

    def ring(d):
        other = (x + d + 4) % 4
        return (z * 8 + (other // 2) * 4 + y, (other % 2) * 2 + core)

    mate = (c, chip * 2 + (1 - core))
    barrier = pltpu.get_barrier_semaphore()
    partners = [ctx_of(1, 0, 0), ctx_of(-1, 0, 0), ctx_of(0, 0, 1), ctx_of(0, 0, -1), ctx_of(0, 0, 2), ctx_of(2, 0, 0), ctx_of(-2, 0, 0)]
    for d in range(4):
        for k in range(2):
            other = (x + d) % 4
            who = (z * 8 + (other // 2) * 4 + y, (other % 2) * 2 + (core + k) % 2)
            if d or k:
                partners.append(who)
    for j in (BACK, 64 - BACK):
        partners.append(((c + j) % 64, t))
    for d in partners:
        pl.semaphore_signal(barrier, inc=1, device_id=d, device_id_type=MESH)

    own = pl.ds(BACK * TOK, TOK)
    loads = {
        "pos": pltpu.make_async_copy(pos_hbm, pos.at[pl.ds(0, 3)], local.at[3]),
        "k": pltpu.make_async_copy(k_hbm, kraw, local.at[0]),
        "seg": pltpu.make_async_copy(seg_hbm, seg, local.at[4]),
        "v": pltpu.make_async_copy(v_hbm, vbuf.at[own], local.at[1]),
        "q": pltpu.make_async_copy(q_hbm, q, local.at[2]),
        "res": pltpu.make_async_copy(res_hbm, res, local.at[6]),
    }
    for cp in loads.values():
        cp.start()
    w_rows = {"a": pl.ds(0, ROWS_A), "b": pl.ds(ROWS_A, ROWS_B)}
    w_buf = {"a": wa, "b": wb}
    w_local = {
        k: pltpu.make_async_copy(w_hbm.at[w_rows[k]], w_buf[k].at[z, t], local.at[7 + i])
        for i, k in enumerate("ab")
    }

    @pl.when(owner == t)
    def _():
        for k in "ab":
            w_local[k].start()

    with jax.named_scope("tables"):
        pos[3:8, :] = jnp.zeros((5, TOK), jnp.int32)
        loads["pos"].wait()
        place = jnp.transpose(pos[...].astype(jnp.float32))
        lane = lax.broadcasted_iota(jnp.int32, (TOK, HD), 1) % (HD // 2)
        chosen = jnp.where(
            lane < HD // 8, place[:, 0:1],
            jnp.where(lane < HD // 8 + 3 * HD // 16, place[:, 1:2], place[:, 2:3]))
        cosine, sine = cos_sin(chosen * freq_ref[0:1, :])
        upper = lax.broadcasted_iota(jnp.int32, (TOK, HD), 1) < HD // 2
        cos[...] = cosine
        sin[...] = jnp.where(upper, -sine, sine)
        loads["k"].wait()
        kf = kraw[...].astype(jnp.float32)
        kbuf[own, :] = (kf * cos[...] + pltpu.roll(kf, HD // 2, 1) * sin[...]).astype(jnp.bfloat16)
        loads["v"].wait()
        loads["seg"].wait()
        for j in range(BACK + 1):
            rows = seg[pl.ds(((c - BACK + j + 64) % 64) * 4, 4), :].astype(jnp.float32)
            turned = jnp.transpose(jnp.concatenate([rows, rows], axis=0))
            ids = lax.broadcasted_iota(jnp.int32, (HD, HD), 1).astype(jnp.float32)
            for i in range(4):
                hot[pl.ds(j * TOK + i * HD, HD), :] = (
                    turned[:, i:i + 1] == ids).astype(jnp.float32).astype(jnp.bfloat16)
    with jax.named_scope("barrier"):
        pl.semaphore_wait(barrier, len(partners))

    def slot(which, dy):
        rr = (r - dy + 8) % 4
        near = jnp.where(rr == 3, -1, rr)
        return (z + near + (8 if which == "N" else 12)) % 8

    def halves(half):
        return pl.ds(2 * half, 2)

    def copies(name, incoming):
        kind = name[0]
        n = NUMBER.get(name)

        def one(src, dst, dev, ss=None, rs=None):
            return pltpu.make_async_remote_copy(
                src_ref=src, dst_ref=dst,
                send_sem=send_sem.at[n] if ss is None else ss,
                recv_sem=recv_sem.at[n] if rs is None else rs,
                device_id=dev, device_id_type=MESH)

        def same(ref, dev, **k):
            return one(ref, ref, dev, **k)

        if kind in ("kv", "kw"):
            j = name[1]
            to = pl.ds((BACK - j) * TOK, TOK)
            n = NUMBER[("kv", j)]
            wrap = y + j >= 4
            dev = ((c + 4) % 64, t) if j == 4 else ctx_of(0, 0, j)
            cond = None if j == 4 else (wrap if kind == "kw" else jnp.logical_not(wrap))
            at = own if kind == "kv" else pl.ds(0, TOK)
            if incoming:
                if kind == "kw":
                    return []
                cond = None
            return [(cond, one(vbuf.at[at], vbuf.at[to], dev, kv_send.at[j - 1], kv_recv.at[j - 1])),
                    (cond, one(kbuf.at[at], kbuf.at[to], dev))]
        if kind == "tg":
            k = name[1]
            i = "ab".index(k)
            if not incoming:
                return [(owner != t, one(w_hbm.at[w_rows[k]], w_buf[k].at[z, t], (c, owner),
                                         rs=tg_recv.at[i, t]))]
            return [((r == 0) & (t != u),
                     same(w_buf[k].at[z, u], (c, owner), rs=tg_recv.at[i, u])) for u in range(4)]
        if kind in ("at+", "at-", "ar2+", "ar2-", "am"):
            m = name[1]
            rows = pl.ds(m * CHUNK, CHUNK)
            if kind == "am":
                k = name[2]
                d = {"own": 0, "+": -1, "-": 1, "+2": 2, "-2": 2}[k]
                from_core = (1 - core) if incoming else core
                if k == "+2":
                    rows = pl.ds(m * CHUNK, CHUNK // 2)
                if k == "-2":
                    rows = pl.ds(m * CHUNK + CHUNK // 2, CHUNK // 2)
                i = ((x + d + 4) % 4) * 2 + from_core
                return [(None, same(att.at[i, rows], mate))]
            sign = 1 if kind[-1] == "+" else -1
            d = -sign * ((1 if kind[:3] == "ar2" else 0) + (1 if incoming else 0))
            if kind[:3] == "ar2":
                rows = pl.ds(m * CHUNK + (0 if sign > 0 else CHUNK // 2), CHUNK // 2)
            i = ((x + d + 4) % 4) * 2 + core
            return [(None, same(att.at[i, rows], ring(sign)))]
        if kind == "ay":
            d = name[1]
            cond = (r == (4 - d) % 4) if incoming else (r == 0)
            return [(cond, same(wa.at[z], ctx_of(0, 0, d)))]
        if kind == "bs":
            d, p = name[1], name[2]
            zs = (z - (d if incoming else 0) + 8) % 8
            cond = (r == (4 - d) % 4) if incoming else (r == 0)
            return [(cond, same(wb.at[zs, p], ctx_of(d, 0, 0)))]
        if kind == "bf":
            stage, p = name[1], name[2]
            out = []
            for sign, sender, carried in {
                1: ((1, 3, 1), (-1, 2, 2)),
                2: ((1, 2, 2),),
                3: ((1, 1, 3), (-1, 3, 3)),
            }[stage]:
                if stage == 3 and (p < 2) != (sign > 0):
                    continue
                rr = (sender - sign + 4) % 4 if incoming else sender
                zs = (z - sign * (carried + (1 if incoming else 0)) + 8) % 8
                out.append((r == rr, same(wb.at[zs, p], ctx_of(sign, 0, 0))))
            return out
        sign = 1 if kind[2] == "+" else -1
        if kind[:2] == "az":
            s = name[1]
            zz = (z - sign * (s + (1 if incoming else 0)) + 8) % 8
            ref = wa.at[zz] if s < 3 else wa.at[zz, halves(0 if sign > 0 else 1)]
            return [(None, same(ref, ctx_of(sign, 0, 0)))]
        which, half = name[1], name[2]
        step = (1 if kind[:2] == "bq" else 0) + (1 if incoming else 0)
        zs = slot(which, -sign * step)
        return [(None, same(wb.at[zs, halves(half)], ctx_of(0, 0, sign)))]

    def under(cond, act):
        if cond is None:
            act()
        else:
            pl.when(cond)(act)

    got = set()

    def need(names):
        for name in names:
            if name not in got and name[0] != "att":
                got.add(name)
                if name[0] == "tg":
                    @pl.when(owner == t)
                    def _(name=name):
                        w_local[name[1]].wait()
                for cond, cp in copies(name, True):
                    under(cond, cp.wait_recv)

    def send(name):
        need(TASKS[name][2])
        for cond, cp in copies(name, False):
            under(cond, cp.start)

    scale2 = (1.0 / math.sqrt(HD)) * math.log2(math.e)

    def rotate_queries():
        loads["q"].wait()

        def body(hd, carry):
            cols = pl.ds(pl.multiple_of(hd * HD, HD), HD)
            v = q[:, cols].astype(jnp.float32)
            v = v * cos[...] + pltpu.roll(v, HD // 2, 1) * sin[...]
            q[:, cols] = v.astype(jnp.bfloat16)
            return carry

        lax.fori_loop(0, HEADS, body, 0)

    def attend(m, g):
        rows = pl.ds(pl.multiple_of(m * CHUNK, CHUNK), CHUNK)
        keys = pl.ds(pl.multiple_of(m * CHUNK, CHUNK), WINDOW)
        mine = hot[pl.ds(pl.multiple_of(BACK * TOK + m * CHUNK, CHUNK), CHUNK), :]
        heads = []
        for i in range(4):
            qh = q[rows, pl.ds(pl.multiple_of((g * 4 + i) * HD, HD), HD)]
            heads.append(jnp.concatenate([qh, mine], axis=1))
        qs = jnp.concatenate(heads, axis=0)
        other = ((hot[keys, :].astype(jnp.float32) - 1.0) * BIG).astype(jnp.bfloat16)
        ks = jnp.concatenate([kbuf[keys, :], other], axis=1)
        score = lax.dot_general(
            qs, ks, (((1,), (1,)), ((), ())), preferred_element_type=jnp.float32)
        row = lax.broadcasted_iota(jnp.int32, (4 * CHUNK, CHUNK), 0) % CHUNK
        col = lax.broadcasted_iota(jnp.int32, (4 * CHUNK, CHUNK), 1)
        edge = jnp.where(col <= row, score[:, WINDOW - CHUNK:], -BIG)
        score = jnp.concatenate([score[:, :WINDOW - CHUNK], edge], axis=1)
        peak = jnp.max(score, axis=1, keepdims=True)
        prob = jnp.exp2((score - peak) * scale2).astype(jnp.bfloat16)
        vs = jnp.concatenate([vbuf[keys, :], jnp.ones((WINDOW, HD), jnp.bfloat16)], axis=1)
        mixed = jnp.dot(prob, vs, preferred_element_type=jnp.float32)
        result = (mixed[:, :HD] / mixed[:, HD:]).astype(jnp.bfloat16)
        for i in range(4):
            att[me, rows, pl.ds(pl.multiple_of((g * 4 + i) * HD, HD), HD)] = (
                result[i * CHUNK:(i + 1) * CHUNK])

    def part_cols(part):
        return pl.ds(PARTS[part][0] * HD, PARTS[part][1] * HD)

    def c_copy(m, hh, part):
        return pltpu.make_async_remote_copy(
            src_ref=csend.at[m, hh, :, part_cols(part)], dst_ref=crecv.at[me, :, part_cols(part)],
            send_sem=c_send.at[m, hh, part], recv_sem=c_recv.at[me, part],
            device_id=(z * 8 + hh * 4 + y, m), device_id_type=MESH)

    def matmul(m, part):
        need(mat_needs(m, part))
        rows = pl.ds(m * CHUNK, CHUNK)
        begin, count = PARTS[part]
        for at in range(begin, begin + count, 2):
            total = None
            wide = range(at, min(at + 2, begin + count))
            zs = [(z + ORDERED[i] + 8) % 8 for i in wide]
            for u in range(4):
                lhs = jnp.concatenate([att[u, rows, :], att[4 + u, rows, :]], axis=0)
                rhs = [jnp.concatenate([wa[i, u], wb[i, u]], axis=0) for i in zs]
                rhs = jnp.concatenate(rhs, axis=1) if len(rhs) > 1 else rhs[0]
                one = jnp.dot(lhs, rhs, preferred_element_type=jnp.float32)
                total = one if total is None else total + one
            total = total.astype(jnp.bfloat16)
            cols = pl.ds(at * HD, len(wide) * HD)
            for hh in range(2):
                csend[m, hh, :, cols] = total[hh * CHUNK:(hh + 1) * CHUNK]
        for hh in range(2):
            mine = (h == hh) & (t == m)

            @pl.when(mine)
            def _(hh=hh):
                crecv[me, :, part_cols(part)] = csend[m, hh, :, part_cols(part)]

            pl.when(jnp.logical_not(mine))(c_copy(m, hh, part).start)

    def final(part):
        if part == 0:
            loads["res"].wait()

        def body(s, carry):
            hs, ts = s // 4, s % 4
            cp = pltpu.make_async_remote_copy(
                src_ref=csend.at[0, 0, :, part_cols(part)], dst_ref=crecv.at[s, :, part_cols(part)],
                send_sem=c_send.at[0, 0, part], recv_sem=c_recv.at[s, part],
                device_id=mate, device_id_type=MESH)
            pl.when(s != me)(cp.wait_recv)
            for i in range(PARTS[part][0], sum(PARTS[part])):
                zs = (z + ORDERED[i] + 8) % 8
                col = (zs * 8 + hs * 4 + (ts - zs + 8) % 4) * HD
                wide = pl.ds(pl.multiple_of(col, HD), HD)
                got_c = crecv[s, :, i * HD:(i + 1) * HD].astype(jnp.float32)
                out_ref[:, wide] = (got_c + res[:, wide].astype(jnp.float32)).astype(jnp.bfloat16)
            return carry

        lax.fori_loop(0, 8, body, 0)

    items = list(ORDER)
    first = next(i for i, it in enumerate(items) if it[0] == "step")
    last = max(i for i, it in enumerate(items) if it[0] == "step")
    rotated = False
    for it in items[:first]:
        if not rotated and it[1][0] != "tg" and it[1][0] != "kv":
            rotated = True
            with jax.named_scope("rotq"):
                rotate_queries()
        with jax.named_scope("s_" + "_".join(map(str, it[1])).replace("+", "p").replace("-", "m")):
            send(it[1])
    need([("kv", j) for j in range(1, BACK + 1)])
    slots, at_step = {}, -1
    for it in items[first:last + 1]:
        if it[0] == "step":
            at_step += 1
        else:
            slots.setdefault(at_step, []).append(it[1])

    def step(i, carry):
        with jax.named_scope("attend"):
            attend(i // 2, i % 2)
        for k, names in slots.items():
            def issue(names=names):
                for name in names:
                    send(name)
            pl.when(i == k)(issue)
        return carry

    lax.fori_loop(0, 8, step, 0)
    for it in items[last + 1:]:
        if it[0] == "send":
            with jax.named_scope("s_" + "_".join(map(str, it[1])).replace("+", "p").replace("-", "m")):
                send(it[1])
        elif it[0] == "M":
            with jax.named_scope("M%d%d" % it[1:]):
                matmul(*it[1:])
        else:
            with jax.named_scope("F%d" % it[1]):
                final(it[1])
    for name in NAMES:
        need([name])
        for cond, cp in copies(name, False):
            under(cond, cp.wait_send)
    for m in range(4):
        for hh in range(2):
            for part in range(len(PARTS)):
                pl.when(jnp.logical_not((h == hh) & (t == m)))(c_copy(m, hh, part).wait_send)


def on_device(queries, keys, values, positions, segment_ids, out_weight, residual):
    half = jnp.arange(HD // 2).astype(jnp.float32)
    freq = theta_base ** (-2.0 * half / HD)
    freq = jnp.broadcast_to(jnp.concatenate([freq, freq])[None], (8, HD))
    anyspec = pl.BlockSpec(memory_space=pl.ANY)
    nt = len(NAMES)
    bf, f32 = jnp.bfloat16, jnp.float32
    dma = pltpu.SemaphoreType.DMA
    return pl.pallas_call(
        kernel,
        out_shape=jax.ShapeDtypeStruct((CHUNK, 8192), bf),
        in_specs=[anyspec] * 5 + [pl.BlockSpec(memory_space=pltpu.VMEM)] + [anyspec] * 2,
        out_specs=pl.BlockSpec(memory_space=pltpu.VMEM),
        scratch_shapes=[
            pltpu.VMEM((8, 4, ROWS_A, HD), bf),
            pltpu.VMEM((8, 4, ROWS_B, HD), bf),
            pltpu.VMEM((TOK, 1024), bf),
            pltpu.VMEM((TOK, HD), f32),
            pltpu.VMEM((TOK, HD), f32),
            pltpu.VMEM((TOK, HD), bf),
            pltpu.VMEM((SPAN, HD), bf),
            pltpu.VMEM((SPAN, HD), bf),
            pltpu.VMEM((SPAN, HD), bf),
            pltpu.VMEM((8, TOK), jnp.int32),
            pltpu.VMEM((256, HD), jnp.int32),
            pltpu.VMEM((8, TOK, 1024), bf),
            pltpu.VMEM((4, 2, CHUNK, 1024), bf),
            pltpu.VMEM((8, CHUNK, 1024), bf),
            pltpu.VMEM((CHUNK, 8192), bf),
            dma((nt,)),
            dma((nt,)),
            dma((BACK,)),
            dma((BACK,)),
            dma((2, 4)),
            dma((4, 2, len(PARTS))),
            dma((8, len(PARTS))),
            dma((9,)),
        ],
        compiler_params=pltpu.CompilerParams(
            collective_id=0, has_side_effects=True, vmem_limit_bytes=62 * 1024 * 1024),
    )(queries, keys, values, positions, segment_ids.reshape(256, HD), freq, out_weight, residual)


def solution(mesh):
    return jax.shard_map(
        on_device,
        mesh=mesh,
        in_specs=(
            P("ctx", "tp"),
            P("ctx", "tp"),
            P("ctx", "tp"),
            P(None, "ctx"),
            P(),
            P("tp", "ctx"),
            P(("ctx", "tp"), None),
        ),
        out_specs=P(("ctx", "tp"), None),
        check_vma=False,
    )
```
